8 devices in a mesh: data: 1 (over z), model: 2 (over y), stage: 4 (over x, core).
Axes of the slice: x: 2, y: 2, z: 1, core: 2. Of those that a mesh axis runs over, the one named last changes fastest.
Arguments:
- inputs: bfloat16 [12, 512, 2560], P('data')
- targets: bfloat16 [12, 512, 2560], P('data')
- w_in: bfloat16 [4, 1, 2560, 10240], P('stage', None, None, 'model')
- w_out: bfloat16 [4, 1, 10240, 2560], P('stage', None, 'model')
Outputs:
- output 1: float32 [4, 1, 2560, 10240], P(('data', 'stage'), None, None, 'model')
- output 2: float32 [4, 1, 10240, 2560], P(('data', 'stage'), None, 'model')
- output 3: float32 [1], P('data')
All inputs are finite; a program needn't handle non-finite values.
Results may differ from the reference program's by a relative error of at most 0.00358275.
Values are sent between devices in bfloat16 or wider.
A program may use at most 1 GiB of HBM per device.

```python
import jax
import jax.numpy as jnp
from jax import lax

STAGES = 4
LAYERS_PER_STAGE = 1
MODEL_DIM = 2560
HIDDEN_DIM = 10240
MICRO_BATCHES = 12
MICRO_TOKENS = 512

TOTAL_LAYERS = STAGES * LAYERS_PER_STAGE
GELU_COEF = 0.7978845608028654
CUBIC_COEF = 0.044715


def gelu_tanh(values):
    inner_arg = GELU_COEF * (values + CUBIC_COEF * values * values * values)
    return 0.5 * values * (1.0 + jnp.tanh(inner_arg))


def gelu_slope(values):
    tanh_val = jnp.tanh(GELU_COEF * (values + CUBIC_COEF * values * values * values))
    return 0.5 * (1.0 + tanh_val) + 0.5 * values * (1.0 - tanh_val * tanh_val) * GELU_COEF * (1.0 + 3.0 * CUBIC_COEF * values * values)


def setup_inputs(seed: int = 0, part: int = 0) -> dict:
    part_key = jax.random.fold_in(jax.random.key(seed), part)
    key_in, key_tgt = jax.random.split(part_key, 2)
    key_w1, key_w2 = jax.random.split(jax.random.key(seed + 1), 2)
    act_shape = (MICRO_BATCHES, MICRO_TOKENS, MODEL_DIM)
    inputs = jax.random.normal(key_in, act_shape, jnp.float32).astype(jnp.bfloat16)
    targets = jax.random.normal(key_tgt, act_shape, jnp.float32).astype(jnp.bfloat16)
    in_scale = MODEL_DIM ** -0.5
    out_scale = (HIDDEN_DIM ** -0.5) * (2.0 / TOTAL_LAYERS) ** 0.5
    w_in = (jax.random.normal(key_w1, (STAGES, LAYERS_PER_STAGE, MODEL_DIM, HIDDEN_DIM), jnp.float32) * in_scale).astype(jnp.bfloat16)
    w_out = (jax.random.normal(key_w2, (STAGES, LAYERS_PER_STAGE, HIDDEN_DIM, MODEL_DIM), jnp.float32) * out_scale).astype(jnp.bfloat16)
    return {"inputs": inputs, "targets": targets, "w_in": w_in, "w_out": w_out}


def layer_forward(hidden, w_in_l, w_out_l):
    pre_act = jnp.dot(hidden, w_in_l, preferred_element_type=jnp.float32).astype(jnp.bfloat16)
    act_out = gelu_tanh(pre_act.astype(jnp.float32)).astype(jnp.bfloat16)
    branch = jnp.dot(act_out, w_out_l, preferred_element_type=jnp.float32)
    return (hidden.astype(jnp.float32) + branch).astype(jnp.bfloat16)


def layer_backward(grad_h, hidden, w_in_l, w_out_l):
    pre_act = jnp.dot(hidden, w_in_l, preferred_element_type=jnp.float32).astype(jnp.bfloat16)
    act_out = gelu_tanh(pre_act.astype(jnp.float32)).astype(jnp.bfloat16)
    grad_act = jnp.dot(grad_h, w_out_l.T, preferred_element_type=jnp.float32).astype(jnp.bfloat16)
    grad_pre = (gelu_slope(pre_act.astype(jnp.float32)) * grad_act.astype(jnp.float32)).astype(jnp.bfloat16)
    grad_prev = (grad_h.astype(jnp.float32) + jnp.dot(grad_pre, w_in_l.T, preferred_element_type=jnp.float32)).astype(jnp.bfloat16)
    part_in = jnp.dot(hidden.T, grad_pre, preferred_element_type=jnp.float32)
    part_out = jnp.dot(act_out.T, grad_h, preferred_element_type=jnp.float32)
    return grad_prev, part_in, part_out


def reference(inputs, targets, w_in, w_out):
    w_in_flat = w_in.reshape(TOTAL_LAYERS, MODEL_DIM, HIDDEN_DIM)
    w_out_flat = w_out.reshape(TOTAL_LAYERS, HIDDEN_DIM, MODEL_DIM)
    grad_scale = 1.0 / (MICRO_BATCHES * MICRO_TOKENS * MODEL_DIM)

    def fwd_step(hidden, layer_w):
        return layer_forward(hidden, layer_w[0], layer_w[1]), hidden

    def bwd_step(grad_h, layer_data):
        w_in_l, w_out_l, saved_in, acc_in, acc_out = layer_data
        grad_prev, part_in, part_out = layer_backward(grad_h, saved_in, w_in_l, w_out_l)
        return grad_prev, (acc_in + part_in, acc_out + part_out)

    def micro_step(state_in, micro_pair):
        acc_in, acc_out, loss_sum = state_in
        final_out, saved_in = lax.scan(fwd_step, micro_pair[0], (w_in_flat, w_out_flat))
        out_err = final_out.astype(jnp.float32) - micro_pair[1].astype(jnp.float32)
        start_grad = (out_err * grad_scale).astype(jnp.bfloat16)
        input_grad, (acc_in, acc_out) = lax.scan(bwd_step, start_grad, (w_in_flat, w_out_flat, saved_in, acc_in, acc_out), reverse=True)
        return (acc_in, acc_out, loss_sum + 0.5 * jnp.sum(out_err * out_err)), None

    init_state = (jnp.zeros((TOTAL_LAYERS, MODEL_DIM, HIDDEN_DIM), jnp.float32), jnp.zeros((TOTAL_LAYERS, HIDDEN_DIM, MODEL_DIM), jnp.float32), jnp.zeros((), jnp.float32))
    (acc_in, acc_out, loss_sum), unused_ys = lax.scan(micro_step, init_state, (inputs, targets))
    grad_in = acc_in.reshape(STAGES, LAYERS_PER_STAGE, MODEL_DIM, HIDDEN_DIM)
    grad_out = acc_out.reshape(STAGES, LAYERS_PER_STAGE, HIDDEN_DIM, MODEL_DIM)
    return grad_in, grad_out, jnp.reshape(loss_sum * grad_scale, (1,))
```

```python
import jax
import jax.numpy as jnp
from jax import lax
from jax.experimental import pallas as pl
from jax.experimental.pallas import tpu as pltpu
from jax.sharding import PartitionSpec as P

GELU_COEF = 0.7978845608028654
CUBIC_COEF = 0.044715

N_MB = 24
TOK = 256
HALF = TOK // 2
DIM = 2560
HID = 5120
HB = 512
N_BLK = HID // HB
GROUP = 4
N_GRP = N_MB // GROUP - 1
GTOK = GROUP * TOK
N_ELEM = N_MB * TOK * DIM
MESH = pl.DeviceIdType.MESH
BF = jnp.bfloat16
F32 = jnp.float32


def dot_nn(a, b):
    return lax.dot_general(a, b, (((1,), (0,)), ((), ())), preferred_element_type=F32)


def dot_nt(a, b):
    return lax.dot_general(a, b, (((1,), (1,)), ((), ())), preferred_element_type=F32)


def dot_tn(a, b):
    return lax.dot_general(a, b, (((0,), (0,)), ((), ())), preferred_element_type=F32)


def gelu(v):
    return 0.5 * v * (1.0 + jnp.tanh(GELU_COEF * (v + CUBIC_COEF * v * v * v)))


def gelu_slope(v):
    t = jnp.tanh(GELU_COEF * (v + CUBIC_COEF * v * v * v))
    return 0.5 * (1.0 + t) + 0.5 * v * (1.0 - t * t) * GELU_COEF * (1.0 + 3.0 * CUBIC_COEF * v * v)


def pipeline_kernel(
    x_in, tgt, w1, w2,
    x_all, e_all, u_all, a_all, g_all, rsf, rsb, acc1, acc2, loss,
    xbuf, w1buf, w2buf, ubuf, abuf, gbuf, uin, accf, accb, rsv, res, tbuf, yf, yb, wide, narrow, wtile,
    w_sem, x_sem, uo_sem, ao_sem, go_sem, ui_sem, p_sem, wd_sem, wn_sem, wl_sem, ws_sem,
    xr_sem, er_sem, rf_sem, rb_sem, sf_sem, sb_sem, yf_sem, yb_sem,
):
    my = lax.axis_index("model")
    st = lax.axis_index("stage")
    other = 1 - my
    last = st == 3
    first = st == 0
    warm = jnp.where(st == 0, 16, jnp.where(st == 1, 12, jnp.where(st == 2, 6, 2)))
    partner = {"model": other}
    nxt = jnp.minimum(st + 1, 3)
    prv = jnp.maximum(st - 1, 0)

    def rows_of(m, half):
        return pl.ds(pl.multiple_of(m * TOK + half * HALF, HALF), HALF)

    def mb_rows(m):
        return pl.ds(pl.multiple_of(m * TOK, TOK), TOK)

    def half_rows(half):
        return pl.ds(pl.multiple_of(half * HALF, HALF), HALF)

    def cols(j, width=HB):
        return pl.ds(pl.multiple_of(j * width, width), width)

    def w_copies(j, slot):
        return (
            pltpu.make_async_copy(w1.at[:, cols(j)], w1buf.at[slot], w_sem.at[slot, 0]),
            pltpu.make_async_copy(w2.at[cols(j), :], w2buf.at[slot], w_sem.at[slot, 1]),
        )

    def rs_copy(acc, slot, buf, m, send, recv):
        return pltpu.make_async_remote_copy(
            src_ref=acc.at[slot, half_rows(other), :],
            dst_ref=buf.at[pl.ds(pl.multiple_of(m * HALF, HALF), HALF), :],
            send_sem=send.at[slot],
            recv_sem=recv.at[m],
            device_id=partner,
            device_id_type=MESH,
        )

    def half_copy(src, slot, dst, m, half, send, k, recv, dev):
        return pltpu.make_async_remote_copy(
            src_ref=src.at[slot],
            dst_ref=dst.at[rows_of(m, half), :],
            send_sem=send.at[slot, k],
            recv_sem=recv.at[m, half],
            device_id=dev,
            device_id_type=MESH,
        )

    def yf_pair(m, slot):
        return (
            half_copy(yf, slot, x_all, m, my, yf_sem, 0, xr_sem, {"model": my, "stage": nxt}),
            half_copy(yf, slot, x_all, m, my, yf_sem, 1, xr_sem, {"model": other, "stage": nxt}),
        )

    def yl_own(m, slot):
        return pltpu.make_async_copy(yf.at[slot], e_all.at[rows_of(m, my), :], er_sem.at[m, my])

    def yl_send(m, slot):
        return half_copy(yf, slot, e_all, m, my, yf_sem, 1, er_sem, partner)

    def yb_pair(m, slot):
        return (
            half_copy(yb, slot, e_all, m, my, yb_sem, 0, er_sem, {"model": my, "stage": prv}),
            half_copy(yb, slot, e_all, m, my, yb_sem, 1, er_sem, {"model": other, "stage": prv}),
        )

    def wait_in(dst, m, recv):
        for half in range(2):
            ref = dst.at[rows_of(m, half), :]
            pltpu.make_async_copy(ref, ref, recv.at[m, half]).wait()

    def out_copy(buf, slot, dst, m, j, sem):
        return pltpu.make_async_copy(buf.at[slot], dst.at[mb_rows(m), cols(j)], sem.at[slot])

    def u_load(m, j, slot):
        return pltpu.make_async_copy(u_all.at[mb_rows(m), cols(j)], uin.at[slot], ui_sem.at[slot])

    def load_x(src, m):
        cp = pltpu.make_async_copy(src.at[mb_rows(m), :], xbuf, x_sem)
        cp.start()
        cp.wait()

    def forward(m):
        slot_m = lax.rem(m, 2)

        @pl.when(first)
        def _():
            load_x(x_in, m)

        @pl.when(jnp.logical_not(first))
        def _():
            wait_in(x_all, m, xr_sem)
            load_x(x_all, m)

        @pl.when(m >= 2)
        def _():
            rs_copy(accf, slot_m, rsf, m - 2, sf_sem, rf_sem).wait_send()

        @pl.loop(0, N_BLK)
        def _(j):
            slot = lax.rem(j, 2)
            for cp in w_copies(j, slot):
                cp.wait()
            for cp in w_copies(lax.rem(j + 1, N_BLK), 1 - slot):
                cp.start()

            @pl.when(m * N_BLK + j >= 2)
            def _():
                out_copy(ubuf, slot, u_all, m, j, uo_sem).wait()
                out_copy(abuf, slot, a_all, m, j, ao_sem).wait()

            ubuf[slot] = dot_nn(xbuf[...], w1buf[slot]).astype(BF)
            abuf[slot] = gelu(ubuf[slot].astype(F32)).astype(BF)
            out_copy(ubuf, slot, u_all, m, j, uo_sem).start()
            out_copy(abuf, slot, a_all, m, j, ao_sem).start()

            @pl.when(j == 0)
            def _():
                accf[slot_m] = jnp.zeros((TOK, DIM), F32)

            accf[slot_m] += dot_nn(abuf[slot], w2buf[slot])

        rs_copy(accf, slot_m, rsf, m, sf_sem, rf_sem).start()

        @pl.when(m == N_MB - 1)
        def _():
            for slot in range(2):
                out_copy(ubuf, slot, u_all, m, slot, uo_sem).wait()
                out_copy(abuf, slot, a_all, m, slot, ao_sem).wait()

    def load_post(acc_buf, m, recv, src):
        ref = acc_buf.at[pl.ds(pl.multiple_of(m * HALF, HALF), HALF), :]
        pltpu.make_async_copy(ref, ref, recv.at[m]).wait()
        a = pltpu.make_async_copy(ref, rsv, p_sem.at[0])
        a.start()
        b = pltpu.make_async_copy(src.at[rows_of(m, my), :], res, p_sem.at[1])
        b.start()
        return a, b

    def forward_post(m):
        slot = lax.rem(m, 2)

        def run(src):
            t = pltpu.make_async_copy(tgt.at[rows_of(m, my), :], tbuf, p_sem.at[2])
            t.start()
            for cp in load_post(rsf, m, rf_sem, src):
                cp.wait()
            t.wait()

        @pl.when(first)
        def _():
            run(x_in)

        @pl.when(jnp.logical_not(first))
        def _():
            run(x_all)

        @pl.when(m >= 2)
        def _():
            @pl.when(last)
            def _():
                yl_send(m, slot).wait_send()

            @pl.when(jnp.logical_not(last))
            def _():
                for cp in yf_pair(m, slot):
                    cp.wait_send()

        y = (res[...].astype(F32) + (accf[slot, half_rows(my), :] + rsv[...])).astype(BF)

        @pl.when(jnp.logical_not(last))
        def _():
            yf[slot] = y
            for cp in yf_pair(m, slot):
                cp.start()

        @pl.when(last)
        def _():
            err = y.astype(F32) - tbuf[...].astype(F32)
            yf[slot] = (err * (1.0 / N_ELEM)).astype(BF)
            sq = err * err
            part = sq[:, 0:128]
            for c in range(1, DIM // 128):
                part = part + sq[:, c * 128 : (c + 1) * 128]
            loss[...] += jnp.sum(part.reshape(HALF // 8, 8, 128), axis=0)
            yl_own(m, slot).start()
            yl_send(m, slot).start()

    def backward(m):
        slot_m = lax.rem(m, 2)
        u_load(m, 0, 0).start()
        wait_in(e_all, m, er_sem)
        load_x(e_all, m)

        @pl.when(jnp.logical_and(m >= 2, jnp.logical_not(first)))
        def _():
            rs_copy(accb, slot_m, rsb, m - 2, sb_sem, rb_sem).wait_send()

        @pl.loop(0, N_BLK)
        def _(j):
            slot = lax.rem(j, 2)
            for cp in w_copies(j, slot):
                cp.wait()
            for cp in w_copies(lax.rem(j + 1, N_BLK), 1 - slot):
                cp.start()
            u_load(m, j, slot).wait()

            @pl.when(j + 1 < N_BLK)
            def _():
                u_load(m, j + 1, 1 - slot).start()

            @pl.when(m * N_BLK + j >= 2)
            def _():
                out_copy(gbuf, slot, g_all, m, j, go_sem).wait()

            q = dot_nt(xbuf[...], w2buf[slot]).astype(BF)
            gbuf[slot] = (gelu_slope(uin[slot].astype(F32)) * q.astype(F32)).astype(BF)
            out_copy(gbuf, slot, g_all, m, j, go_sem).start()

            @pl.when(jnp.logical_not(first))
            def _():
                @pl.when(j == 0)
                def _():
                    accb[slot_m] = jnp.zeros((TOK, DIM), F32)

                accb[slot_m] += dot_nt(gbuf[slot], w1buf[slot])

        @pl.when(jnp.logical_not(first))
        def _():
            rs_copy(accb, slot_m, rsb, m, sb_sem, rb_sem).start()

    def backward_post(m):
        slot = lax.rem(m, 2)
        for cp in load_post(rsb, m, rb_sem, e_all):
            cp.wait()

        @pl.when(m >= 2)
        def _():
            for cp in yb_pair(m, slot):
                cp.wait_send()

        yb[slot] = (res[...].astype(F32) + (accb[slot, half_rows(my), :] + rsv[...])).astype(BF)
        for cp in yb_pair(m, slot):
            cp.start()

    def weight_step(v):
        grp = v // GROUP
        quart = lax.rem(v, GROUP)
        rows = pl.ds(pl.multiple_of(grp * GTOK, GTOK), GTOK)
        out2 = quart < 2

        def on_tile(t, fn2, fn1):
            @pl.when(out2)
            def _():
                fn2(cols(quart * 5 + t))

            @pl.when(jnp.logical_not(out2))
            def _():
                fn1(cols(t), cols(quart - 2, DIM))

        def start_narrow(t, slot):
            def fn2(blk):
                pltpu.make_async_copy(a_all.at[rows, blk], narrow.at[slot], wn_sem.at[slot]).start()

            def fn1(dblk, half):
                @pl.when(first)
                def _():
                    pltpu.make_async_copy(x_in.at[rows, dblk], narrow.at[slot], wn_sem.at[slot]).start()

                @pl.when(jnp.logical_not(first))
                def _():
                    pltpu.make_async_copy(x_all.at[rows, dblk], narrow.at[slot], wn_sem.at[slot]).start()

            on_tile(t, fn2, fn1)

        def start_tile(t, slot):
            def fn2(blk):
                pltpu.make_async_copy(acc2.at[blk, :], wtile.at[slot], wl_sem.at[slot]).start()

            def fn1(dblk, half):
                pltpu.make_async_copy(acc1.at[dblk, half], wtile.at[slot], wl_sem.at[slot]).start()

            on_tile(t, fn2, fn1)

        def start_store(t, slot):
            def fn2(blk):
                pltpu.make_async_copy(wtile.at[slot], acc2.at[blk, :], ws_sem.at[slot]).start()

            def fn1(dblk, half):
                pltpu.make_async_copy(wtile.at[slot], acc1.at[dblk, half], ws_sem.at[slot]).start()

            on_tile(t, fn2, fn1)

        def wait_store(slot):
            pltpu.make_async_copy(wtile.at[slot], acc2.at[pl.ds(0, HB), :], ws_sem.at[slot]).wait()

        @pl.when(out2)
        def _():
            pltpu.make_async_copy(e_all.at[rows, :], wide, wd_sem).start()

        @pl.when(jnp.logical_not(out2))
        def _():
            pltpu.make_async_copy(g_all.at[rows, cols(quart - 2, DIM)], wide, wd_sem).start()

        start_narrow(0, 0)

        @pl.when(grp > 0)
        def _():
            start_tile(0, 0)

        pltpu.make_async_copy(e_all.at[rows, :], wide, wd_sem).wait()

        @pl.loop(0, 5)
        def _(t):
            slot = lax.rem(t, 2)
            pltpu.make_async_copy(a_all.at[rows, pl.ds(0, HB)], narrow.at[slot], wn_sem.at[slot]).wait()

            @pl.when(grp > 0)
            def _():
                pltpu.make_async_copy(acc2.at[pl.ds(0, HB), :], wtile.at[slot], wl_sem.at[slot]).wait()

            @pl.when(t >= 1)
            def _():
                wait_store(1 - slot)

            @pl.when(t < 4)
            def _():
                start_narrow(t + 1, 1 - slot)

                @pl.when(grp > 0)
                def _():
                    start_tile(t + 1, 1 - slot)

            @pl.when(grp == 0)
            def _():
                wtile[slot] = jnp.zeros((HB, DIM), F32)

            wtile[slot] += dot_tn(narrow[slot], wide[...])
            start_store(t, slot)

        wait_store(0)

    loss[...] = jnp.zeros((8, 128), F32)
    for cp in w_copies(0, 0):
        cp.start()

    @pl.loop(0, N_MB + warm)
    def _(k):
        b = k - warm
        p = k - 1
        v = b - GROUP
        b_on = b >= 0
        f_on = k < N_MB
        p_on = jnp.logical_and(p >= 0, p < N_MB)
        pb_on = jnp.logical_and(b_on, jnp.logical_not(first))

        @pl.when(b_on)
        def _():
            backward(b)

        @pl.when(jnp.logical_and(b_on, p_on))
        def _():
            forward_post(p)

        @pl.when(f_on)
        def _():
            forward(k)

        @pl.when(jnp.logical_and(jnp.logical_not(b_on), p_on))
        def _():
            forward_post(p)

        @pl.when(jnp.logical_and(pb_on, f_on))
        def _():
            backward_post(b)

        @pl.when(v >= 0)
        def _():
            weight_step(v)

        @pl.when(jnp.logical_and(pb_on, jnp.logical_not(f_on)))
        def _():
            backward_post(b)

    for cp in w_copies(0, 0):
        cp.wait()
    for m in (N_MB - 2, N_MB - 1):
        slot = m % 2
        out_copy(gbuf, slot, g_all, m, 0, go_sem).wait()
        rs_copy(accf, slot, rsf, m, sf_sem, rf_sem).wait_send()

        @pl.when(jnp.logical_not(first))
        def _():
            rs_copy(accb, slot, rsb, m, sb_sem, rb_sem).wait_send()
            for cp in yb_pair(m, slot):
                cp.wait_send()

        @pl.when(last)
        def _():
            yl_send(m, slot).wait_send()

        @pl.when(jnp.logical_not(last))
        def _():
            for cp in yf_pair(m, slot):
                cp.wait_send()


def run_pipeline(x_in, tgt, w1, w2):
    tokens = N_MB * TOK
    hbm = pl.BlockSpec(memory_space=pl.ANY)
    dma = pltpu.SemaphoreType.DMA
    shapes = [
        ((tokens, DIM), BF), ((tokens, DIM), BF),
        ((tokens, HID), BF), ((tokens, HID), BF), ((tokens, HID), BF),
        ((tokens // 2, DIM), F32), ((tokens // 2, DIM), F32),
        ((DIM, HID), F32), ((HID, DIM), F32),
    ]
    out_shape = [jax.ShapeDtypeStruct(s, d) for s, d in shapes] + [jax.ShapeDtypeStruct((8, 128), F32)]
    return pl.pallas_call(
        pipeline_kernel,
        out_shape=out_shape,
        in_specs=[hbm] * 4,
        out_specs=[hbm] * 9 + [pl.BlockSpec(memory_space=pltpu.VMEM)],
        scratch_shapes=[
            pltpu.VMEM((TOK, DIM), BF),
            pltpu.VMEM((2, DIM, HB), BF),
            pltpu.VMEM((2, HB, DIM), BF),
            pltpu.VMEM((2, TOK, HB), BF),
            pltpu.VMEM((2, TOK, HB), BF),
            pltpu.VMEM((2, TOK, HB), BF),
            pltpu.VMEM((2, TOK, HB), BF),
            pltpu.VMEM((2, TOK, DIM), F32),
            pltpu.VMEM((2, TOK, DIM), F32),
            pltpu.VMEM((HALF, DIM), F32),
            pltpu.VMEM((HALF, DIM), BF),
            pltpu.VMEM((HALF, DIM), BF),
            pltpu.VMEM((2, HALF, DIM), BF),
            pltpu.VMEM((2, HALF, DIM), BF),
            pltpu.VMEM((GTOK, DIM), BF),
            pltpu.VMEM((2, GTOK, HB), BF),
            pltpu.VMEM((2, HB, DIM), F32),
            dma((2, 2)), dma, dma((2,)), dma((2,)), dma((2,)), dma((2,)), dma((3,)), dma, dma((2,)), dma((2,)), dma((2,)),
            dma((N_MB, 2)), dma((N_MB, 2)), dma((N_MB,)), dma((N_MB,)), dma((2,)), dma((2,)), dma((2, 2)), dma((2, 2)),
        ],
        compiler_params=pltpu.CompilerParams(vmem_limit_bytes=66_000_000, has_side_effects=True),
        name="pipeline",
    )(x_in, tgt, w1, w2)


def solution(mesh):
    def stage_step(inputs, targets, w_in, w_out):
        tokens = N_MB * TOK
        x_in = inputs.reshape(tokens, DIM)
        tgt = targets.reshape(tokens, DIM)
        x_all, e_all, _, a_all, g_all, _, _, acc1, acc2, loss = run_pipeline(x_in, tgt, w_in[0, 0], w_out[0, 0])
        tail = slice(N_GRP * GTOK, tokens)
        x_tail = jnp.where(lax.axis_index("stage") == 0, x_in[tail], x_all[tail])
        grad_in = acc1 + dot_tn(x_tail, g_all[tail])
        grad_out = acc2 + dot_tn(a_all[tail], e_all[tail])
        total = lax.psum(jnp.sum(loss), ("model", "stage")) * (0.5 / N_ELEM)
        return grad_in[None, None], grad_out[None, None], jnp.reshape(total, (1,))

    return jax.shard_map(
        stage_step,
        mesh=mesh,
        in_specs=(P("data", None, None), P("data", None, None), P("stage", None, None, "model"), P("stage", None, "model", None)),
        out_specs=(P(("data", "stage"), None, None, "model"), P(("data", "stage"), None, "model", None), P("data")),
        check_vma=False,
    )
```

```python
import jax
import jax.numpy as jnp
from jax import lax
from jax.experimental import pallas as pl
from jax.experimental.pallas import tpu as pltpu
from jax.sharding import PartitionSpec as P

GELU_COEF = 0.7978845608028654
CUBIC_COEF = 0.044715

N_MB = 24
TOK = 256
HALF = TOK // 2
DIM = 2560
HID = 5120
HB = 512
N_BLK = HID // HB
GROUP = 4
N_GRP = N_MB // GROUP - 1
GTOK = GROUP * TOK
N_ELEM = N_MB * TOK * DIM
RELAY0 = 3
MESH = pl.DeviceIdType.MESH
BF = jnp.bfloat16
F32 = jnp.float32


def dot_nn(a, b):
    return lax.dot_general(a, b, (((1,), (0,)), ((), ())), preferred_element_type=F32)


def dot_nt(a, b):
    return lax.dot_general(a, b, (((1,), (1,)), ((), ())), preferred_element_type=F32)


def dot_tn(a, b):
    return lax.dot_general(a, b, (((0,), (0,)), ((), ())), preferred_element_type=F32)


def gelu(v):
    return 0.5 * v * (1.0 + jnp.tanh(GELU_COEF * (v + CUBIC_COEF * v * v * v)))


def gelu_slope(v):
    t = jnp.tanh(GELU_COEF * (v + CUBIC_COEF * v * v * v))
    return 0.5 * (1.0 + t) + 0.5 * v * (1.0 - t * t) * GELU_COEF * (1.0 + 3.0 * CUBIC_COEF * v * v)


def pipeline_kernel(
    x_in, tgt, w1, w2,
    x_all, e_all, u_all, a_all, g_all, rsf, rsb, fwd, acc1, acc2, loss,
    xbuf, w1buf, w2buf, ubuf, abuf, gbuf, uin, accf, accb, rsv, res, tbuf, yf, yb, wide, narrow, wtile, lsum, lrx,
    w_sem, x_sem, uo_sem, ao_sem, go_sem, ui_sem, p_sem, wd_sem, wn_sem, wl_sem, ws_sem,
    xr_sem, er_sem, rf_sem, rb_sem, sf_sem, sb_sem, yf_sem, yb_sem, fr_sem, fs_sem, ls_sem, lr_sem,
):
    my = lax.axis_index("model")
    st = lax.axis_index("stage")
    other = 1 - my
    last = st == 3
    first = st == 0
    warm = jnp.where(st == 0, 16, jnp.where(st == 1, 10, jnp.where(st == 2, 5, 2)))
    partner = {"model": other}
    nxt = jnp.minimum(st + 1, 3)
    prv = jnp.maximum(st - 1, 0)

    def rows_of(m, half):
        return pl.ds(pl.multiple_of(m * TOK + half * HALF, HALF), HALF)

    def mb_rows(m):
        return pl.ds(pl.multiple_of(m * TOK, TOK), TOK)

    def half_rows(half):
        return pl.ds(pl.multiple_of(half * HALF, HALF), HALF)

    def cols(j, width=HB):
        return pl.ds(pl.multiple_of(j * width, width), width)

    def w_copies(j, slot):
        return (
            pltpu.make_async_copy(w1.at[:, cols(j)], w1buf.at[slot], w_sem.at[slot, 0]),
            pltpu.make_async_copy(w2.at[cols(j), :], w2buf.at[slot], w_sem.at[slot, 1]),
        )

    def rs_copy(acc, slot, buf, m, send, recv):
        return pltpu.make_async_remote_copy(
            src_ref=acc.at[slot, half_rows(other), :],
            dst_ref=buf.at[pl.ds(pl.multiple_of(m * HALF, HALF), HALF), :],
            send_sem=send.at[slot],
            recv_sem=recv.at[m],
            device_id=partner,
            device_id_type=MESH,
        )

    def half_copy(src, slot, dst, m, half, send, k, recv, dev):
        return pltpu.make_async_remote_copy(
            src_ref=src.at[slot],
            dst_ref=dst.at[rows_of(m, half), :],
            send_sem=send.at[slot, k],
            recv_sem=recv.at[m, half],
            device_id=dev,
            device_id_type=MESH,
        )

    def yf_pair(m, slot):
        return (
            half_copy(yf, slot, x_all, m, my, yf_sem, 0, xr_sem, {"model": my, "stage": nxt}),
            half_copy(yf, slot, x_all, m, my, yf_sem, 1, xr_sem, {"model": other, "stage": nxt}),
        )

    def fwd_rows(m):
        return pl.ds(pl.multiple_of(m * HALF, HALF), HALF)

    def fwd_send(m, slot):
        return pltpu.make_async_remote_copy(
            src_ref=yf.at[slot],
            dst_ref=fwd.at[fwd_rows(m), :],
            send_sem=yf_sem.at[slot, 1],
            recv_sem=fr_sem.at[m],
            device_id=partner,
            device_id_type=MESH,
        )

    def relay_copy(m):
        return pltpu.make_async_remote_copy(
            src_ref=fwd.at[fwd_rows(m), :],
            dst_ref=x_all.at[rows_of(m, other), :],
            send_sem=fs_sem.at[lax.rem(m, 2)],
            recv_sem=xr_sem.at[m, other],
            device_id={"model": my, "stage": nxt},
            device_id_type=MESH,
        )

    def yl_own(m, slot):
        return pltpu.make_async_copy(yf.at[slot], e_all.at[rows_of(m, my), :], er_sem.at[m, my])

    def yl_send(m, slot):
        return half_copy(yf, slot, e_all, m, my, yf_sem, 1, er_sem, partner)

    def yb_pair(m, slot):
        return (
            half_copy(yb, slot, e_all, m, my, yb_sem, 0, er_sem, {"model": my, "stage": prv}),
            half_copy(yb, slot, e_all, m, my, yb_sem, 1, er_sem, {"model": other, "stage": prv}),
        )

    def wait_in(dst, m, recv):
        for half in range(2):
            ref = dst.at[rows_of(m, half), :]
            pltpu.make_async_copy(ref, ref, recv.at[m, half]).wait()

    def out_copy(buf, slot, dst, m, j, sem):
        return pltpu.make_async_copy(buf.at[slot], dst.at[mb_rows(m), cols(j)], sem.at[slot])

    def u_load(m, j, slot):
        return pltpu.make_async_copy(u_all.at[mb_rows(m), cols(j)], uin.at[slot], ui_sem.at[slot])

    def load_x(src, m):
        cp = pltpu.make_async_copy(src.at[mb_rows(m), :], xbuf, x_sem)
        cp.start()
        cp.wait()

    def forward(m):
        slot_m = lax.rem(m, 2)

        @pl.when(first)
        def _():
            load_x(x_in, m)

            @pl.when(m >= N_GRP * GROUP)
            def _():
                cp = pltpu.make_async_copy(xbuf, x_all.at[mb_rows(m), :], x_sem)
                cp.start()
                cp.wait()

        @pl.when(jnp.logical_not(first))
        def _():
            wait_in(x_all, m, xr_sem)
            load_x(x_all, m)

        @pl.when(m >= 2)
        def _():
            rs_copy(accf, slot_m, rsf, m - 2, sf_sem, rf_sem).wait_send()

        @pl.loop(0, N_BLK)
        def _(j):
            slot = lax.rem(j, 2)
            for cp in w_copies(j, slot):
                cp.wait()
            for cp in w_copies(lax.rem(j + 1, N_BLK), 1 - slot):
                cp.start()

            @pl.when(m * N_BLK + j >= 2)
            def _():
                out_copy(ubuf, slot, u_all, m, j, uo_sem).wait()
                out_copy(abuf, slot, a_all, m, j, ao_sem).wait()

            ubuf[slot] = dot_nn(xbuf[...], w1buf[slot]).astype(BF)
            abuf[slot] = gelu(ubuf[slot].astype(F32)).astype(BF)
            out_copy(ubuf, slot, u_all, m, j, uo_sem).start()
            out_copy(abuf, slot, a_all, m, j, ao_sem).start()

            @pl.when(j == 0)
            def _():
                accf[slot_m] = jnp.zeros((TOK, DIM), F32)

            accf[slot_m] += dot_nn(abuf[slot], w2buf[slot])

        rs_copy(accf, slot_m, rsf, m, sf_sem, rf_sem).start()

        @pl.when(m == N_MB - 1)
        def _():
            for slot in range(2):
                out_copy(ubuf, slot, u_all, m, slot, uo_sem).wait()
                out_copy(abuf, slot, a_all, m, slot, ao_sem).wait()

    def load_post(acc_buf, m, recv, src):
        ref = acc_buf.at[pl.ds(pl.multiple_of(m * HALF, HALF), HALF), :]
        pltpu.make_async_copy(ref, ref, recv.at[m]).wait()
        a = pltpu.make_async_copy(ref, rsv, p_sem.at[0])
        a.start()
        b = pltpu.make_async_copy(src.at[rows_of(m, my), :], res, p_sem.at[1])
        b.start()
        return a, b

    def forward_post(m):
        slot = lax.rem(m, 2)

        def run(src):
            t = pltpu.make_async_copy(tgt.at[rows_of(m, my), :], tbuf, p_sem.at[2])
            t.start()
            for cp in load_post(rsf, m, rf_sem, src):
                cp.wait()
            t.wait()

        @pl.when(first)
        def _():
            run(x_in)

        @pl.when(jnp.logical_not(first))
        def _():
            run(x_all)

        @pl.when(m >= 2)
        def _():
            @pl.when(last)
            def _():
                yl_send(m, slot).wait_send()

            @pl.when(jnp.logical_not(last))
            def _():
                for cp in yf_pair(m, slot):
                    cp.wait_send()

        y = (res[...].astype(F32) + (accf[slot, half_rows(my), :] + rsv[...])).astype(BF)

        @pl.when(jnp.logical_not(last))
        def _():
            yf[slot] = y
            own, cross = yf_pair(m, slot)
            own.start()
            by_pair = jnp.logical_and(st == 1, m >= RELAY0)

            @pl.when(by_pair)
            def _():
                fwd_send(m, slot).start()

            @pl.when(jnp.logical_not(by_pair))
            def _():
                cross.start()

        @pl.when(last)
        def _():
            err = y.astype(F32) - tbuf[...].astype(F32)
            yf[slot] = (err * (1.0 / N_ELEM)).astype(BF)
            sq = err * err
            part = sq[:, 0:128]
            for c in range(1, DIM // 128):
                part = part + sq[:, c * 128 : (c + 1) * 128]
            lsum[...] += jnp.sum(part.reshape(HALF // 8, 8, 128), axis=0)
            yl_own(m, slot).start()
            yl_send(m, slot).start()

            @pl.when(m == N_MB - 1)
            def _():
                pltpu.make_async_copy(lsum, lrx.at[my], lr_sem.at[my]).start()
                for cond, cp in loss_sends():
                    pl.when(cond)(cp.start)

    def relay(m):
        @pl.when(jnp.logical_and(st == 1, jnp.logical_and(m >= RELAY0, m < N_MB)))
        def _():
            ref = fwd.at[fwd_rows(m), :]
            pltpu.make_async_copy(ref, ref, fr_sem.at[m]).wait()

            @pl.when(m >= RELAY0 + 2)
            def _():
                relay_copy(m - 2).wait_send()

            relay_copy(m).start()

    def loss_sends():
        for y in range(2):
            for s in range(4):
                cp = pltpu.make_async_remote_copy(
                    src_ref=lsum,
                    dst_ref=lrx.at[my],
                    send_sem=ls_sem.at[y * 4 + s],
                    recv_sem=lr_sem.at[my],
                    device_id={"model": y, "stage": s},
                    device_id_type=MESH,
                )
                yield (True if s < 3 else my != y), cp

    def backward(m):
        slot_m = lax.rem(m, 2)
        u_load(m, 0, 0).start()
        wait_in(e_all, m, er_sem)
        load_x(e_all, m)

        @pl.when(jnp.logical_and(m >= 2, jnp.logical_not(first)))
        def _():
            rs_copy(accb, slot_m, rsb, m - 2, sb_sem, rb_sem).wait_send()

        @pl.loop(0, N_BLK)
        def _(j):
            slot = lax.rem(j, 2)
            for cp in w_copies(j, slot):
                cp.wait()
            for cp in w_copies(lax.rem(j + 1, N_BLK), 1 - slot):
                cp.start()
            u_load(m, j, slot).wait()

            @pl.when(j + 1 < N_BLK)
            def _():
                u_load(m, j + 1, 1 - slot).start()

            @pl.when(m * N_BLK + j >= 2)
            def _():
                out_copy(gbuf, slot, g_all, m, j, go_sem).wait()

            q = dot_nt(xbuf[...], w2buf[slot]).astype(BF)
            gbuf[slot] = (gelu_slope(uin[slot].astype(F32)) * q.astype(F32)).astype(BF)
            out_copy(gbuf, slot, g_all, m, j, go_sem).start()

            @pl.when(jnp.logical_not(first))
            def _():
                @pl.when(j == 0)
                def _():
                    accb[slot_m] = jnp.zeros((TOK, DIM), F32)

                accb[slot_m] += dot_nt(gbuf[slot], w1buf[slot])

        @pl.when(jnp.logical_not(first))
        def _():
            rs_copy(accb, slot_m, rsb, m, sb_sem, rb_sem).start()

    def backward_post(m):
        slot = lax.rem(m, 2)
        for cp in load_post(rsb, m, rb_sem, e_all):
            cp.wait()

        @pl.when(m >= 2)
        def _():
            for cp in yb_pair(m, slot):
                cp.wait_send()

        yb[slot] = (res[...].astype(F32) + (accb[slot, half_rows(my), :] + rsv[...])).astype(BF)
        for cp in yb_pair(m, slot):
            cp.start()

    def weight_step(v):
        grp = v // GROUP
        quart = lax.rem(v, GROUP)
        rows = pl.ds(pl.multiple_of(grp * GTOK, GTOK), GTOK)
        out2 = quart < 2

        def on_tile(t, fn2, fn1):
            @pl.when(out2)
            def _():
                fn2(cols(quart * 5 + t))

            @pl.when(jnp.logical_not(out2))
            def _():
                fn1(cols(t), cols(quart - 2, DIM))

        def start_narrow(t, slot):
            def fn2(blk):
                pltpu.make_async_copy(a_all.at[rows, blk], narrow.at[slot], wn_sem.at[slot]).start()

            def fn1(dblk, half):
                @pl.when(first)
                def _():
                    pltpu.make_async_copy(x_in.at[rows, dblk], narrow.at[slot], wn_sem.at[slot]).start()

                @pl.when(jnp.logical_not(first))
                def _():
                    pltpu.make_async_copy(x_all.at[rows, dblk], narrow.at[slot], wn_sem.at[slot]).start()

            on_tile(t, fn2, fn1)

        def start_tile(t, slot):
            def fn2(blk):
                pltpu.make_async_copy(acc2.at[blk, :], wtile.at[slot], wl_sem.at[slot]).start()

            def fn1(dblk, half):
                pltpu.make_async_copy(acc1.at[dblk, half], wtile.at[slot], wl_sem.at[slot]).start()

            on_tile(t, fn2, fn1)

        def start_store(t, slot):
            def fn2(blk):
                pltpu.make_async_copy(wtile.at[slot], acc2.at[blk, :], ws_sem.at[slot]).start()

            def fn1(dblk, half):
                pltpu.make_async_copy(wtile.at[slot], acc1.at[dblk, half], ws_sem.at[slot]).start()

            on_tile(t, fn2, fn1)

        def wait_store(slot):
            pltpu.make_async_copy(wtile.at[slot], acc2.at[pl.ds(0, HB), :], ws_sem.at[slot]).wait()

        @pl.when(out2)
        def _():
            pltpu.make_async_copy(e_all.at[rows, :], wide, wd_sem).start()

        @pl.when(jnp.logical_not(out2))
        def _():
            pltpu.make_async_copy(g_all.at[rows, cols(quart - 2, DIM)], wide, wd_sem).start()

        start_narrow(0, 0)

        @pl.when(grp > 0)
        def _():
            start_tile(0, 0)

        pltpu.make_async_copy(e_all.at[rows, :], wide, wd_sem).wait()

        @pl.loop(0, 5)
        def _(t):
            slot = lax.rem(t, 2)
            pltpu.make_async_copy(a_all.at[rows, pl.ds(0, HB)], narrow.at[slot], wn_sem.at[slot]).wait()

            @pl.when(grp > 0)
            def _():
                pltpu.make_async_copy(acc2.at[pl.ds(0, HB), :], wtile.at[slot], wl_sem.at[slot]).wait()

            @pl.when(t >= 1)
            def _():
                wait_store(1 - slot)

            @pl.when(t < 4)
            def _():
                start_narrow(t + 1, 1 - slot)

                @pl.when(grp > 0)
                def _():
                    start_tile(t + 1, 1 - slot)

            @pl.when(grp == 0)
            def _():
                wtile[slot] = jnp.zeros((HB, DIM), F32)

            wtile[slot] += dot_tn(narrow[slot], wide[...])
            start_store(t, slot)

        wait_store(0)

    lsum[...] = jnp.zeros((8, 128), F32)
    for cp in w_copies(0, 0):
        cp.start()

    @pl.loop(0, N_MB + warm)
    def _(k):
        b = k - warm
        p = k - 1
        v = b - GROUP
        b_on = b >= 0
        f_on = k < N_MB
        p_on = jnp.logical_and(p >= 0, p < N_MB)
        pb_on = jnp.logical_and(b_on, jnp.logical_not(first))

        @pl.when(b_on)
        def _():
            backward(b)

        @pl.when(jnp.logical_and(b_on, p_on))
        def _():
            forward_post(p)

        @pl.when(b_on)
        def _():
            relay(k - 2)

        @pl.when(f_on)
        def _():
            forward(k)

        @pl.when(jnp.logical_and(jnp.logical_not(b_on), p_on))
        def _():
            forward_post(p)

        @pl.when(jnp.logical_not(b_on))
        def _():
            relay(k - 2)

        @pl.when(jnp.logical_and(pb_on, f_on))
        def _():
            backward_post(b)

        @pl.when(v >= 0)
        def _():
            weight_step(v)

        @pl.when(jnp.logical_and(pb_on, jnp.logical_not(f_on)))
        def _():
            backward_post(b)

    for half in range(2):
        pltpu.make_async_copy(lsum, lrx.at[half], lr_sem.at[half]).wait()
    loss[...] = lrx[0] + lrx[1]

    for cp in w_copies(0, 0):
        cp.wait()
    for m in (N_MB - 2, N_MB - 1):
        slot = m % 2
        out_copy(gbuf, slot, g_all, m, 0, go_sem).wait()
        rs_copy(accf, slot, rsf, m, sf_sem, rf_sem).wait_send()

        @pl.when(jnp.logical_not(first))
        def _():
            rs_copy(accb, slot, rsb, m, sb_sem, rb_sem).wait_send()
            for cp in yb_pair(m, slot):
                cp.wait_send()

        @pl.when(last)
        def _():
            yl_send(m, slot).wait_send()

        @pl.when(jnp.logical_not(last))
        def _():
            for cp in yf_pair(m, slot):
                cp.wait_send()

        @pl.when(st == 1)
        def _():
            relay_copy(m).wait_send()

    @pl.when(last)
    def _():
        for cond, cp in loss_sends():
            pl.when(cond)(cp.wait_send)


def run_pipeline(x_in, tgt, w1, w2):
    tokens = N_MB * TOK
    hbm = pl.BlockSpec(memory_space=pl.ANY)
    dma = pltpu.SemaphoreType.DMA
    shapes = [
        ((tokens, DIM), BF), ((tokens, DIM), BF),
        ((tokens, HID), BF), ((tokens, HID), BF), ((tokens, HID), BF),
        ((tokens // 2, DIM), F32), ((tokens // 2, DIM), F32), ((tokens // 2, DIM), BF),
        ((DIM, HID), F32), ((HID, DIM), F32),
    ]
    out_shape = [jax.ShapeDtypeStruct(s, d) for s, d in shapes] + [jax.ShapeDtypeStruct((8, 128), F32)]
    return pl.pallas_call(
        pipeline_kernel,
        out_shape=out_shape,
        in_specs=[hbm] * 4,
        out_specs=[hbm] * 10 + [pl.BlockSpec(memory_space=pltpu.VMEM)],
        scratch_shapes=[
            pltpu.VMEM((TOK, DIM), BF),
            pltpu.VMEM((2, DIM, HB), BF),
            pltpu.VMEM((2, HB, DIM), BF),
            pltpu.VMEM((2, TOK, HB), BF),
            pltpu.VMEM((2, TOK, HB), BF),
            pltpu.VMEM((2, TOK, HB), BF),
            pltpu.VMEM((2, TOK, HB), BF),
            pltpu.VMEM((2, TOK, DIM), F32),
            pltpu.VMEM((2, TOK, DIM), F32),
            pltpu.VMEM((HALF, DIM), F32),
            pltpu.VMEM((HALF, DIM), BF),
            pltpu.VMEM((HALF, DIM), BF),
            pltpu.VMEM((2, HALF, DIM), BF),
            pltpu.VMEM((2, HALF, DIM), BF),
            pltpu.VMEM((GTOK, DIM), BF),
            pltpu.VMEM((2, GTOK, HB), BF),
            pltpu.VMEM((2, HB, DIM), F32),
            pltpu.VMEM((8, 128), F32),
            pltpu.VMEM((2, 8, 128), F32),
            dma((2, 2)), dma, dma((2,)), dma((2,)), dma((2,)), dma((2,)), dma((3,)), dma, dma((2,)), dma((2,)), dma((2,)),
            dma((N_MB, 2)), dma((N_MB, 2)), dma((N_MB,)), dma((N_MB,)), dma((2,)), dma((2,)), dma((2, 2)), dma((2, 2)),
            dma((N_MB,)), dma((2,)), dma((8,)), dma((2,)),
        ],
        compiler_params=pltpu.CompilerParams(vmem_limit_bytes=66_000_000, has_side_effects=True),
        name="pipeline",
    )(x_in, tgt, w1, w2)


def add_tail(acc, left, right, n_row_blk, n_col_blk, name):
    rows = TOK

    def body(acc_ref, l_ref, r_ref, o_ref):
        o_ref[...] = acc_ref[...] + dot_tn(l_ref[...], r_ref[...])

    return pl.pallas_call(
        body,
        grid=(n_col_blk, n_row_blk),
        in_specs=[
            pl.BlockSpec((rows, DIM), lambda c, r: (r, c)),
            pl.BlockSpec((GTOK, rows), lambda c, r: (N_GRP, r)),
            pl.BlockSpec((GTOK, DIM), lambda c, r: (N_GRP, c)),
        ],
        out_specs=pl.BlockSpec((rows, DIM), lambda c, r: (r, c)),
        out_shape=jax.ShapeDtypeStruct(acc.shape, F32),
        compiler_params=pltpu.CompilerParams(vmem_limit_bytes=56_000_000),
        name=name,
    )(acc, left, right)


def solution(mesh):
    def stage_step(inputs, targets, w_in, w_out):
        tokens = N_MB * TOK
        x_in = inputs.reshape(tokens, DIM)
        tgt = targets.reshape(tokens, DIM)
        x_all, e_all, _, a_all, g_all, _, _, _, acc1, acc2, loss = run_pipeline(x_in, tgt, w_in[0, 0], w_out[0, 0])
        grad_in = add_tail(acc1, x_all, g_all, DIM // TOK, HID // DIM, "tail_in")
        grad_out = add_tail(acc2, a_all, e_all, HID // TOK, 1, "tail_out")
        total = jnp.sum(loss) * (0.5 / N_ELEM)
        return grad_in[None, None], grad_out[None, None], jnp.reshape(total, (1,))

    return jax.shard_map(
        stage_step,
        mesh=mesh,
        in_specs=(P("data", None, None), P("data", None, None), P("stage", None, None, "model"), P("stage", None, "model", None)),
        out_specs=(P(("data", "stage"), None, None, "model"), P(("data", "stage"), None, "model", None), P("data")),
        check_vma=False,
    )
```

```python
import jax
import jax.numpy as jnp
from jax import lax
from jax.experimental import pallas as pl
from jax.experimental.pallas import tpu as pltpu
from jax.sharding import PartitionSpec as P

GELU_COEF = 0.7978845608028654
CUBIC_COEF = 0.044715

N_MB = 24
TOK = 256
HALF = TOK // 2
DIM = 2560
HID = 5120
HB = 512
N_BLK = HID // HB
W_SLOTS = 3
GROUP = 4
N_GRP = N_MB // GROUP - 1
GTOK = GROUP * TOK
N_ELEM = N_MB * TOK * DIM
RELAY0 = 3
MESH = pl.DeviceIdType.MESH
BF = jnp.bfloat16
F32 = jnp.float32


def dot_nn(a, b):
    return lax.dot_general(a, b, (((1,), (0,)), ((), ())), preferred_element_type=F32)


def dot_nt(a, b):
    return lax.dot_general(a, b, (((1,), (1,)), ((), ())), preferred_element_type=F32)


def dot_tn(a, b):
    return lax.dot_general(a, b, (((0,), (0,)), ((), ())), preferred_element_type=F32)


def gelu(v):
    return 0.5 * v * (1.0 + jnp.tanh(GELU_COEF * (v + CUBIC_COEF * v * v * v)))


def gelu_slope(v):
    t = jnp.tanh(GELU_COEF * (v + CUBIC_COEF * v * v * v))
    return 0.5 * (1.0 + t) + 0.5 * v * (1.0 - t * t) * GELU_COEF * (1.0 + 3.0 * CUBIC_COEF * v * v)


def pipeline_kernel(
    x_in, tgt, w1, w2,
    x_all, e_all, u_all, a_all, g_all, rsf, rsb, fwd, acc1, acc2, loss,
    xbuf, w1buf, w2buf, ubuf, abuf, gbuf, uin, accf, accb, rsv, res, tbuf, yf, yb, wide, narrow, wtile, lsum, lrx,
    w_sem, x_sem, uo_sem, ao_sem, go_sem, ui_sem, p_sem, wd_sem, wn_sem, wl_sem, ws_sem,
    xr_sem, er_sem, rf_sem, rb_sem, sf_sem, sb_sem, yf_sem, yb_sem, fr_sem, fs_sem, ls_sem, lr_sem,
):
    my = lax.axis_index("model")
    st = lax.axis_index("stage")
    other = 1 - my
    last = st == 3
    first = st == 0
    warm = jnp.where(st == 0, 16, jnp.where(st == 1, 10, jnp.where(st == 2, 5, 2)))
    partner = {"model": other}
    nxt = jnp.minimum(st + 1, 3)
    prv = jnp.maximum(st - 1, 0)

    def rows_of(m, half):
        return pl.ds(pl.multiple_of(m * TOK + half * HALF, HALF), HALF)

    def mb_rows(m):
        return pl.ds(pl.multiple_of(m * TOK, TOK), TOK)

    def half_rows(half):
        return pl.ds(pl.multiple_of(half * HALF, HALF), HALF)

    def cols(j, width=HB):
        return pl.ds(pl.multiple_of(j * width, width), width)

    def w_copies(j, slot):
        return (
            pltpu.make_async_copy(w1.at[:, cols(j)], w1buf.at[slot], w_sem.at[slot, 0]),
            pltpu.make_async_copy(w2.at[cols(j), :], w2buf.at[slot], w_sem.at[slot, 1]),
        )

    def rs_copy(acc, slot, buf, m, send, recv):
        return pltpu.make_async_remote_copy(
            src_ref=acc.at[slot, half_rows(other), :],
            dst_ref=buf.at[pl.ds(pl.multiple_of(m * HALF, HALF), HALF), :],
            send_sem=send.at[slot],
            recv_sem=recv.at[m],
            device_id=partner,
            device_id_type=MESH,
        )

    def half_copy(src, slot, dst, m, half, send, k, recv, dev):
        return pltpu.make_async_remote_copy(
            src_ref=src.at[slot],
            dst_ref=dst.at[rows_of(m, half), :],
            send_sem=send.at[slot, k],
            recv_sem=recv.at[m, half],
            device_id=dev,
            device_id_type=MESH,
        )

    def yf_pair(m, slot):
        return (
            half_copy(yf, slot, x_all, m, my, yf_sem, 0, xr_sem, {"model": my, "stage": nxt}),
            half_copy(yf, slot, x_all, m, my, yf_sem, 1, xr_sem, {"model": other, "stage": nxt}),
        )

    def fwd_rows(m):
        return pl.ds(pl.multiple_of(m * HALF, HALF), HALF)

    def fwd_send(m, slot):
        return pltpu.make_async_remote_copy(
            src_ref=yf.at[slot],
            dst_ref=fwd.at[fwd_rows(m), :],
            send_sem=yf_sem.at[slot, 1],
            recv_sem=fr_sem.at[m],
            device_id=partner,
            device_id_type=MESH,
        )

    def relay_copy(m):
        return pltpu.make_async_remote_copy(
            src_ref=fwd.at[fwd_rows(m), :],
            dst_ref=x_all.at[rows_of(m, other), :],
            send_sem=fs_sem.at[lax.rem(m, 2)],
            recv_sem=xr_sem.at[m, other],
            device_id={"model": my, "stage": nxt},
            device_id_type=MESH,
        )

    def yl_own(m, slot):
        return pltpu.make_async_copy(yf.at[slot], e_all.at[rows_of(m, my), :], er_sem.at[m, my])

    def yl_send(m, slot):
        return half_copy(yf, slot, e_all, m, my, yf_sem, 1, er_sem, partner)

    def yb_pair(m, slot):
        return (
            half_copy(yb, slot, e_all, m, my, yb_sem, 0, er_sem, {"model": my, "stage": prv}),
            half_copy(yb, slot, e_all, m, my, yb_sem, 1, er_sem, {"model": other, "stage": prv}),
        )

    def wait_in(dst, m, recv):
        for half in range(2):
            ref = dst.at[rows_of(m, half), :]
            pltpu.make_async_copy(ref, ref, recv.at[m, half]).wait()

    def out_copy(buf, slot, dst, m, j, sem):
        return pltpu.make_async_copy(buf.at[slot], dst.at[mb_rows(m), cols(j)], sem.at[slot])

    def u_load(m, j, slot):
        return pltpu.make_async_copy(u_all.at[mb_rows(m), cols(j)], uin.at[slot], ui_sem.at[slot])

    def load_x(src, m):
        cp = pltpu.make_async_copy(src.at[mb_rows(m), :], xbuf, x_sem)
        cp.start()
        cp.wait()

    def next_weights(count, j):
        at = count * N_BLK + j
        slot = lax.rem(at, W_SLOTS)
        for cp in w_copies(j, slot):
            cp.wait()
        ahead = W_SLOTS - 1
        for cp in w_copies(lax.rem(j + ahead, N_BLK), lax.rem(at + ahead, W_SLOTS)):
            cp.start()
        return slot

    def forward(m, count):
        slot_m = lax.rem(m, 2)

        @pl.when(first)
        def _():
            load_x(x_in, m)

            @pl.when(m >= N_GRP * GROUP)
            def _():
                cp = pltpu.make_async_copy(xbuf, x_all.at[mb_rows(m), :], x_sem)
                cp.start()
                cp.wait()

        @pl.when(jnp.logical_not(first))
        def _():
            wait_in(x_all, m, xr_sem)
            load_x(x_all, m)

        @pl.when(m >= 2)
        def _():
            rs_copy(accf, slot_m, rsf, m - 2, sf_sem, rf_sem).wait_send()

        @pl.loop(0, N_BLK)
        def _(j):
            slot = lax.rem(j, 2)
            ws = next_weights(count, j)

            @pl.when(m * N_BLK + j >= 2)
            def _():
                out_copy(ubuf, slot, u_all, m, j, uo_sem).wait()
                out_copy(abuf, slot, a_all, m, j, ao_sem).wait()

            ubuf[slot] = dot_nn(xbuf[...], w1buf[ws]).astype(BF)
            abuf[slot] = gelu(ubuf[slot].astype(F32)).astype(BF)
            out_copy(ubuf, slot, u_all, m, j, uo_sem).start()
            out_copy(abuf, slot, a_all, m, j, ao_sem).start()

            @pl.when(j == 0)
            def _():
                accf[slot_m] = jnp.zeros((TOK, DIM), F32)

            accf[slot_m] += dot_nn(abuf[slot], w2buf[ws])

        rs_copy(accf, slot_m, rsf, m, sf_sem, rf_sem).start()

        @pl.when(m == N_MB - 1)
        def _():
            for slot in range(2):
                out_copy(ubuf, slot, u_all, m, slot, uo_sem).wait()
                out_copy(abuf, slot, a_all, m, slot, ao_sem).wait()

    def load_post(acc_buf, m, recv, src):
        ref = acc_buf.at[pl.ds(pl.multiple_of(m * HALF, HALF), HALF), :]
        pltpu.make_async_copy(ref, ref, recv.at[m]).wait()
        a = pltpu.make_async_copy(ref, rsv, p_sem.at[0])
        a.start()
        b = pltpu.make_async_copy(src.at[rows_of(m, my), :], res, p_sem.at[1])
        b.start()
        return a, b

    def forward_post(m):
        slot = lax.rem(m, 2)

        def run(src):
            t = pltpu.make_async_copy(tgt.at[rows_of(m, my), :], tbuf, p_sem.at[2])
            t.start()
            for cp in load_post(rsf, m, rf_sem, src):
                cp.wait()
            t.wait()

        @pl.when(first)
        def _():
            run(x_in)

        @pl.when(jnp.logical_not(first))
        def _():
            run(x_all)

        @pl.when(m >= 2)
        def _():
            @pl.when(last)
            def _():
                yl_send(m, slot).wait_send()

            @pl.when(jnp.logical_not(last))
            def _():
                for cp in yf_pair(m, slot):
                    cp.wait_send()

        y = (res[...].astype(F32) + (accf[slot, half_rows(my), :] + rsv[...])).astype(BF)

        @pl.when(jnp.logical_not(last))
        def _():
            yf[slot] = y
            own, cross = yf_pair(m, slot)
            own.start()
            by_pair = jnp.logical_and(st == 1, m >= RELAY0)

            @pl.when(by_pair)
            def _():
                fwd_send(m, slot).start()

            @pl.when(jnp.logical_not(by_pair))
            def _():
                cross.start()

        @pl.when(last)
        def _():
            err = y.astype(F32) - tbuf[...].astype(F32)
            yf[slot] = (err * (1.0 / N_ELEM)).astype(BF)
            sq = err * err
            part = sq[:, 0:128]
            for c in range(1, DIM // 128):
                part = part + sq[:, c * 128 : (c + 1) * 128]
            lsum[...] += jnp.sum(part.reshape(HALF // 8, 8, 128), axis=0)
            yl_own(m, slot).start()
            yl_send(m, slot).start()

            @pl.when(m == N_MB - 1)
            def _():
                pltpu.make_async_copy(lsum, lrx.at[my], lr_sem.at[my]).start()
                for cond, cp in loss_sends():
                    pl.when(cond)(cp.start)

    def relay(m):
        @pl.when(jnp.logical_and(st == 1, jnp.logical_and(m >= RELAY0, m < N_MB)))
        def _():
            ref = fwd.at[fwd_rows(m), :]
            pltpu.make_async_copy(ref, ref, fr_sem.at[m]).wait()

            @pl.when(m >= RELAY0 + 2)
            def _():
                relay_copy(m - 2).wait_send()

            relay_copy(m).start()

    def loss_sends():
        for y in range(2):
            for s in range(4):
                cp = pltpu.make_async_remote_copy(
                    src_ref=lsum,
                    dst_ref=lrx.at[my],
                    send_sem=ls_sem.at[y * 4 + s],
                    recv_sem=lr_sem.at[my],
                    device_id={"model": y, "stage": s},
                    device_id_type=MESH,
                )
                yield (True if s < 3 else my != y), cp

    def backward(m, count):
        slot_m = lax.rem(m, 2)
        u_load(m, 0, 0).start()
        wait_in(e_all, m, er_sem)
        load_x(e_all, m)

        @pl.when(jnp.logical_and(m >= 2, jnp.logical_not(first)))
        def _():
            rs_copy(accb, slot_m, rsb, m - 2, sb_sem, rb_sem).wait_send()

        @pl.loop(0, N_BLK)
        def _(j):
            slot = lax.rem(j, 2)
            ws = next_weights(count, j)
            u_load(m, j, slot).wait()

            @pl.when(j + 1 < N_BLK)
            def _():
                u_load(m, j + 1, 1 - slot).start()

            @pl.when(m * N_BLK + j >= 2)
            def _():
                out_copy(gbuf, slot, g_all, m, j, go_sem).wait()

            q = dot_nt(xbuf[...], w2buf[ws]).astype(BF)
            gbuf[slot] = (gelu_slope(uin[slot].astype(F32)) * q.astype(F32)).astype(BF)
            out_copy(gbuf, slot, g_all, m, j, go_sem).start()

            @pl.when(jnp.logical_not(first))
            def _():
                @pl.when(j == 0)
                def _():
                    accb[slot_m] = jnp.zeros((TOK, DIM), F32)

                accb[slot_m] += dot_nt(gbuf[slot], w1buf[ws])

        @pl.when(jnp.logical_not(first))
        def _():
            rs_copy(accb, slot_m, rsb, m, sb_sem, rb_sem).start()

    def backward_post(m):
        slot = lax.rem(m, 2)
        for cp in load_post(rsb, m, rb_sem, e_all):
            cp.wait()

        @pl.when(m >= 2)
        def _():
            for cp in yb_pair(m, slot):
                cp.wait_send()

        yb[slot] = (res[...].astype(F32) + (accb[slot, half_rows(my), :] + rsv[...])).astype(BF)
        for cp in yb_pair(m, slot):
            cp.start()

    def weight_ops(v):
        grp = v // GROUP
        quart = lax.rem(v, GROUP)
        rows = pl.ds(pl.multiple_of(grp * GTOK, GTOK), GTOK)
        out2 = quart < 2

        def on_tile(t, fn2, fn1):
            @pl.when(out2)
            def _():
                fn2(cols(quart * 5 + t))

            @pl.when(jnp.logical_not(out2))
            def _():
                fn1(cols(t), cols(quart - 2, DIM))

        def start_tile(t):
            n_slot = lax.rem(t, 2)
            slot = lax.rem(t, 3)

            def fn2(blk):
                pltpu.make_async_copy(a_all.at[rows, blk], narrow.at[n_slot], wn_sem.at[n_slot]).start()

                @pl.when(grp > 0)
                def _():
                    pltpu.make_async_copy(acc2.at[blk, :], wtile.at[slot], wl_sem.at[slot]).start()

            def fn1(dblk, half):
                @pl.when(first)
                def _():
                    pltpu.make_async_copy(x_in.at[rows, dblk], narrow.at[n_slot], wn_sem.at[n_slot]).start()

                @pl.when(jnp.logical_not(first))
                def _():
                    pltpu.make_async_copy(x_all.at[rows, dblk], narrow.at[n_slot], wn_sem.at[n_slot]).start()

                @pl.when(grp > 0)
                def _():
                    pltpu.make_async_copy(acc1.at[dblk, half], wtile.at[slot], wl_sem.at[slot]).start()

            on_tile(t, fn2, fn1)

        def start_store(t):
            slot = lax.rem(t, 3)

            def fn2(blk):
                pltpu.make_async_copy(wtile.at[slot], acc2.at[blk, :], ws_sem.at[slot]).start()

            def fn1(dblk, half):
                pltpu.make_async_copy(wtile.at[slot], acc1.at[dblk, half], ws_sem.at[slot]).start()

            on_tile(t, fn2, fn1)

        def wait_store(slot):
            pltpu.make_async_copy(wtile.at[slot], acc2.at[pl.ds(0, HB), :], ws_sem.at[slot]).wait()

        def start():
            @pl.when(out2)
            def _():
                pltpu.make_async_copy(e_all.at[rows, :], wide, wd_sem).start()

            @pl.when(jnp.logical_not(out2))
            def _():
                pltpu.make_async_copy(g_all.at[rows, cols(quart - 2, DIM)], wide, wd_sem).start()

            start_tile(0)

        def run():
            pltpu.make_async_copy(e_all.at[rows, :], wide, wd_sem).wait()

            @pl.loop(0, 5)
            def _(t):
                slot = lax.rem(t, 3)
                n_slot = lax.rem(t, 2)

                @pl.when(t >= 2)
                def _():
                    wait_store(lax.rem(t + 1, 3))

                @pl.when(t < 4)
                def _():
                    start_tile(t + 1)

                pltpu.make_async_copy(a_all.at[rows, pl.ds(0, HB)], narrow.at[n_slot], wn_sem.at[n_slot]).wait()

                @pl.when(grp > 0)
                def _():
                    pltpu.make_async_copy(acc2.at[pl.ds(0, HB), :], wtile.at[slot], wl_sem.at[slot]).wait()

                @pl.when(grp == 0)
                def _():
                    wtile[slot] = jnp.zeros((HB, DIM), F32)

                wtile[slot] += dot_tn(narrow[n_slot], wide[...])
                start_store(t)

            wait_store(0)
            wait_store(1)

        return start, run

    lsum[...] = jnp.zeros((8, 128), F32)
    for j in range(W_SLOTS - 1):
        for cp in w_copies(j, j):
            cp.start()

    @pl.loop(0, N_MB + warm)
    def _(k):
        b = k - warm
        p = k - 1
        v = b - GROUP
        b_on = b >= 0
        f_on = k < N_MB
        p_on = jnp.logical_and(p >= 0, p < N_MB)
        pb_on = jnp.logical_and(b_on, jnp.logical_not(first))

        @pl.when(b_on)
        def _():
            backward(b, b + jnp.minimum(k, N_MB))

        @pl.when(jnp.logical_and(b_on, p_on))
        def _():
            forward_post(p)

        @pl.when(b_on)
        def _():
            relay(k - 2)

        @pl.when(v >= 0)
        def _():
            weight_ops(v)[0]()

        @pl.when(f_on)
        def _():
            forward(k, k + jnp.maximum(b + 1, 0))

        @pl.when(jnp.logical_and(jnp.logical_not(b_on), p_on))
        def _():
            forward_post(p)

        @pl.when(jnp.logical_not(b_on))
        def _():
            relay(k - 2)

        @pl.when(jnp.logical_and(pb_on, f_on))
        def _():
            backward_post(b)

        @pl.when(v >= 0)
        def _():
            weight_ops(v)[1]()

        @pl.when(jnp.logical_and(pb_on, jnp.logical_not(f_on)))
        def _():
            backward_post(b)

    for half in range(2):
        pltpu.make_async_copy(lsum, lrx.at[half], lr_sem.at[half]).wait()
    loss[...] = lrx[0] + lrx[1]

    for j in range(W_SLOTS - 1):
        for cp in w_copies(j, (2 * N_MB * N_BLK + j) % W_SLOTS):
            cp.wait()
    for m in (N_MB - 2, N_MB - 1):
        slot = m % 2
        out_copy(gbuf, slot, g_all, m, 0, go_sem).wait()
        rs_copy(accf, slot, rsf, m, sf_sem, rf_sem).wait_send()

        @pl.when(jnp.logical_not(first))
        def _():
            rs_copy(accb, slot, rsb, m, sb_sem, rb_sem).wait_send()
            for cp in yb_pair(m, slot):
                cp.wait_send()

        @pl.when(last)
        def _():
            yl_send(m, slot).wait_send()

        @pl.when(jnp.logical_not(last))
        def _():
            for cp in yf_pair(m, slot):
                cp.wait_send()

        @pl.when(st == 1)
        def _():
            relay_copy(m).wait_send()

    @pl.when(last)
    def _():
        for cond, cp in loss_sends():
            pl.when(cond)(cp.wait_send)


def run_pipeline(x_in, tgt, w1, w2):
    tokens = N_MB * TOK
    hbm = pl.BlockSpec(memory_space=pl.ANY)
    dma = pltpu.SemaphoreType.DMA
    shapes = [
        ((tokens, DIM), BF), ((tokens, DIM), BF),
        ((tokens, HID), BF), ((tokens, HID), BF), ((tokens, HID), BF),
        ((tokens // 2, DIM), F32), ((tokens // 2, DIM), F32), ((tokens // 2, DIM), BF),
        ((DIM, HID), F32), ((HID, DIM), F32),
    ]
    out_shape = [jax.ShapeDtypeStruct(s, d) for s, d in shapes] + [jax.ShapeDtypeStruct((8, 128), F32)]
    return pl.pallas_call(
        pipeline_kernel,
        out_shape=out_shape,
        in_specs=[hbm] * 4,
        out_specs=[hbm] * 10 + [pl.BlockSpec(memory_space=pltpu.VMEM)],
        scratch_shapes=[
            pltpu.VMEM((TOK, DIM), BF),
            pltpu.VMEM((W_SLOTS, DIM, HB), BF),
            pltpu.VMEM((W_SLOTS, HB, DIM), BF),
            pltpu.VMEM((2, TOK, HB), BF),
            pltpu.VMEM((2, TOK, HB), BF),
            pltpu.VMEM((2, TOK, HB), BF),
            pltpu.VMEM((2, TOK, HB), BF),
            pltpu.VMEM((2, TOK, DIM), F32),
            pltpu.VMEM((2, TOK, DIM), F32),
            pltpu.VMEM((HALF, DIM), F32),
            pltpu.VMEM((HALF, DIM), BF),
            pltpu.VMEM((HALF, DIM), BF),
            pltpu.VMEM((2, HALF, DIM), BF),
            pltpu.VMEM((2, HALF, DIM), BF),
            pltpu.VMEM((GTOK, DIM), BF),
            pltpu.VMEM((2, GTOK, HB), BF),
            pltpu.VMEM((3, HB, DIM), F32),
            pltpu.VMEM((8, 128), F32),
            pltpu.VMEM((2, 8, 128), F32),
            dma((W_SLOTS, 2)), dma, dma((2,)), dma((2,)), dma((2,)), dma((2,)), dma((3,)), dma, dma((2,)), dma((3,)), dma((3,)),
            dma((N_MB, 2)), dma((N_MB, 2)), dma((N_MB,)), dma((N_MB,)), dma((2,)), dma((2,)), dma((2, 2)), dma((2, 2)),
            dma((N_MB,)), dma((2,)), dma((8,)), dma((2,)),
        ],
        compiler_params=pltpu.CompilerParams(vmem_limit_bytes=66_000_000, has_side_effects=True),
        name="pipeline",
    )(x_in, tgt, w1, w2)


def add_tail(acc, left, right, n_row_blk, n_col_blk, name):
    rows = HB

    def body(acc_ref, l_ref, r_ref, o_ref):
        o_ref[...] = acc_ref[...] + dot_tn(l_ref[...], r_ref[...])

    return pl.pallas_call(
        body,
        grid=(n_col_blk, n_row_blk),
        in_specs=[
            pl.BlockSpec((rows, DIM), lambda c, r: (r, c)),
            pl.BlockSpec((GTOK, rows), lambda c, r: (N_GRP, r)),
            pl.BlockSpec((GTOK, DIM), lambda c, r: (N_GRP, c)),
        ],
        out_specs=pl.BlockSpec((rows, DIM), lambda c, r: (r, c)),
        out_shape=jax.ShapeDtypeStruct(acc.shape, F32),
        compiler_params=pltpu.CompilerParams(vmem_limit_bytes=56_000_000),
        name=name,
    )(acc, left, right)


def solution(mesh):
    def stage_step(inputs, targets, w_in, w_out):
        tokens = N_MB * TOK
        x_in = inputs.reshape(tokens, DIM)
        tgt = targets.reshape(tokens, DIM)
        x_all, e_all, _, a_all, g_all, _, _, _, acc1, acc2, loss = run_pipeline(x_in, tgt, w_in[0, 0], w_out[0, 0])
        grad_in = add_tail(acc1, x_all, g_all, DIM // HB, HID // DIM, "tail_in")
        grad_out = add_tail(acc2, a_all, e_all, HID // HB, 1, "tail_out")
        total = jnp.sum(loss) * (0.5 / N_ELEM)
        return grad_in[None, None], grad_out[None, None], jnp.reshape(total, (1,))

    return jax.shard_map(
        stage_step,
        mesh=mesh,
        in_specs=(P("data", None, None), P("data", None, None), P("stage", None, None, "model"), P("stage", None, "model", None)),
        out_specs=(P(("data", "stage"), None, None, "model"), P(("data", "stage"), None, "model", None), P("data")),
        check_vma=False,
    )
```

```python
import jax
import jax.numpy as jnp
from jax import lax
from jax.experimental import pallas as pl
from jax.experimental.pallas import tpu as pltpu
from jax.sharding import PartitionSpec as P

GELU_COEF = 0.7978845608028654
CUBIC_COEF = 0.044715

N_MB = 24
TOK = 256
HALF = TOK // 2
DIM = 2560
HID = 5120
HB = 512
N_BLK = HID // HB
W_SLOTS = 3
GROUP = 4
N_GRP = N_MB // GROUP - 1
GTOK = GROUP * TOK
N_ELEM = N_MB * TOK * DIM
RELAY0 = 3
RELAY3 = 10
LEAD3 = 3
MESH = pl.DeviceIdType.MESH
BF = jnp.bfloat16
F32 = jnp.float32


def dot_nn(a, b):
    return lax.dot_general(a, b, (((1,), (0,)), ((), ())), preferred_element_type=F32)


def dot_nt(a, b):
    return lax.dot_general(a, b, (((1,), (1,)), ((), ())), preferred_element_type=F32)


def dot_tn(a, b):
    return lax.dot_general(a, b, (((0,), (0,)), ((), ())), preferred_element_type=F32)


def gelu(v):
    return 0.5 * v * (1.0 + jnp.tanh(GELU_COEF * (v + CUBIC_COEF * v * v * v)))


def gelu_slope(v):
    t = jnp.tanh(GELU_COEF * (v + CUBIC_COEF * v * v * v))
    return 0.5 * (1.0 + t) + 0.5 * v * (1.0 - t * t) * GELU_COEF * (1.0 + 3.0 * CUBIC_COEF * v * v)


def pipeline_kernel(
    x_in, tgt, w1, w2,
    x_all, e_all, u_all, a_all, g_all, rsf, rsb, fwd, acc1, acc2, loss,
    xbuf, w1buf, w2buf, ubuf, abuf, gbuf, uin, accf, accb, rsv, res, tbuf, yf, yb, wide, narrow, wtile, lsum, lrx,
    w_sem, x_sem, uo_sem, ao_sem, go_sem, ui_sem, p_sem, wd_sem, wn_sem, wl_sem, ws_sem,
    xr_sem, er_sem, rf_sem, rb_sem, sf_sem, sb_sem, yf_sem, yb_sem, fr_sem, fs_sem, ls_sem, lr_sem,
):
    my = lax.axis_index("model")
    st = lax.axis_index("stage")
    other = 1 - my
    last = st == 3
    first = st == 0
    warm = jnp.where(st == 0, 16, jnp.where(st == 1, 10, jnp.where(st == 2, 5, 2)))
    partner = {"model": other}
    nxt = jnp.minimum(st + 1, 3)
    prv = jnp.maximum(st - 1, 0)

    def rows_of(m, half):
        return pl.ds(pl.multiple_of(m * TOK + half * HALF, HALF), HALF)

    def mb_rows(m):
        return pl.ds(pl.multiple_of(m * TOK, TOK), TOK)

    def half_rows(half):
        return pl.ds(pl.multiple_of(half * HALF, HALF), HALF)

    def cols(j, width=HB):
        return pl.ds(pl.multiple_of(j * width, width), width)

    def w_copies(j, slot):
        return (
            pltpu.make_async_copy(w1.at[:, cols(j)], w1buf.at[slot], w_sem.at[slot, 0]),
            pltpu.make_async_copy(w2.at[cols(j), :], w2buf.at[slot], w_sem.at[slot, 1]),
        )

    def rs_copy(acc, slot, buf, m, send, recv):
        return pltpu.make_async_remote_copy(
            src_ref=acc.at[slot, half_rows(other), :],
            dst_ref=buf.at[pl.ds(pl.multiple_of(m * HALF, HALF), HALF), :],
            send_sem=send.at[slot],
            recv_sem=recv.at[m],
            device_id=partner,
            device_id_type=MESH,
        )

    def half_copy(src, slot, dst, m, half, send, k, recv, dev):
        return pltpu.make_async_remote_copy(
            src_ref=src.at[slot],
            dst_ref=dst.at[rows_of(m, half), :],
            send_sem=send.at[slot, k],
            recv_sem=recv.at[m, half],
            device_id=dev,
            device_id_type=MESH,
        )

    def yf_pair(m, slot):
        return (
            half_copy(yf, slot, x_all, m, my, yf_sem, 0, xr_sem, {"model": my, "stage": nxt}),
            half_copy(yf, slot, x_all, m, my, yf_sem, 1, xr_sem, {"model": other, "stage": nxt}),
        )

    def fwd_rows(m):
        return pl.ds(pl.multiple_of(m * HALF, HALF), HALF)

    def fwd_send(m, slot):
        return pltpu.make_async_remote_copy(
            src_ref=yf.at[slot],
            dst_ref=fwd.at[fwd_rows(m), :],
            send_sem=yf_sem.at[slot, 1],
            recv_sem=fr_sem.at[m],
            device_id=partner,
            device_id_type=MESH,
        )

    def relay_copy(m, dst, recv, to):
        return pltpu.make_async_remote_copy(
            src_ref=fwd.at[fwd_rows(m), :],
            dst_ref=dst.at[rows_of(m, other), :],
            send_sem=fs_sem.at[lax.rem(m, 2)],
            recv_sem=recv.at[m, other],
            device_id={"model": my, "stage": to},
            device_id_type=MESH,
        )

    def relay_x(m):
        return relay_copy(m, x_all, xr_sem, 2)

    def relay_e(m):
        return relay_copy(m, e_all, er_sem, 2)

    def far_send(m, slot):
        return pltpu.make_async_remote_copy(
            src_ref=yb.at[slot],
            dst_ref=fwd.at[fwd_rows(m), :],
            send_sem=yb_sem.at[slot, 1],
            recv_sem=fr_sem.at[m],
            device_id={"model": other, "stage": 0},
            device_id_type=MESH,
        )

    def yl_own(m, slot):
        return pltpu.make_async_copy(yf.at[slot], e_all.at[rows_of(m, my), :], er_sem.at[m, my])

    def yl_send(m, slot):
        return half_copy(yf, slot, e_all, m, my, yf_sem, 1, er_sem, partner)

    def yb_pair(m, slot):
        return (
            half_copy(yb, slot, e_all, m, my, yb_sem, 0, er_sem, {"model": my, "stage": prv}),
            half_copy(yb, slot, e_all, m, my, yb_sem, 1, er_sem, {"model": other, "stage": prv}),
        )

    def wait_in(dst, m, recv):
        for half in range(2):
            ref = dst.at[rows_of(m, half), :]
            pltpu.make_async_copy(ref, ref, recv.at[m, half]).wait()

    def out_copy(buf, slot, dst, m, j, sem):
        return pltpu.make_async_copy(buf.at[slot], dst.at[mb_rows(m), cols(j)], sem.at[slot])

    def u_load(m, j, slot):
        return pltpu.make_async_copy(u_all.at[mb_rows(m), cols(j)], uin.at[slot], ui_sem.at[slot])

    def load_x(src, m):
        cp = pltpu.make_async_copy(src.at[mb_rows(m), :], xbuf, x_sem)
        cp.start()
        cp.wait()

    def next_weights(count, j):
        at = count * N_BLK + j
        slot = lax.rem(at, W_SLOTS)
        for cp in w_copies(j, slot):
            cp.wait()
        ahead = W_SLOTS - 1
        for cp in w_copies(lax.rem(j + ahead, N_BLK), lax.rem(at + ahead, W_SLOTS)):
            cp.start()
        return slot

    def forward(m, count):
        slot_m = lax.rem(m, 2)

        @pl.when(first)
        def _():
            load_x(x_in, m)

            @pl.when(m >= N_GRP * GROUP)
            def _():
                cp = pltpu.make_async_copy(xbuf, x_all.at[mb_rows(m), :], x_sem)
                cp.start()
                cp.wait()

        @pl.when(jnp.logical_not(first))
        def _():
            wait_in(x_all, m, xr_sem)
            load_x(x_all, m)

        @pl.when(m >= 2)
        def _():
            rs_copy(accf, slot_m, rsf, m - 2, sf_sem, rf_sem).wait_send()

        @pl.loop(0, N_BLK)
        def _(j):
            slot = lax.rem(j, 2)
            ws = next_weights(count, j)

            @pl.when(m * N_BLK + j >= 2)
            def _():
                out_copy(ubuf, slot, u_all, m, j, uo_sem).wait()
                out_copy(abuf, slot, a_all, m, j, ao_sem).wait()

            ubuf[slot] = dot_nn(xbuf[...], w1buf[ws]).astype(BF)
            abuf[slot] = gelu(ubuf[slot].astype(F32)).astype(BF)
            out_copy(ubuf, slot, u_all, m, j, uo_sem).start()
            out_copy(abuf, slot, a_all, m, j, ao_sem).start()

            @pl.when(j == 0)
            def _():
                accf[slot_m] = jnp.zeros((TOK, DIM), F32)

            accf[slot_m] += dot_nn(abuf[slot], w2buf[ws])

        rs_copy(accf, slot_m, rsf, m, sf_sem, rf_sem).start()

        @pl.when(m == N_MB - 1)
        def _():
            for slot in range(2):
                out_copy(ubuf, slot, u_all, m, slot, uo_sem).wait()
                out_copy(abuf, slot, a_all, m, slot, ao_sem).wait()

    def load_post(acc_buf, m, recv, src):
        ref = acc_buf.at[pl.ds(pl.multiple_of(m * HALF, HALF), HALF), :]
        pltpu.make_async_copy(ref, ref, recv.at[m]).wait()
        a = pltpu.make_async_copy(ref, rsv, p_sem.at[0])
        a.start()
        b = pltpu.make_async_copy(src.at[rows_of(m, my), :], res, p_sem.at[1])
        b.start()
        return a, b

    def forward_post(m):
        slot = lax.rem(m, 2)

        def run(src):
            t = pltpu.make_async_copy(tgt.at[rows_of(m, my), :], tbuf, p_sem.at[2])
            t.start()
            for cp in load_post(rsf, m, rf_sem, src):
                cp.wait()
            t.wait()

        @pl.when(first)
        def _():
            run(x_in)

        @pl.when(jnp.logical_not(first))
        def _():
            run(x_all)

        @pl.when(m >= 2)
        def _():
            @pl.when(last)
            def _():
                yl_send(m, slot).wait_send()

            @pl.when(jnp.logical_not(last))
            def _():
                for cp in yf_pair(m, slot):
                    cp.wait_send()

        y = (res[...].astype(F32) + (accf[slot, half_rows(my), :] + rsv[...])).astype(BF)

        @pl.when(jnp.logical_not(last))
        def _():
            yf[slot] = y
            own, cross = yf_pair(m, slot)
            own.start()
            by_pair = jnp.logical_and(st == 1, m >= RELAY0)

            @pl.when(by_pair)
            def _():
                fwd_send(m, slot).start()

            @pl.when(jnp.logical_not(by_pair))
            def _():
                cross.start()

        @pl.when(last)
        def _():
            err = y.astype(F32) - tbuf[...].astype(F32)
            yf[slot] = (err * (1.0 / N_ELEM)).astype(BF)
            sq = err * err
            part = sq[:, 0:128]
            for c in range(1, DIM // 128):
                part = part + sq[:, c * 128 : (c + 1) * 128]
            lsum[...] += jnp.sum(part.reshape(HALF // 8, 8, 128), axis=0)
            yl_own(m, slot).start()
            yl_send(m, slot).start()

            @pl.when(m == N_MB - 1)
            def _():
                pltpu.make_async_copy(lsum, lrx.at[my], lr_sem.at[my]).start()
                for cond, cp in loss_sends():
                    pl.when(cond)(cp.start)

    def pass_on(m, base, copy):
        ref = fwd.at[fwd_rows(m), :]
        pltpu.make_async_copy(ref, ref, fr_sem.at[m]).wait()

        @pl.when(m >= base + 2)
        def _():
            copy(m - 2).wait_send()

        copy(m).start()

    def relay(m):
        @pl.when(jnp.logical_and(st == 1, jnp.logical_and(m >= RELAY0, m < N_MB)))
        def _():
            pass_on(m, RELAY0, relay_x)

    def relay_back(m):
        @pl.when(jnp.logical_and(first, jnp.logical_and(m >= RELAY3, m < N_MB)))
        def _():
            pass_on(m, RELAY3, relay_e)

    def loss_sends():
        for y in range(2):
            for s in range(4):
                cp = pltpu.make_async_remote_copy(
                    src_ref=lsum,
                    dst_ref=lrx.at[my],
                    send_sem=ls_sem.at[y * 4 + s],
                    recv_sem=lr_sem.at[my],
                    device_id={"model": y, "stage": s},
                    device_id_type=MESH,
                )
                yield (True if s < 3 else my != y), cp

    def backward(m, count):
        slot_m = lax.rem(m, 2)
        u_load(m, 0, 0).start()
        wait_in(e_all, m, er_sem)
        load_x(e_all, m)

        @pl.when(jnp.logical_and(m >= 2, jnp.logical_not(first)))
        def _():
            rs_copy(accb, slot_m, rsb, m - 2, sb_sem, rb_sem).wait_send()

        @pl.loop(0, N_BLK)
        def _(j):
            slot = lax.rem(j, 2)
            ws = next_weights(count, j)
            u_load(m, j, slot).wait()

            @pl.when(j + 1 < N_BLK)
            def _():
                u_load(m, j + 1, 1 - slot).start()

            @pl.when(m * N_BLK + j >= 2)
            def _():
                out_copy(gbuf, slot, g_all, m, j, go_sem).wait()

            q = dot_nt(xbuf[...], w2buf[ws]).astype(BF)
            gbuf[slot] = (gelu_slope(uin[slot].astype(F32)) * q.astype(F32)).astype(BF)
            out_copy(gbuf, slot, g_all, m, j, go_sem).start()

            @pl.when(jnp.logical_not(first))
            def _():
                @pl.when(j == 0)
                def _():
                    accb[slot_m] = jnp.zeros((TOK, DIM), F32)

                accb[slot_m] += dot_nt(gbuf[slot], w1buf[ws])

        @pl.when(jnp.logical_not(first))
        def _():
            rs_copy(accb, slot_m, rsb, m, sb_sem, rb_sem).start()

    def backward_post(m):
        slot = lax.rem(m, 2)
        for cp in load_post(rsb, m, rb_sem, e_all):
            cp.wait()

        @pl.when(m >= 2)
        def _():
            for cp in yb_pair(m, slot):
                cp.wait_send()

        yb[slot] = (res[...].astype(F32) + (accb[slot, half_rows(my), :] + rsv[...])).astype(BF)
        own, cross = yb_pair(m, slot)
        own.start()
        far = jnp.logical_and(last, m >= RELAY3)

        @pl.when(far)
        def _():
            far_send(m, slot).start()

        @pl.when(jnp.logical_not(far))
        def _():
            cross.start()

    def weight_ops(v):
        grp = v // GROUP
        quart = lax.rem(v, GROUP)
        rows = pl.ds(pl.multiple_of(grp * GTOK, GTOK), GTOK)
        out2 = quart < 2

        def on_tile(t, fn2, fn1):
            @pl.when(out2)
            def _():
                fn2(cols(quart * 5 + t))

            @pl.when(jnp.logical_not(out2))
            def _():
                fn1(cols(t), cols(quart - 2, DIM))

        def start_tile(t):
            n_slot = lax.rem(t, 2)
            slot = lax.rem(t, 3)

            def fn2(blk):
                pltpu.make_async_copy(a_all.at[rows, blk], narrow.at[n_slot], wn_sem.at[n_slot]).start()

                @pl.when(grp > 0)
                def _():
                    pltpu.make_async_copy(acc2.at[blk, :], wtile.at[slot], wl_sem.at[slot]).start()

            def fn1(dblk, half):
                @pl.when(first)
                def _():
                    pltpu.make_async_copy(x_in.at[rows, dblk], narrow.at[n_slot], wn_sem.at[n_slot]).start()

                @pl.when(jnp.logical_not(first))
                def _():
                    pltpu.make_async_copy(x_all.at[rows, dblk], narrow.at[n_slot], wn_sem.at[n_slot]).start()

                @pl.when(grp > 0)
                def _():
                    pltpu.make_async_copy(acc1.at[dblk, half], wtile.at[slot], wl_sem.at[slot]).start()

            on_tile(t, fn2, fn1)

        def start_store(t):
            slot = lax.rem(t, 3)

            def fn2(blk):
                pltpu.make_async_copy(wtile.at[slot], acc2.at[blk, :], ws_sem.at[slot]).start()

            def fn1(dblk, half):
                pltpu.make_async_copy(wtile.at[slot], acc1.at[dblk, half], ws_sem.at[slot]).start()

            on_tile(t, fn2, fn1)

        def wait_store(slot):
            pltpu.make_async_copy(wtile.at[slot], acc2.at[pl.ds(0, HB), :], ws_sem.at[slot]).wait()

        def start():
            @pl.when(out2)
            def _():
                pltpu.make_async_copy(e_all.at[rows, :], wide, wd_sem).start()

            @pl.when(jnp.logical_not(out2))
            def _():
                pltpu.make_async_copy(g_all.at[rows, cols(quart - 2, DIM)], wide, wd_sem).start()

            start_tile(0)

        def run():
            pltpu.make_async_copy(e_all.at[rows, :], wide, wd_sem).wait()

            @pl.loop(0, 5)
            def _(t):
                slot = lax.rem(t, 3)
                n_slot = lax.rem(t, 2)

                @pl.when(t >= 2)
                def _():
                    wait_store(lax.rem(t + 1, 3))

                @pl.when(t < 4)
                def _():
                    start_tile(t + 1)

                pltpu.make_async_copy(a_all.at[rows, pl.ds(0, HB)], narrow.at[n_slot], wn_sem.at[n_slot]).wait()

                @pl.when(grp > 0)
                def _():
                    pltpu.make_async_copy(acc2.at[pl.ds(0, HB), :], wtile.at[slot], wl_sem.at[slot]).wait()

                @pl.when(grp == 0)
                def _():
                    wtile[slot] = jnp.zeros((HB, DIM), F32)

                wtile[slot] += dot_tn(narrow[n_slot], wide[...])
                start_store(t)

            wait_store(0)
            wait_store(1)

        return start, run

    lsum[...] = jnp.zeros((8, 128), F32)
    for j in range(W_SLOTS - 1):
        for cp in w_copies(j, j):
            cp.start()

    @pl.loop(0, N_MB + warm)
    def _(k):
        b = k - warm
        p = k - 1
        v = b - GROUP
        b_on = b >= 0
        f_on = k < N_MB
        p_on = jnp.logical_and(p >= 0, p < N_MB)
        pb_on = jnp.logical_and(b_on, jnp.logical_not(first))
        w_on = jnp.logical_and(v >= 0, jnp.logical_not(first))

        @pl.when(jnp.logical_and(first, v >= 0))
        def _():
            start, run = weight_ops(v)
            start()
            run()

        @pl.when(b_on)
        def _():
            backward(b, b + jnp.minimum(k, N_MB))
            relay_back(b + LEAD3)

        @pl.when(jnp.logical_and(b_on, p_on))
        def _():
            forward_post(p)

        @pl.when(b_on)
        def _():
            relay(k - 2)

        @pl.when(w_on)
        def _():
            weight_ops(v)[0]()

        @pl.when(f_on)
        def _():
            forward(k, k + jnp.maximum(b + 1, 0))

        @pl.when(jnp.logical_and(jnp.logical_not(b_on), p_on))
        def _():
            forward_post(p)

        @pl.when(jnp.logical_not(b_on))
        def _():
            relay(k - 2)

        @pl.when(jnp.logical_and(pb_on, f_on))
        def _():
            backward_post(b)

        @pl.when(w_on)
        def _():
            weight_ops(v)[1]()

        @pl.when(jnp.logical_and(pb_on, jnp.logical_not(f_on)))
        def _():
            backward_post(b)

    for half in range(2):
        pltpu.make_async_copy(lsum, lrx.at[half], lr_sem.at[half]).wait()
    loss[...] = lrx[0] + lrx[1]

    for j in range(W_SLOTS - 1):
        for cp in w_copies(j, (2 * N_MB * N_BLK + j) % W_SLOTS):
            cp.wait()
    for m in (N_MB - 2, N_MB - 1):
        slot = m % 2
        out_copy(gbuf, slot, g_all, m, 0, go_sem).wait()
        rs_copy(accf, slot, rsf, m, sf_sem, rf_sem).wait_send()

        @pl.when(jnp.logical_not(first))
        def _():
            rs_copy(accb, slot, rsb, m, sb_sem, rb_sem).wait_send()
            for cp in yb_pair(m, slot):
                cp.wait_send()

        @pl.when(last)
        def _():
            yl_send(m, slot).wait_send()

        @pl.when(jnp.logical_not(last))
        def _():
            for cp in yf_pair(m, slot):
                cp.wait_send()

        @pl.when(st == 1)
        def _():
            relay_x(m).wait_send()

        @pl.when(first)
        def _():
            relay_e(m).wait_send()

    @pl.when(last)
    def _():
        for cond, cp in loss_sends():
            pl.when(cond)(cp.wait_send)


def run_pipeline(x_in, tgt, w1, w2):
    tokens = N_MB * TOK
    hbm = pl.BlockSpec(memory_space=pl.ANY)
    dma = pltpu.SemaphoreType.DMA
    shapes = [
        ((tokens, DIM), BF), ((tokens, DIM), BF),
        ((tokens, HID), BF), ((tokens, HID), BF), ((tokens, HID), BF),
        ((tokens // 2, DIM), F32), ((tokens // 2, DIM), F32), ((tokens // 2, DIM), BF),
        ((DIM, HID), F32), ((HID, DIM), F32),
    ]
    out_shape = [jax.ShapeDtypeStruct(s, d) for s, d in shapes] + [jax.ShapeDtypeStruct((8, 128), F32)]
    return pl.pallas_call(
        pipeline_kernel,
        out_shape=out_shape,
        in_specs=[hbm] * 4,
        out_specs=[hbm] * 10 + [pl.BlockSpec(memory_space=pltpu.VMEM)],
        scratch_shapes=[
            pltpu.VMEM((TOK, DIM), BF),
            pltpu.VMEM((W_SLOTS, DIM, HB), BF),
            pltpu.VMEM((W_SLOTS, HB, DIM), BF),
            pltpu.VMEM((2, TOK, HB), BF),
            pltpu.VMEM((2, TOK, HB), BF),
            pltpu.VMEM((2, TOK, HB), BF),
            pltpu.VMEM((2, TOK, HB), BF),
            pltpu.VMEM((2, TOK, DIM), F32),
            pltpu.VMEM((2, TOK, DIM), F32),
            pltpu.VMEM((HALF, DIM), F32),
            pltpu.VMEM((HALF, DIM), BF),
            pltpu.VMEM((HALF, DIM), BF),
            pltpu.VMEM((2, HALF, DIM), BF),
            pltpu.VMEM((2, HALF, DIM), BF),
            pltpu.VMEM((GTOK, DIM), BF),
            pltpu.VMEM((2, GTOK, HB), BF),
            pltpu.VMEM((3, HB, DIM), F32),
            pltpu.VMEM((8, 128), F32),
            pltpu.VMEM((2, 8, 128), F32),
            dma((W_SLOTS, 2)), dma, dma((2,)), dma((2,)), dma((2,)), dma((2,)), dma((3,)), dma, dma((2,)), dma((3,)), dma((3,)),
            dma((N_MB, 2)), dma((N_MB, 2)), dma((N_MB,)), dma((N_MB,)), dma((2,)), dma((2,)), dma((2, 2)), dma((2, 2)),
            dma((N_MB,)), dma((2,)), dma((8,)), dma((2,)),
        ],
        compiler_params=pltpu.CompilerParams(vmem_limit_bytes=66_000_000, has_side_effects=True),
        name="pipeline",
    )(x_in, tgt, w1, w2)


def tail_kernel(x_all, e_all, a_all, g_all, acc1, acc2, out1, out2, wide, narrow, tile, wide_sem, n_sem, l_sem, s_sem):
    rows = pl.ds(N_GRP * GTOK, GTOK)
    n2 = HID // HB
    n1 = DIM // HB

    def cols(j, width=HB):
        return pl.ds(pl.multiple_of(j * width, width), width)

    def on_tile(t, fn2, fn1):
        @pl.when(t < n2)
        def _():
            fn2(cols(t))

        @pl.when(t >= n2)
        def _():
            fn1(cols(lax.rem(t - n2, n1)), cols((t - n2) // n1, DIM))

    def start_tile(t):
        slot = lax.rem(t, 4)
        n_slot = lax.rem(t, 3)

        def fn2(blk):
            pltpu.make_async_copy(acc2.at[blk, :], tile.at[slot], l_sem.at[slot]).start()
            pltpu.make_async_copy(a_all.at[rows, blk], narrow.at[n_slot], n_sem.at[n_slot]).start()

        def fn1(dblk, half):
            pltpu.make_async_copy(acc1.at[dblk, half], tile.at[slot], l_sem.at[slot]).start()
            pltpu.make_async_copy(x_all.at[rows, dblk], narrow.at[n_slot], n_sem.at[n_slot]).start()

        on_tile(t, fn2, fn1)

    def start_store(t):
        slot = lax.rem(t, 4)

        def fn2(blk):
            pltpu.make_async_copy(tile.at[slot], out2.at[blk, :], s_sem.at[slot]).start()

        def fn1(dblk, half):
            pltpu.make_async_copy(tile.at[slot], out1.at[dblk, half], s_sem.at[slot]).start()

        on_tile(t, fn2, fn1)

    def wait_store(slot):
        pltpu.make_async_copy(tile.at[slot], out2.at[pl.ds(0, HB), :], s_sem.at[slot]).wait()

    def wide_copy(i):
        src = e_all.at[rows, :] if i == 0 else g_all.at[rows, pl.ds((i - 1) * DIM, DIM)]
        return pltpu.make_async_copy(src, wide.at[i], wide_sem.at[i])

    start_tile(0)
    wide_copy(0).start()
    start_tile(1)

    @pl.loop(0, n2 + 2 * n1)
    def _(t):
        slot = lax.rem(t, 4)
        n_slot = lax.rem(t, 3)

        @pl.when(t >= 2)
        def _():
            wait_store(lax.rem(t + 2, 4))

        @pl.when(t + 2 < n2 + 2 * n1)
        def _():
            start_tile(t + 2)

        for i in range(1, 3):

            @pl.when(t == n2 + (i - 1) * n1 - 4)
            def _():
                wide_copy(i).start()

        for i in range(3):

            @pl.when(t == (0 if i == 0 else n2 + (i - 1) * n1))
            def _():
                wide_copy(i).wait()

        pltpu.make_async_copy(a_all.at[rows, pl.ds(0, HB)], narrow.at[n_slot], n_sem.at[n_slot]).wait()
        pltpu.make_async_copy(acc2.at[pl.ds(0, HB), :], tile.at[slot], l_sem.at[slot]).wait()
        which = jnp.where(t < n2, 0, 1 + (t - n2) // n1)
        tile[slot] += dot_tn(narrow[n_slot], wide[which])
        start_store(t)

    wait_store(2)
    wait_store(3)


def add_tail(x_all, e_all, a_all, g_all, acc1, acc2):
    hbm = pl.BlockSpec(memory_space=pl.ANY)
    dma = pltpu.SemaphoreType.DMA
    return pl.pallas_call(
        tail_kernel,
        in_specs=[hbm] * 6,
        out_specs=[hbm] * 2,
        out_shape=[jax.ShapeDtypeStruct(acc1.shape, F32), jax.ShapeDtypeStruct(acc2.shape, F32)],
        scratch_shapes=[
            pltpu.VMEM((3, GTOK, DIM), BF),
            pltpu.VMEM((3, GTOK, HB), BF),
            pltpu.VMEM((4, HB, DIM), F32),
            dma((3,)), dma((3,)), dma((4,)), dma((4,)),
        ],
        compiler_params=pltpu.CompilerParams(vmem_limit_bytes=60_000_000),
        name="tail",
    )(x_all, e_all, a_all, g_all, acc1, acc2)


def solution(mesh):
    def stage_step(inputs, targets, w_in, w_out):
        tokens = N_MB * TOK
        x_in = inputs.reshape(tokens, DIM)
        tgt = targets.reshape(tokens, DIM)
        x_all, e_all, _, a_all, g_all, _, _, _, acc1, acc2, loss = run_pipeline(x_in, tgt, w_in[0, 0], w_out[0, 0])
        grad_in, grad_out = add_tail(x_all, e_all, a_all, g_all, acc1, acc2)
        total = jnp.sum(loss) * (0.5 / N_ELEM)
        return grad_in[None, None], grad_out[None, None], jnp.reshape(total, (1,))

    return jax.shard_map(
        stage_step,
        mesh=mesh,
        in_specs=(P("data", None, None), P("data", None, None), P("stage", None, None, "model"), P("stage", None, "model", None)),
        out_specs=(P(("data", "stage"), None, None, "model"), P(("data", "stage"), None, "model", None), P("data")),
        check_vma=False,
    )
```

```python
import jax
import jax.numpy as jnp
from jax import lax
from jax.experimental import pallas as pl
from jax.experimental.pallas import tpu as pltpu
from jax.sharding import PartitionSpec as P

GELU_COEF = 0.7978845608028654
CUBIC_COEF = 0.044715

N_MB = 24
TOK = 256
HALF = TOK // 2
DIM = 2560
HID = 5120
HB = 512
N_BLK = HID // HB
W_SLOTS = 3
WT = HB // 2
N_WT = 6
GROUP = 4
N_GRP = N_MB // GROUP - 1
GTOK = GROUP * TOK
N_ELEM = N_MB * TOK * DIM
RELAY0 = 3
RELAY3 = 10
LEAD3 = 3
MESH = pl.DeviceIdType.MESH
BF = jnp.bfloat16
F32 = jnp.float32


def dot_nn(a, b):
    return lax.dot_general(a, b, (((1,), (0,)), ((), ())), preferred_element_type=F32)


def dot_nt(a, b):
    return lax.dot_general(a, b, (((1,), (1,)), ((), ())), preferred_element_type=F32)


def dot_tn(a, b):
    return lax.dot_general(a, b, (((0,), (0,)), ((), ())), preferred_element_type=F32)


def gelu(v):
    return 0.5 * v * (1.0 + jnp.tanh(GELU_COEF * (v + CUBIC_COEF * v * v * v)))


def gelu_slope(v):
    t = jnp.tanh(GELU_COEF * (v + CUBIC_COEF * v * v * v))
    return 0.5 * (1.0 + t) + 0.5 * v * (1.0 - t * t) * GELU_COEF * (1.0 + 3.0 * CUBIC_COEF * v * v)


def pipeline_kernel(
    x_in, tgt, w1, w2,
    x_all, e_all, u_all, a_all, g_all, rsf, rsb, fwd, acc1, acc2, loss,
    xbuf, w1buf, w2buf, ubuf0, ubuf1, abuf0, abuf1, gbuf0, gbuf1, uin0, uin1, qbuf, accf, accb, rsv, res, tbuf, yf, yb, wide, narrow, wtile, lsum, lrx,
    w_sem, x_sem, uo_sem, ao_sem, go_sem, ui_sem, p_sem, wd_sem, wn_sem, wl_sem, ws_sem,
    xr_sem, er_sem, rf_sem, rb_sem, sf_sem, sb_sem, yf_sem, yb_sem, fr_sem, fs_sem, ls_sem, lr_sem,
):
    my = lax.axis_index("model")
    st = lax.axis_index("stage")
    other = 1 - my
    last = st == 3
    first = st == 0
    warm = jnp.where(st == 0, 16, jnp.where(st == 1, 10, jnp.where(st == 2, 5, 2)))
    partner = {"model": other}
    nxt = jnp.minimum(st + 1, 3)
    prv = jnp.maximum(st - 1, 0)

    def rows_of(m, half):
        return pl.ds(pl.multiple_of(m * TOK + half * HALF, HALF), HALF)

    def mb_rows(m):
        return pl.ds(pl.multiple_of(m * TOK, TOK), TOK)

    def half_rows(half):
        return pl.ds(pl.multiple_of(half * HALF, HALF), HALF)

    def cols(j, width=HB):
        return pl.ds(pl.multiple_of(j * width, width), width)

    ubuf, abuf, gbuf, uin = (ubuf0, ubuf1), (abuf0, abuf1), (gbuf0, gbuf1), (uin0, uin1)

    def w1_copy(j, slot):
        return pltpu.make_async_copy(w1.at[:, cols(j)], w1buf.at[slot], w_sem.at[slot, 0])

    def w2_copy(j, slot):
        return pltpu.make_async_copy(w2.at[cols(j), :], w2buf.at[slot], w_sem.at[slot, 1])

    def use(copy, at):
        slot = lax.rem(at, W_SLOTS)
        copy(lax.rem(at, N_BLK), slot).wait()
        ahead = at + W_SLOTS - 1
        copy(lax.rem(ahead, N_BLK), lax.rem(ahead, W_SLOTS)).start()
        return slot

    def rs_copy(acc, slot, buf, m, send, recv):
        return pltpu.make_async_remote_copy(
            src_ref=acc.at[slot, half_rows(other), :],
            dst_ref=buf.at[pl.ds(pl.multiple_of(m * HALF, HALF), HALF), :],
            send_sem=send.at[slot],
            recv_sem=recv.at[m],
            device_id=partner,
            device_id_type=MESH,
        )

    def half_copy(src, slot, dst, m, half, send, k, recv, dev):
        return pltpu.make_async_remote_copy(
            src_ref=src.at[slot],
            dst_ref=dst.at[rows_of(m, half), :],
            send_sem=send.at[slot, k],
            recv_sem=recv.at[m, half],
            device_id=dev,
            device_id_type=MESH,
        )

    def yf_pair(m, slot):
        return (
            half_copy(yf, slot, x_all, m, my, yf_sem, 0, xr_sem, {"model": my, "stage": nxt}),
            half_copy(yf, slot, x_all, m, my, yf_sem, 1, xr_sem, {"model": other, "stage": nxt}),
        )

    def fwd_rows(m):
        return pl.ds(pl.multiple_of(m * HALF, HALF), HALF)

    def fwd_send(m, slot):
        return pltpu.make_async_remote_copy(
            src_ref=yf.at[slot],
            dst_ref=fwd.at[fwd_rows(m), :],
            send_sem=yf_sem.at[slot, 1],
            recv_sem=fr_sem.at[m],
            device_id=partner,
            device_id_type=MESH,
        )

    def relay_copy(m, dst, recv, to):
        return pltpu.make_async_remote_copy(
            src_ref=fwd.at[fwd_rows(m), :],
            dst_ref=dst.at[rows_of(m, other), :],
            send_sem=fs_sem.at[lax.rem(m, 2)],
            recv_sem=recv.at[m, other],
            device_id={"model": my, "stage": to},
            device_id_type=MESH,
        )

    def relay_x(m):
        return relay_copy(m, x_all, xr_sem, 2)

    def relay_e(m):
        return relay_copy(m, e_all, er_sem, 2)

    def far_send(m, slot):
        return pltpu.make_async_remote_copy(
            src_ref=yb.at[slot],
            dst_ref=fwd.at[fwd_rows(m), :],
            send_sem=yb_sem.at[slot, 1],
            recv_sem=fr_sem.at[m],
            device_id={"model": other, "stage": 0},
            device_id_type=MESH,
        )

    def yl_own(m, slot):
        return pltpu.make_async_copy(yf.at[slot], e_all.at[rows_of(m, my), :], er_sem.at[m, my])

    def yl_send(m, slot):
        return half_copy(yf, slot, e_all, m, my, yf_sem, 1, er_sem, partner)

    def yb_pair(m, slot):
        return (
            half_copy(yb, slot, e_all, m, my, yb_sem, 0, er_sem, {"model": my, "stage": prv}),
            half_copy(yb, slot, e_all, m, my, yb_sem, 1, er_sem, {"model": other, "stage": prv}),
        )

    def wait_in(dst, m, recv):
        for half in range(2):
            ref = dst.at[rows_of(m, half), :]
            pltpu.make_async_copy(ref, ref, recv.at[m, half]).wait()

    def out_copy(buf, slot, dst, m, j, sem):
        return pltpu.make_async_copy(buf[slot], dst.at[mb_rows(m), cols(j)], sem.at[slot])

    def u_load(m, j, slot):
        return pltpu.make_async_copy(u_all.at[mb_rows(m), cols(j)], uin[slot], ui_sem.at[slot])

    def load_x(src, m, also=None):
        cp = pltpu.make_async_copy(src.at[mb_rows(m), :], xbuf, x_sem)
        cp.start()
        if also is not None:
            also()
        cp.wait()

    def forward(m, count, also):
        slot_m = lax.rem(m, 2)
        base = count * N_BLK

        @pl.when(first)
        def _():
            load_x(x_in, m)

            @pl.when(m >= N_GRP * GROUP)
            def _():
                cp = pltpu.make_async_copy(xbuf, x_all.at[mb_rows(m), :], x_sem)
                cp.start()
                cp.wait()

        @pl.when(jnp.logical_not(first))
        def _():
            wait_in(x_all, m, xr_sem)
            load_x(x_all, m, also)

        @pl.when(m >= 2)
        def _():
            rs_copy(accf, slot_m, rsf, m - 2, sf_sem, rf_sem).wait_send()

        def block(j, slot):
            w1s = use(w1_copy, base + j)
            w2s = None if isinstance(j, int) and j == 0 else use(w2_copy, base + j - 1)

            def drain():
                out_copy(ubuf, slot, u_all, m, j, uo_sem).wait()
                out_copy(abuf, slot, a_all, m, j, ao_sem).wait()

            if isinstance(j, int) and j == 0:
                pl.when(m >= 1)(drain)
            else:
                pl.when(jnp.logical_or(m >= 1, j >= 2))(drain)
            ubuf[slot][...] = dot_nn(xbuf[...], w1buf[w1s]).astype(BF)
            if w2s is None:
                accf[slot_m] = jnp.zeros((TOK, DIM), F32)
            else:
                accf[slot_m] += dot_nn(abuf[1 - slot][...], w2buf[w2s])
            abuf[slot][...] = gelu(ubuf[slot][...].astype(F32)).astype(BF)
            out_copy(ubuf, slot, u_all, m, j, uo_sem).start()
            out_copy(abuf, slot, a_all, m, j, ao_sem).start()

        block(0, 0)

        @pl.loop(0, (N_BLK - 2) // 2)
        def _(i):
            block(2 * i + 1, 1)
            block(2 * i + 2, 0)

        block(N_BLK - 1, 1)
        w2s = use(w2_copy, base + N_BLK - 1)
        accf[slot_m] += dot_nn(abuf[1][...], w2buf[w2s])
        rs_copy(accf, slot_m, rsf, m, sf_sem, rf_sem).start()

        @pl.when(m == N_MB - 1)
        def _():
            for slot in range(2):
                out_copy(ubuf, slot, u_all, m, slot, uo_sem).wait()
                out_copy(abuf, slot, a_all, m, slot, ao_sem).wait()

    def load_post(acc_buf, m, recv, src):
        ref = acc_buf.at[pl.ds(pl.multiple_of(m * HALF, HALF), HALF), :]
        pltpu.make_async_copy(ref, ref, recv.at[m]).wait()
        a = pltpu.make_async_copy(ref, rsv, p_sem.at[0])
        a.start()
        b = pltpu.make_async_copy(src.at[rows_of(m, my), :], res, p_sem.at[1])
        b.start()
        return a, b

    def forward_post(m):
        slot = lax.rem(m, 2)

        def run(src):
            t = pltpu.make_async_copy(tgt.at[rows_of(m, my), :], tbuf, p_sem.at[2])
            t.start()
            for cp in load_post(rsf, m, rf_sem, src):
                cp.wait()
            t.wait()

        @pl.when(first)
        def _():
            run(x_in)

        @pl.when(jnp.logical_not(first))
        def _():
            run(x_all)

        @pl.when(m >= 2)
        def _():
            @pl.when(last)
            def _():
                yl_send(m, slot).wait_send()

            @pl.when(jnp.logical_not(last))
            def _():
                for cp in yf_pair(m, slot):
                    cp.wait_send()

        y = (res[...].astype(F32) + (accf[slot, half_rows(my), :] + rsv[...])).astype(BF)

        @pl.when(jnp.logical_not(last))
        def _():
            yf[slot] = y
            own, cross = yf_pair(m, slot)
            own.start()
            by_pair = jnp.logical_and(st == 1, m >= RELAY0)

            @pl.when(by_pair)
            def _():
                fwd_send(m, slot).start()

            @pl.when(jnp.logical_not(by_pair))
            def _():
                cross.start()

        @pl.when(last)
        def _():
            err = y.astype(F32) - tbuf[...].astype(F32)
            yf[slot] = (err * (1.0 / N_ELEM)).astype(BF)
            sq = err * err
            part = sq[:, 0:128]
            for c in range(1, DIM // 128):
                part = part + sq[:, c * 128 : (c + 1) * 128]
            lsum[...] += jnp.sum(part.reshape(HALF // 8, 8, 128), axis=0)
            yl_own(m, slot).start()
            yl_send(m, slot).start()

            @pl.when(m == N_MB - 1)
            def _():
                pltpu.make_async_copy(lsum, lrx.at[my], lr_sem.at[my]).start()
                for cond, cp in loss_sends():
                    pl.when(cond)(cp.start)

    def pass_on(m, base, copy):
        ref = fwd.at[fwd_rows(m), :]
        pltpu.make_async_copy(ref, ref, fr_sem.at[m]).wait()

        @pl.when(m >= base + 2)
        def _():
            copy(m - 2).wait_send()

        copy(m).start()

    def relay(m):
        @pl.when(jnp.logical_and(st == 1, jnp.logical_and(m >= RELAY0, m < N_MB)))
        def _():
            pass_on(m, RELAY0, relay_x)

    def relay_back(m):
        @pl.when(jnp.logical_and(first, jnp.logical_and(m >= RELAY3, m < N_MB)))
        def _():
            pass_on(m, RELAY3, relay_e)

    def loss_sends():
        for y in range(2):
            for s in range(4):
                cp = pltpu.make_async_remote_copy(
                    src_ref=lsum,
                    dst_ref=lrx.at[my],
                    send_sem=ls_sem.at[y * 4 + s],
                    recv_sem=lr_sem.at[my],
                    device_id={"model": y, "stage": s},
                    device_id_type=MESH,
                )
                yield (True if s < 3 else my != y), cp

    def backward(m, count):
        slot_m = lax.rem(m, 2)
        base = count * N_BLK
        u_load(m, 0, 0).start()
        wait_in(e_all, m, er_sem)
        load_x(e_all, m)

        @pl.when(jnp.logical_and(m >= 2, jnp.logical_not(first)))
        def _():
            rs_copy(accb, slot_m, rsb, m - 2, sb_sem, rb_sem).wait_send()

        def block(j, slot, chain):
            start = isinstance(j, int) and j == 0
            w2s = use(w2_copy, base + j)
            w1s = None if start else use(w1_copy, base + j - 1)
            u_load(m, j, slot).wait()
            if not (isinstance(j, int) and j == N_BLK - 1):
                u_load(m, j + 1, 1 - slot).start()
            drain = out_copy(gbuf, slot, g_all, m, j, go_sem).wait
            if start:
                pl.when(m >= 1)(drain)
            else:
                pl.when(jnp.logical_or(m >= 1, j >= 2))(drain)
            qbuf[...] = dot_nt(xbuf[...], w2buf[w2s]).astype(BF)
            if chain and start:
                accb[slot_m] = jnp.zeros((TOK, DIM), F32)
            elif chain:
                accb[slot_m] += dot_nt(gbuf[1 - slot][...], w1buf[w1s])
            gbuf[slot][...] = (gelu_slope(uin[slot][...].astype(F32)) * qbuf[...].astype(F32)).astype(BF)
            out_copy(gbuf, slot, g_all, m, j, go_sem).start()

        def blocks(chain):
            block(0, 0, chain)

            @pl.loop(0, (N_BLK - 2) // 2)
            def _(i):
                block(2 * i + 1, 1, chain)
                block(2 * i + 2, 0, chain)

            block(N_BLK - 1, 1, chain)
            w1s = use(w1_copy, base + N_BLK - 1)
            if chain:
                accb[slot_m] += dot_nt(gbuf[1][...], w1buf[w1s])
                rs_copy(accb, slot_m, rsb, m, sb_sem, rb_sem).start()

        @pl.when(first)
        def _():
            blocks(False)

        @pl.when(jnp.logical_not(first))
        def _():
            blocks(True)

    def backward_post(m):
        slot = lax.rem(m, 2)
        for cp in load_post(rsb, m, rb_sem, e_all):
            cp.wait()

        @pl.when(m >= 2)
        def _():
            for cp in yb_pair(m, slot):
                cp.wait_send()

        yb[slot] = (res[...].astype(F32) + (accb[slot, half_rows(my), :] + rsv[...])).astype(BF)
        own, cross = yb_pair(m, slot)
        own.start()
        far = jnp.logical_and(last, m >= RELAY3)

        @pl.when(far)
        def _():
            far_send(m, slot).start()

        @pl.when(jnp.logical_not(far))
        def _():
            cross.start()

    def weight_ops(v):
        grp = v // GROUP
        quart = lax.rem(v, GROUP)
        rows = pl.ds(pl.multiple_of(grp * GTOK, GTOK), GTOK)
        out2 = quart < 2

        def on_tile(t, fn2, fn1):
            @pl.when(out2)
            def _():
                fn2(cols(quart * (HID // WT // 2) + t, WT))

            @pl.when(jnp.logical_not(out2))
            def _():
                fn1(cols(t, WT), cols(quart - 2, DIM))

        def start_tile(t):
            n_slot = lax.rem(t, 4)
            slot = lax.rem(t, N_WT)

            def fn2(blk):
                pltpu.make_async_copy(a_all.at[rows, blk], narrow.at[n_slot], wn_sem.at[n_slot]).start()

                @pl.when(grp > 0)
                def _():
                    pltpu.make_async_copy(acc2.at[blk, :], wtile.at[slot], wl_sem.at[slot]).start()

            def fn1(dblk, half):
                @pl.when(first)
                def _():
                    pltpu.make_async_copy(x_in.at[rows, dblk], narrow.at[n_slot], wn_sem.at[n_slot]).start()

                @pl.when(jnp.logical_not(first))
                def _():
                    pltpu.make_async_copy(x_all.at[rows, dblk], narrow.at[n_slot], wn_sem.at[n_slot]).start()

                @pl.when(grp > 0)
                def _():
                    pltpu.make_async_copy(acc1.at[dblk, half], wtile.at[slot], wl_sem.at[slot]).start()

            on_tile(t, fn2, fn1)

        def start_store(t):
            slot = lax.rem(t, N_WT)

            def fn2(blk):
                pltpu.make_async_copy(wtile.at[slot], acc2.at[blk, :], ws_sem.at[slot]).start()

            def fn1(dblk, half):
                pltpu.make_async_copy(wtile.at[slot], acc1.at[dblk, half], ws_sem.at[slot]).start()

            on_tile(t, fn2, fn1)

        def wait_store(slot):
            pltpu.make_async_copy(wtile.at[slot], acc2.at[pl.ds(0, WT), :], ws_sem.at[slot]).wait()

        def start():
            @pl.when(out2)
            def _():
                pltpu.make_async_copy(e_all.at[rows, :], wide, wd_sem).start()

            @pl.when(jnp.logical_not(out2))
            def _():
                pltpu.make_async_copy(g_all.at[rows, cols(quart - 2, DIM)], wide, wd_sem).start()

            for t in range(N_WT // 2):
                start_tile(t)

        n_tiles = DIM // WT

        def run(low, high):
            if low == 0:
                pltpu.make_async_copy(e_all.at[rows, :], wide, wd_sem).wait()

            @pl.loop(low, high)
            def _(t):
                slot = lax.rem(t, N_WT)
                n_slot = lax.rem(t, 4)

                @pl.when(t >= N_WT // 2)
                def _():
                    wait_store(lax.rem(t + N_WT // 2, N_WT))

                @pl.when(t + N_WT // 2 < n_tiles)
                def _():
                    start_tile(t + N_WT // 2)

                pltpu.make_async_copy(a_all.at[rows, pl.ds(0, WT)], narrow.at[n_slot], wn_sem.at[n_slot]).wait()

                @pl.when(grp > 0)
                def _():
                    pltpu.make_async_copy(acc2.at[pl.ds(0, WT), :], wtile.at[slot], wl_sem.at[slot]).wait()

                @pl.when(grp == 0)
                def _():
                    wtile[slot] = jnp.zeros((WT, DIM), F32)

                wtile[slot] += dot_tn(narrow[n_slot], wide[...])
                start_store(t)

            if high == n_tiles:
                for t in range(n_tiles - N_WT // 2, n_tiles):
                    wait_store(t % N_WT)

        return start, run

    lsum[...] = jnp.zeros((8, 128), F32)
    for j in range(W_SLOTS - 1):
        w1_copy(j, j).start()
        w2_copy(j, j).start()

    @pl.loop(0, N_MB + warm)
    def _(k):
        b = k - warm
        p = k - 1
        v = b - GROUP
        b_on = b >= 0
        f_on = k < N_MB
        p_on = jnp.logical_and(p >= 0, p < N_MB)
        pb_on = jnp.logical_and(b_on, jnp.logical_not(first))
        w_on = jnp.logical_and(v >= 0, jnp.logical_not(first))

        @pl.when(jnp.logical_and(first, v >= 0))
        def _():
            start, run = weight_ops(v)
            start()
            run(0, DIM // WT)

        @pl.when(b_on)
        def _():
            backward(b, b + jnp.minimum(k, N_MB))
            relay_back(b + LEAD3)

        @pl.when(jnp.logical_and(b_on, p_on))
        def _():
            forward_post(p)

        @pl.when(b_on)
        def _():
            relay(k - 2)

        @pl.when(jnp.logical_and(w_on, jnp.logical_not(f_on)))
        def _():
            weight_ops(v)[0]()

        @pl.when(f_on)
        def _():
            forward(k, k + jnp.maximum(b + 1, 0), lambda: pl.when(w_on)(weight_ops(v)[0]))

        @pl.when(jnp.logical_and(jnp.logical_not(b_on), p_on))
        def _():
            forward_post(p)

        @pl.when(jnp.logical_not(b_on))
        def _():
            relay(k - 2)

        @pl.when(jnp.logical_and(pb_on, f_on))
        def _():
            backward_post(b)

        half_tiles = DIM // WT // 2

        @pl.when(w_on)
        def _():
            weight_ops(v)[1](0, half_tiles)

        @pl.when(jnp.logical_and(pb_on, jnp.logical_not(f_on)))
        def _():
            backward_post(b)

        @pl.when(w_on)
        def _():
            weight_ops(v)[1](half_tiles, 2 * half_tiles)

    for half in range(2):
        pltpu.make_async_copy(lsum, lrx.at[half], lr_sem.at[half]).wait()
    loss[...] = lrx[0] + lrx[1]

    for j in range(W_SLOTS - 1):
        w1_copy(j, (2 * N_MB * N_BLK + j) % W_SLOTS).wait()
        w2_copy(j, (2 * N_MB * N_BLK + j) % W_SLOTS).wait()
    for m in (N_MB - 2, N_MB - 1):
        slot = m % 2
        out_copy(gbuf, slot, g_all, m, 0, go_sem).wait()
        rs_copy(accf, slot, rsf, m, sf_sem, rf_sem).wait_send()

        @pl.when(jnp.logical_not(first))
        def _():
            rs_copy(accb, slot, rsb, m, sb_sem, rb_sem).wait_send()
            for cp in yb_pair(m, slot):
                cp.wait_send()

        @pl.when(last)
        def _():
            yl_send(m, slot).wait_send()

        @pl.when(jnp.logical_not(last))
        def _():
            for cp in yf_pair(m, slot):
                cp.wait_send()

        @pl.when(st == 1)
        def _():
            relay_x(m).wait_send()

        @pl.when(first)
        def _():
            relay_e(m).wait_send()

    @pl.when(last)
    def _():
        for cond, cp in loss_sends():
            pl.when(cond)(cp.wait_send)


def run_pipeline(x_in, tgt, w1, w2):
    tokens = N_MB * TOK
    hbm = pl.BlockSpec(memory_space=pl.ANY)
    dma = pltpu.SemaphoreType.DMA
    shapes = [
        ((tokens, DIM), BF), ((tokens, DIM), BF),
        ((tokens, HID), BF), ((tokens, HID), BF), ((tokens, HID), BF),
        ((tokens // 2, DIM), F32), ((tokens // 2, DIM), F32), ((tokens // 2, DIM), BF),
        ((DIM, HID), F32), ((HID, DIM), F32),
    ]
    out_shape = [jax.ShapeDtypeStruct(s, d) for s, d in shapes] + [jax.ShapeDtypeStruct((8, 128), F32)]
    return pl.pallas_call(
        pipeline_kernel,
        out_shape=out_shape,
        in_specs=[hbm] * 4,
        out_specs=[hbm] * 10 + [pl.BlockSpec(memory_space=pltpu.VMEM)],
        scratch_shapes=[
            pltpu.VMEM((TOK, DIM), BF),
            pltpu.VMEM((W_SLOTS, DIM, HB), BF),
            pltpu.VMEM((W_SLOTS, HB, DIM), BF),
            pltpu.VMEM((TOK, HB), BF), pltpu.VMEM((TOK, HB), BF),
            pltpu.VMEM((TOK, HB), BF), pltpu.VMEM((TOK, HB), BF),
            pltpu.VMEM((TOK, HB), BF), pltpu.VMEM((TOK, HB), BF),
            pltpu.VMEM((TOK, HB), BF), pltpu.VMEM((TOK, HB), BF),
            pltpu.VMEM((TOK, HB), BF),
            pltpu.VMEM((2, TOK, DIM), F32),
            pltpu.VMEM((2, TOK, DIM), F32),
            pltpu.VMEM((HALF, DIM), F32),
            pltpu.VMEM((HALF, DIM), BF),
            pltpu.VMEM((HALF, DIM), BF),
            pltpu.VMEM((2, HALF, DIM), BF),
            pltpu.VMEM((2, HALF, DIM), BF),
            pltpu.VMEM((GTOK, DIM), BF),
            pltpu.VMEM((4, GTOK, WT), BF),
            pltpu.VMEM((N_WT, WT, DIM), F32),
            pltpu.VMEM((8, 128), F32),
            pltpu.VMEM((2, 8, 128), F32),
            dma((W_SLOTS, 2)), dma, dma((2,)), dma((2,)), dma((2,)), dma((2,)), dma((3,)), dma, dma((4,)), dma((N_WT,)), dma((N_WT,)),
            dma((N_MB, 2)), dma((N_MB, 2)), dma((N_MB,)), dma((N_MB,)), dma((2,)), dma((2,)), dma((2, 2)), dma((2, 2)),
            dma((N_MB,)), dma((2,)), dma((8,)), dma((2,)),
        ],
        compiler_params=pltpu.CompilerParams(vmem_limit_bytes=66_000_000, has_side_effects=True),
        name="pipeline",
    )(x_in, tgt, w1, w2)


def tail_kernel(x_all, e_all, a_all, g_all, acc1, acc2, out1, out2, wide, narrow, tile, wide_sem, n_sem, l_sem, s_sem):
    rows = pl.ds(N_GRP * GTOK, GTOK)
    n2 = HID // HB
    n1 = DIM // HB

    def cols(j, width=HB):
        return pl.ds(pl.multiple_of(j * width, width), width)

    def on_tile(t, fn2, fn1):
        @pl.when(t < n2)
        def _():
            fn2(cols(t))

        @pl.when(t >= n2)
        def _():
            fn1(cols(lax.rem(t - n2, n1)), cols((t - n2) // n1, DIM))

    def start_tile(t):
        slot = lax.rem(t, 4)
        n_slot = lax.rem(t, 3)

        def fn2(blk):
            pltpu.make_async_copy(acc2.at[blk, :], tile.at[slot], l_sem.at[slot]).start()
            pltpu.make_async_copy(a_all.at[rows, blk], narrow.at[n_slot], n_sem.at[n_slot]).start()

        def fn1(dblk, half):
            pltpu.make_async_copy(acc1.at[dblk, half], tile.at[slot], l_sem.at[slot]).start()
            pltpu.make_async_copy(x_all.at[rows, dblk], narrow.at[n_slot], n_sem.at[n_slot]).start()

        on_tile(t, fn2, fn1)

    def start_store(t):
        slot = lax.rem(t, 4)

        def fn2(blk):
            pltpu.make_async_copy(tile.at[slot], out2.at[blk, :], s_sem.at[slot]).start()

        def fn1(dblk, half):
            pltpu.make_async_copy(tile.at[slot], out1.at[dblk, half], s_sem.at[slot]).start()

        on_tile(t, fn2, fn1)

    def wait_store(slot):
        pltpu.make_async_copy(tile.at[slot], out2.at[pl.ds(0, HB), :], s_sem.at[slot]).wait()

    def wide_copy(i):
        src = e_all.at[rows, :] if i == 0 else g_all.at[rows, pl.ds((i - 1) * DIM, DIM)]
        return pltpu.make_async_copy(src, wide.at[i], wide_sem.at[i])

    start_tile(0)
    wide_copy(0).start()
    start_tile(1)

    @pl.loop(0, n2 + 2 * n1)
    def _(t):
        slot = lax.rem(t, 4)
        n_slot = lax.rem(t, 3)

        @pl.when(t >= 2)
        def _():
            wait_store(lax.rem(t + 2, 4))

        @pl.when(t + 2 < n2 + 2 * n1)
        def _():
            start_tile(t + 2)

        for i in range(1, 3):

            @pl.when(t == n2 + (i - 1) * n1 - 4)
            def _():
                wide_copy(i).start()

        for i in range(3):

            @pl.when(t == (0 if i == 0 else n2 + (i - 1) * n1))
            def _():
                wide_copy(i).wait()

        pltpu.make_async_copy(a_all.at[rows, pl.ds(0, HB)], narrow.at[n_slot], n_sem.at[n_slot]).wait()
        pltpu.make_async_copy(acc2.at[pl.ds(0, HB), :], tile.at[slot], l_sem.at[slot]).wait()
        which = jnp.where(t < n2, 0, 1 + (t - n2) // n1)
        tile[slot] += dot_tn(narrow[n_slot], wide[which])
        start_store(t)

    wait_store(2)
    wait_store(3)


def add_tail(x_all, e_all, a_all, g_all, acc1, acc2):
    hbm = pl.BlockSpec(memory_space=pl.ANY)
    dma = pltpu.SemaphoreType.DMA
    return pl.pallas_call(
        tail_kernel,
        in_specs=[hbm] * 6,
        out_specs=[hbm] * 2,
        out_shape=[jax.ShapeDtypeStruct(acc1.shape, F32), jax.ShapeDtypeStruct(acc2.shape, F32)],
        scratch_shapes=[
            pltpu.VMEM((3, GTOK, DIM), BF),
            pltpu.VMEM((3, GTOK, HB), BF),
            pltpu.VMEM((4, HB, DIM), F32),
            dma((3,)), dma((3,)), dma((4,)), dma((4,)),
        ],
        compiler_params=pltpu.CompilerParams(vmem_limit_bytes=60_000_000),
        name="tail",
    )(x_all, e_all, a_all, g_all, acc1, acc2)


def solution(mesh):
    def stage_step(inputs, targets, w_in, w_out):
        tokens = N_MB * TOK
        x_in = inputs.reshape(tokens, DIM)
        tgt = targets.reshape(tokens, DIM)
        x_all, e_all, _, a_all, g_all, _, _, _, acc1, acc2, loss = run_pipeline(x_in, tgt, w_in[0, 0], w_out[0, 0])
        grad_in, grad_out = add_tail(x_all, e_all, a_all, g_all, acc1, acc2)
        total = jnp.sum(loss) * (0.5 / N_ELEM)
        return grad_in[None, None], grad_out[None, None], jnp.reshape(total, (1,))

    return jax.shard_map(
        stage_step,
        mesh=mesh,
        in_specs=(P("data", None, None), P("data", None, None), P("stage", None, None, "model"), P("stage", None, "model", None)),
        out_specs=(P(("data", "stage"), None, None, "model"), P(("data", "stage"), None, "model", None), P("data")),
        check_vma=False,
    )
```

```python
import jax
import jax.numpy as jnp
from jax import lax
from jax.experimental import pallas as pl
from jax.experimental.pallas import tpu as pltpu
from jax.sharding import PartitionSpec as P

GELU_COEF = 0.7978845608028654
CUBIC_COEF = 0.044715

N_MB = 24
TOK = 256
HALF = TOK // 2
DIM = 2560
HID = 5120
HB = 512
N_BLK = HID // HB
W_SLOTS = 3
WT = HB // 2
N_WT = 6
GROUP = 4
N_GRP = N_MB // GROUP - 1
GTOK = GROUP * TOK
N_ELEM = N_MB * TOK * DIM
RELAY0 = 3
RELAY3 = 6
LEAD3 = 3
MESH = pl.DeviceIdType.MESH
BF = jnp.bfloat16
F32 = jnp.float32


def dot_nn(a, b):
    return lax.dot_general(a, b, (((1,), (0,)), ((), ())), preferred_element_type=F32)


def dot_nt(a, b):
    return lax.dot_general(a, b, (((1,), (1,)), ((), ())), preferred_element_type=F32)


def dot_tn(a, b):
    return lax.dot_general(a, b, (((0,), (0,)), ((), ())), preferred_element_type=F32)


def gelu(v):
    return 0.5 * v * (1.0 + jnp.tanh(GELU_COEF * (v + CUBIC_COEF * v * v * v)))


def gelu_slope(v):
    t = jnp.tanh(GELU_COEF * (v + CUBIC_COEF * v * v * v))
    return 0.5 * (1.0 + t) + 0.5 * v * (1.0 - t * t) * GELU_COEF * (1.0 + 3.0 * CUBIC_COEF * v * v)


def pipeline_kernel(
    x_in, tgt, w1, w2,
    x_all, e_all, u_all, a_all, g_all, rsf, rsb, fwd, acc1, acc2, loss,
    xbuf, tall, flat, ubuf0, ubuf1, uin0, uin1, qbuf0, qbuf1, mid, accf, accb, rsv, res, tbuf, yf, yb, wide, narrow, wtile, lsum, lrx,
    t_sem, f_sem, x_sem, uo_sem, m_sem, ui_sem, p_sem, wd_sem, wn_sem, wl_sem, ws_sem,
    xr_sem, er_sem, rf_sem, rb_sem, sf_sem, sb_sem, yf_sem, yb_sem, fr_sem, fs_sem, ls_sem, lr_sem,
):
    my = lax.axis_index("model")
    st = lax.axis_index("stage")
    other = 1 - my
    last = st == 3
    first = st == 0
    warm = jnp.where(st == 0, 16, jnp.where(st == 1, 9, jnp.where(st == 2, 5, 2)))
    partner = {"model": other}
    nxt = jnp.minimum(st + 1, 3)
    prv = jnp.maximum(st - 1, 0)

    def rows_of(m, half):
        return pl.ds(pl.multiple_of(m * TOK + half * HALF, HALF), HALF)

    def mb_rows(m):
        return pl.ds(pl.multiple_of(m * TOK, TOK), TOK)

    def half_rows(half):
        return pl.ds(pl.multiple_of(half * HALF, HALF), HALF)

    def cols(j, width=HB):
        return pl.ds(pl.multiple_of(j * width, width), width)

    ubuf, uin, qbuf = (ubuf0, ubuf1), (uin0, uin1), (qbuf0, qbuf1)
    n_back = jnp.where(first, N_BLK, 2 * N_BLK)

    def tall_start(at):
        slot = lax.rem(at, W_SLOTS)
        j = lax.rem(at, 2 * N_BLK)
        i = jnp.maximum(j - N_BLK, 0)

        @pl.when(j < N_BLK)
        def _():
            pltpu.make_async_copy(w1.at[:, cols(j)], tall.at[slot], t_sem.at[slot]).start()

        @pl.when(j >= N_BLK)
        def _():
            pltpu.make_async_copy(w2.at[cols(lax.rem(i, 2), DIM), cols(i // 2)], tall.at[slot], t_sem.at[slot]).start()

    def tall_wait(slot):
        pltpu.make_async_copy(w1.at[:, cols(0)], tall.at[slot], t_sem.at[slot]).wait()

    def flat_start(at):
        slot = lax.rem(at, W_SLOTS)
        j = lax.rem(at, n_back)
        i = jnp.maximum(j - N_BLK, 0)

        @pl.when(j < N_BLK)
        def _():
            pltpu.make_async_copy(w2.at[cols(j), :], flat.at[slot], f_sem.at[slot]).start()

        @pl.when(j >= N_BLK)
        def _():
            pltpu.make_async_copy(w1.at[cols(i // 2), cols(lax.rem(i, 2), DIM)], flat.at[slot], f_sem.at[slot]).start()

    def flat_wait(slot):
        pltpu.make_async_copy(w2.at[cols(0), :], flat.at[slot], f_sem.at[slot]).wait()

    def use(start, wait, at):
        slot = lax.rem(at, W_SLOTS)
        wait(slot)
        start(at + W_SLOTS - 1)
        return slot

    def rs_copy(acc, slot, buf, m, send, recv):
        return pltpu.make_async_remote_copy(
            src_ref=acc.at[slot, half_rows(other), :],
            dst_ref=buf.at[pl.ds(pl.multiple_of(m * HALF, HALF), HALF), :],
            send_sem=send.at[slot],
            recv_sem=recv.at[m],
            device_id=partner,
            device_id_type=MESH,
        )

    def rs_part(acc, slot, buf, m, c, send, recv):
        return pltpu.make_async_remote_copy(
            src_ref=acc.at[slot, half_rows(other), cols(c)],
            dst_ref=buf.at[pl.ds(pl.multiple_of(m * HALF, HALF), HALF), cols(c)],
            send_sem=send.at[slot],
            recv_sem=recv.at[m],
            device_id=partner,
            device_id_type=MESH,
        )

    def half_copy(src, slot, dst, m, half, send, k, recv, dev):
        return pltpu.make_async_remote_copy(
            src_ref=src.at[slot],
            dst_ref=dst.at[rows_of(m, half), :],
            send_sem=send.at[slot, k],
            recv_sem=recv.at[m, half],
            device_id=dev,
            device_id_type=MESH,
        )

    def yf_pair(m, slot):
        return (
            half_copy(yf, slot, x_all, m, my, yf_sem, 0, xr_sem, {"model": my, "stage": nxt}),
            half_copy(yf, slot, x_all, m, my, yf_sem, 1, xr_sem, {"model": other, "stage": nxt}),
        )

    def fwd_rows(m):
        return pl.ds(pl.multiple_of(m * HALF, HALF), HALF)

    def fwd_send(m, slot):
        return pltpu.make_async_remote_copy(
            src_ref=yf.at[slot],
            dst_ref=fwd.at[fwd_rows(m), :],
            send_sem=yf_sem.at[slot, 1],
            recv_sem=fr_sem.at[m],
            device_id=partner,
            device_id_type=MESH,
        )

    def relay_copy(m, dst, recv, to):
        return pltpu.make_async_remote_copy(
            src_ref=fwd.at[fwd_rows(m), :],
            dst_ref=dst.at[rows_of(m, other), :],
            send_sem=fs_sem.at[lax.rem(m, 2)],
            recv_sem=recv.at[m, other],
            device_id={"model": my, "stage": to},
            device_id_type=MESH,
        )

    def relay_x(m):
        return relay_copy(m, x_all, xr_sem, 2)

    def relay_e(m):
        return relay_copy(m, e_all, er_sem, 2)

    def far_send(m, slot):
        return pltpu.make_async_remote_copy(
            src_ref=yb.at[slot],
            dst_ref=fwd.at[fwd_rows(m), :],
            send_sem=yb_sem.at[slot, 1],
            recv_sem=fr_sem.at[m],
            device_id={"model": other, "stage": 0},
            device_id_type=MESH,
        )

    def yl_own(m, slot):
        return pltpu.make_async_copy(yf.at[slot], e_all.at[rows_of(m, my), :], er_sem.at[m, my])

    def yl_send(m, slot):
        return half_copy(yf, slot, e_all, m, my, yf_sem, 1, er_sem, partner)

    def yb_pair(m, slot):
        return (
            half_copy(yb, slot, e_all, m, my, yb_sem, 0, er_sem, {"model": my, "stage": prv}),
            half_copy(yb, slot, e_all, m, my, yb_sem, 1, er_sem, {"model": other, "stage": prv}),
        )

    def wait_in(dst, m, recv):
        for half in range(2):
            ref = dst.at[rows_of(m, half), :]
            pltpu.make_async_copy(ref, ref, recv.at[m, half]).wait()

    def out_copy(buf, slot, dst, m, j, sem):
        return pltpu.make_async_copy(buf[slot], dst.at[mb_rows(m), cols(j)], sem.at[slot])

    def mid_copy(dst, m):
        return pltpu.make_async_copy(mid, dst.at[mb_rows(m), :], m_sem)

    def u_load(m, j, slot):
        return pltpu.make_async_copy(u_all.at[mb_rows(m), cols(j)], uin[slot], ui_sem.at[slot])

    def load_x(src, m, also=None):
        cp = pltpu.make_async_copy(src.at[mb_rows(m), :], xbuf, x_sem)
        cp.start()
        if also is not None:
            also()
        cp.wait()

    def forward(m, also):
        slot_m = lax.rem(m, 2)
        base = m * 2 * N_BLK

        @pl.when(first)
        def _():
            load_x(x_in, m)

            @pl.when(m >= N_GRP * GROUP)
            def _():
                cp = pltpu.make_async_copy(xbuf, x_all.at[mb_rows(m), :], x_sem)
                cp.start()
                cp.wait()

        @pl.when(jnp.logical_not(first))
        def _():
            wait_in(x_all, m, xr_sem)
            load_x(x_all, m, also)

        @pl.when(m >= 2)
        def _():
            rs_copy(accf, slot_m, rsf, m - 2, sf_sem, rf_sem).wait_send()

        def activate(j, slot):
            mid[:, cols(j)] = gelu(ubuf[slot][...].astype(F32)).astype(BF)

        def block(j, slot):
            ws = use(tall_start, tall_wait, base + j)

            @pl.when(j >= 2)
            def _():
                out_copy(ubuf, slot, u_all, m, j, uo_sem).wait()

            ubuf[slot][...] = dot_nn(xbuf[...], tall[ws]).astype(BF)
            if not (isinstance(j, int) and j == 0):
                activate(j - 1, 1 - slot)
            out_copy(ubuf, slot, u_all, m, j, uo_sem).start()

        block(0, 0)

        @pl.loop(0, (N_BLK - 2) // 2)
        def _(i):
            block(2 * i + 1, 1)
            block(2 * i + 2, 0)

        block(N_BLK - 1, 1)
        activate(N_BLK - 1, 1)
        mid_copy(a_all, m).start()

        @pl.loop(0, DIM // HB)
        def _(c):
            ws = use(tall_start, tall_wait, base + N_BLK + 2 * c)
            accf[slot_m, :, cols(c)] = dot_nn(mid[:, 0:DIM], tall[ws])
            ws = use(tall_start, tall_wait, base + N_BLK + 2 * c + 1)
            accf[slot_m, :, cols(c)] += dot_nn(mid[:, DIM:HID], tall[ws])
            rs_part(accf, slot_m, rsf, m, c, sf_sem, rf_sem).start()

        for slot in range(2):
            out_copy(ubuf, slot, u_all, m, slot, uo_sem).wait()
        mid_copy(a_all, m).wait()

    def load_post(acc_buf, m, recv, src):
        ref = acc_buf.at[pl.ds(pl.multiple_of(m * HALF, HALF), HALF), :]
        pltpu.make_async_copy(ref, ref, recv.at[m]).wait()
        a = pltpu.make_async_copy(ref, rsv, p_sem.at[0])
        a.start()
        b = pltpu.make_async_copy(src.at[rows_of(m, my), :], res, p_sem.at[1])
        b.start()
        return a, b

    def forward_post(m):
        slot = lax.rem(m, 2)

        def run(src):
            t = pltpu.make_async_copy(tgt.at[rows_of(m, my), :], tbuf, p_sem.at[2])
            t.start()
            for cp in load_post(rsf, m, rf_sem, src):
                cp.wait()
            t.wait()

        @pl.when(first)
        def _():
            run(x_in)

        @pl.when(jnp.logical_not(first))
        def _():
            run(x_all)

        @pl.when(m >= 2)
        def _():
            @pl.when(last)
            def _():
                yl_send(m, slot).wait_send()

            @pl.when(jnp.logical_not(last))
            def _():
                for cp in yf_pair(m, slot):
                    cp.wait_send()

        y = (res[...].astype(F32) + (accf[slot, half_rows(my), :] + rsv[...])).astype(BF)

        @pl.when(jnp.logical_not(last))
        def _():
            yf[slot] = y
            own, cross = yf_pair(m, slot)
            own.start()
            by_pair = jnp.logical_and(st == 1, m >= RELAY0)

            @pl.when(by_pair)
            def _():
                fwd_send(m, slot).start()

            @pl.when(jnp.logical_not(by_pair))
            def _():
                cross.start()

        @pl.when(last)
        def _():
            err = y.astype(F32) - tbuf[...].astype(F32)
            yf[slot] = (err * (1.0 / N_ELEM)).astype(BF)
            sq = err * err
            part = sq[:, 0:128]
            for c in range(1, DIM // 128):
                part = part + sq[:, c * 128 : (c + 1) * 128]
            lsum[...] += jnp.sum(part.reshape(HALF // 8, 8, 128), axis=0)
            yl_own(m, slot).start()
            yl_send(m, slot).start()

            @pl.when(m == N_MB - 1)
            def _():
                pltpu.make_async_copy(lsum, lrx.at[my], lr_sem.at[my]).start()
                for cond, cp in loss_sends():
                    pl.when(cond)(cp.start)

    def pass_on(m, base, copy):
        ref = fwd.at[fwd_rows(m), :]
        pltpu.make_async_copy(ref, ref, fr_sem.at[m]).wait()

        @pl.when(m >= base + 2)
        def _():
            copy(m - 2).wait_send()

        copy(m).start()

    def relay(m):
        @pl.when(jnp.logical_and(st == 1, jnp.logical_and(m >= RELAY0, m < N_MB)))
        def _():
            pass_on(m, RELAY0, relay_x)

    def relay_back(m):
        @pl.when(jnp.logical_and(first, jnp.logical_and(m >= RELAY3, m < N_MB)))
        def _():
            pass_on(m, RELAY3, relay_e)

    def loss_sends():
        for y in range(2):
            for s in range(4):
                cp = pltpu.make_async_remote_copy(
                    src_ref=lsum,
                    dst_ref=lrx.at[my],
                    send_sem=ls_sem.at[y * 4 + s],
                    recv_sem=lr_sem.at[my],
                    device_id={"model": y, "stage": s},
                    device_id_type=MESH,
                )
                yield (True if s < 3 else my != y), cp

    def backward(m):
        slot_m = lax.rem(m, 2)
        base = m * n_back
        wait_in(e_all, m, er_sem)
        load_x(e_all, m)

        @pl.when(jnp.logical_and(m >= 2, jnp.logical_not(first)))
        def _():
            rs_copy(accb, slot_m, rsb, m - 2, sb_sem, rb_sem).wait_send()

        def slope(j, slot):
            mid[:, cols(j)] = (gelu_slope(uin[slot][...].astype(F32)) * qbuf[slot][...].astype(F32)).astype(BF)

        def block(j, slot):
            start = isinstance(j, int) and j == 0
            ws = use(flat_start, flat_wait, base + j)
            u_load(m, j, slot).start()
            if not start:
                u_load(m, j - 1, 1 - slot).wait()
            qbuf[slot][...] = dot_nt(xbuf[...], flat[ws]).astype(BF)
            if not start:
                slope(j - 1, 1 - slot)

        block(0, 0)

        @pl.loop(0, (N_BLK - 2) // 2)
        def _(i):
            block(2 * i + 1, 1)
            block(2 * i + 2, 0)

        block(N_BLK - 1, 1)
        u_load(m, N_BLK - 1, 1).wait()
        slope(N_BLK - 1, 1)
        mid_copy(g_all, m).start()

        @pl.when(jnp.logical_not(first))
        def _():
            @pl.loop(0, DIM // HB)
            def _(c):
                ws = use(flat_start, flat_wait, base + N_BLK + 2 * c)
                accb[slot_m, :, cols(c)] = dot_nt(mid[:, 0:DIM], flat[ws])
                ws = use(flat_start, flat_wait, base + N_BLK + 2 * c + 1)
                accb[slot_m, :, cols(c)] += dot_nt(mid[:, DIM:HID], flat[ws])
                rs_part(accb, slot_m, rsb, m, c, sb_sem, rb_sem).start()

        mid_copy(g_all, m).wait()

    def backward_post(m):
        slot = lax.rem(m, 2)
        for cp in load_post(rsb, m, rb_sem, e_all):
            cp.wait()

        @pl.when(m >= 2)
        def _():
            for cp in yb_pair(m, slot):
                cp.wait_send()

        yb[slot] = (res[...].astype(F32) + (accb[slot, half_rows(my), :] + rsv[...])).astype(BF)
        own, cross = yb_pair(m, slot)
        own.start()
        far = jnp.logical_and(last, m >= RELAY3)

        @pl.when(far)
        def _():
            far_send(m, slot).start()

        @pl.when(jnp.logical_not(far))
        def _():
            cross.start()

    def weight_ops(v):
        grp = v // GROUP
        quart = lax.rem(v, GROUP)
        rows = pl.ds(pl.multiple_of(grp * GTOK, GTOK), GTOK)
        out2 = quart < 2

        def on_tile(t, fn2, fn1):
            @pl.when(out2)
            def _():
                fn2(cols(quart * (HID // WT // 2) + t, WT))

            @pl.when(jnp.logical_not(out2))
            def _():
                fn1(cols(t, WT), cols(quart - 2, DIM))

        def start_tile(t):
            n_slot = lax.rem(t, 4)
            slot = lax.rem(t, N_WT)

            def fn2(blk):
                pltpu.make_async_copy(a_all.at[rows, blk], narrow.at[n_slot], wn_sem.at[n_slot]).start()

                @pl.when(grp > 0)
                def _():
                    pltpu.make_async_copy(acc2.at[blk, :], wtile.at[slot], wl_sem.at[slot]).start()

            def fn1(dblk, half):
                @pl.when(first)
                def _():
                    pltpu.make_async_copy(x_in.at[rows, dblk], narrow.at[n_slot], wn_sem.at[n_slot]).start()

                @pl.when(jnp.logical_not(first))
                def _():
                    pltpu.make_async_copy(x_all.at[rows, dblk], narrow.at[n_slot], wn_sem.at[n_slot]).start()

                @pl.when(grp > 0)
                def _():
                    pltpu.make_async_copy(acc1.at[dblk, half], wtile.at[slot], wl_sem.at[slot]).start()

            on_tile(t, fn2, fn1)

        def start_store(t):
            slot = lax.rem(t, N_WT)

            def fn2(blk):
                pltpu.make_async_copy(wtile.at[slot], acc2.at[blk, :], ws_sem.at[slot]).start()

            def fn1(dblk, half):
                pltpu.make_async_copy(wtile.at[slot], acc1.at[dblk, half], ws_sem.at[slot]).start()

            on_tile(t, fn2, fn1)

        def wait_store(slot):
            pltpu.make_async_copy(wtile.at[slot], acc2.at[pl.ds(0, WT), :], ws_sem.at[slot]).wait()

        def start():
            @pl.when(out2)
            def _():
                pltpu.make_async_copy(e_all.at[rows, :], wide, wd_sem).start()

            @pl.when(jnp.logical_not(out2))
            def _():
                pltpu.make_async_copy(g_all.at[rows, cols(quart - 2, DIM)], wide, wd_sem).start()

            for t in range(N_WT // 2):
                start_tile(t)

        n_tiles = DIM // WT

        def run(low, high):
            if low == 0:
                pltpu.make_async_copy(e_all.at[rows, :], wide, wd_sem).wait()

            @pl.loop(low, high)
            def _(t):
                slot = lax.rem(t, N_WT)
                n_slot = lax.rem(t, 4)

                @pl.when(t >= N_WT // 2)
                def _():
                    wait_store(lax.rem(t + N_WT // 2, N_WT))

                @pl.when(t + N_WT // 2 < n_tiles)
                def _():
                    start_tile(t + N_WT // 2)

                pltpu.make_async_copy(a_all.at[rows, pl.ds(0, WT)], narrow.at[n_slot], wn_sem.at[n_slot]).wait()

                @pl.when(grp > 0)
                def _():
                    pltpu.make_async_copy(acc2.at[pl.ds(0, WT), :], wtile.at[slot], wl_sem.at[slot]).wait()

                @pl.when(grp == 0)
                def _():
                    wtile[slot] = jnp.zeros((WT, DIM), F32)

                wtile[slot] += dot_tn(narrow[n_slot], wide[...])
                start_store(t)

            if high == n_tiles:
                for t in range(n_tiles - N_WT // 2, n_tiles):
                    wait_store(t % N_WT)

        return start, run

    lsum[...] = jnp.zeros((8, 128), F32)
    for j in range(W_SLOTS - 1):
        tall_start(j)
        flat_start(j)

    @pl.loop(0, N_MB + warm)
    def _(k):
        b = k - warm
        p = k - 1
        v = b - GROUP
        b_on = b >= 0
        f_on = k < N_MB
        p_on = jnp.logical_and(p >= 0, p < N_MB)
        pb_on = jnp.logical_and(b_on, jnp.logical_not(first))
        w_on = jnp.logical_and(v >= 0, jnp.logical_not(first))

        @pl.when(jnp.logical_and(first, v >= 0))
        def _():
            start, run = weight_ops(v)
            start()
            run(0, DIM // WT)

        @pl.when(b_on)
        def _():
            backward(b)
            relay_back(b + LEAD3)

        @pl.when(jnp.logical_and(b_on, p_on))
        def _():
            forward_post(p)

        @pl.when(b_on)
        def _():
            relay(k - 2)

        @pl.when(jnp.logical_and(w_on, jnp.logical_not(f_on)))
        def _():
            weight_ops(v)[0]()

        @pl.when(f_on)
        def _():
            forward(k, lambda: pl.when(w_on)(weight_ops(v)[0]))

        @pl.when(jnp.logical_and(jnp.logical_not(b_on), p_on))
        def _():
            forward_post(p)

        @pl.when(jnp.logical_not(b_on))
        def _():
            relay(k - 2)

        @pl.when(pb_on)
        def _():
            backward_post(b)

        @pl.when(w_on)
        def _():
            weight_ops(v)[1](0, DIM // WT)

    for half in range(2):
        pltpu.make_async_copy(lsum, lrx.at[half], lr_sem.at[half]).wait()
    loss[...] = lrx[0] + lrx[1]

    for j in range(W_SLOTS - 1):
        tall_wait(j)
        flat_wait(j)
    for m in (N_MB - 2, N_MB - 1):
        slot = m % 2
        rs_copy(accf, slot, rsf, m, sf_sem, rf_sem).wait_send()

        @pl.when(jnp.logical_not(first))
        def _():
            rs_copy(accb, slot, rsb, m, sb_sem, rb_sem).wait_send()
            for cp in yb_pair(m, slot):
                cp.wait_send()

        @pl.when(last)
        def _():
            yl_send(m, slot).wait_send()

        @pl.when(jnp.logical_not(last))
        def _():
            for cp in yf_pair(m, slot):
                cp.wait_send()

        @pl.when(st == 1)
        def _():
            relay_x(m).wait_send()

        @pl.when(first)
        def _():
            relay_e(m).wait_send()

    @pl.when(last)
    def _():
        for cond, cp in loss_sends():
            pl.when(cond)(cp.wait_send)


def run_pipeline(x_in, tgt, w1, w2):
    tokens = N_MB * TOK
    hbm = pl.BlockSpec(memory_space=pl.ANY)
    dma = pltpu.SemaphoreType.DMA
    shapes = [
        ((tokens, DIM), BF), ((tokens, DIM), BF),
        ((tokens, HID), BF), ((tokens, HID), BF), ((tokens, HID), BF),
        ((tokens // 2, DIM), F32), ((tokens // 2, DIM), F32), ((tokens // 2, DIM), BF),
        ((DIM, HID), F32), ((HID, DIM), F32),
    ]
    out_shape = [jax.ShapeDtypeStruct(s, d) for s, d in shapes] + [jax.ShapeDtypeStruct((8, 128), F32)]
    return pl.pallas_call(
        pipeline_kernel,
        out_shape=out_shape,
        in_specs=[hbm] * 4,
        out_specs=[hbm] * 10 + [pl.BlockSpec(memory_space=pltpu.VMEM)],
        scratch_shapes=[
            pltpu.VMEM((TOK, DIM), BF),
            pltpu.VMEM((W_SLOTS, DIM, HB), BF),
            pltpu.VMEM((W_SLOTS, HB, DIM), BF),
            pltpu.VMEM((TOK, HB), BF), pltpu.VMEM((TOK, HB), BF),
            pltpu.VMEM((TOK, HB), BF), pltpu.VMEM((TOK, HB), BF),
            pltpu.VMEM((TOK, HB), BF), pltpu.VMEM((TOK, HB), BF),
            pltpu.VMEM((TOK, HID), BF),
            pltpu.VMEM((2, TOK, DIM), F32),
            pltpu.VMEM((2, TOK, DIM), F32),
            pltpu.VMEM((HALF, DIM), F32),
            pltpu.VMEM((HALF, DIM), BF),
            pltpu.VMEM((HALF, DIM), BF),
            pltpu.VMEM((2, HALF, DIM), BF),
            pltpu.VMEM((2, HALF, DIM), BF),
            pltpu.VMEM((GTOK, DIM), BF),
            pltpu.VMEM((4, GTOK, WT), BF),
            pltpu.VMEM((N_WT, WT, DIM), F32),
            pltpu.VMEM((8, 128), F32),
            pltpu.VMEM((2, 8, 128), F32),
            dma((W_SLOTS,)), dma((W_SLOTS,)), dma, dma((2,)), dma, dma((2,)), dma((3,)), dma, dma((4,)), dma((N_WT,)), dma((N_WT,)),
            dma((N_MB, 2)), dma((N_MB, 2)), dma((N_MB,)), dma((N_MB,)), dma((2,)), dma((2,)), dma((2, 2)), dma((2, 2)),
            dma((N_MB,)), dma((2,)), dma((8,)), dma((2,)),
        ],
        compiler_params=pltpu.CompilerParams(vmem_limit_bytes=66_000_000, has_side_effects=True),
        name="pipeline",
    )(x_in, tgt, w1, w2)


def tail_kernel(x_all, e_all, a_all, g_all, acc1, acc2, out1, out2, wide, narrow, tile, wide_sem, n_sem, l_sem, s_sem):
    rows = pl.ds(N_GRP * GTOK, GTOK)
    n2 = HID // HB
    n1 = DIM // HB

    def cols(j, width=HB):
        return pl.ds(pl.multiple_of(j * width, width), width)

    def on_tile(t, fn2, fn1):
        @pl.when(t < n2)
        def _():
            fn2(cols(t))

        @pl.when(t >= n2)
        def _():
            fn1(cols(lax.rem(t - n2, n1)), cols((t - n2) // n1, DIM))

    def start_tile(t):
        slot = lax.rem(t, 4)
        n_slot = lax.rem(t, 3)

        def fn2(blk):
            pltpu.make_async_copy(acc2.at[blk, :], tile.at[slot], l_sem.at[slot]).start()
            pltpu.make_async_copy(a_all.at[rows, blk], narrow.at[n_slot], n_sem.at[n_slot]).start()

        def fn1(dblk, half):
            pltpu.make_async_copy(acc1.at[dblk, half], tile.at[slot], l_sem.at[slot]).start()
            pltpu.make_async_copy(x_all.at[rows, dblk], narrow.at[n_slot], n_sem.at[n_slot]).start()

        on_tile(t, fn2, fn1)

    def start_store(t):
        slot = lax.rem(t, 4)

        def fn2(blk):
            pltpu.make_async_copy(tile.at[slot], out2.at[blk, :], s_sem.at[slot]).start()

        def fn1(dblk, half):
            pltpu.make_async_copy(tile.at[slot], out1.at[dblk, half], s_sem.at[slot]).start()

        on_tile(t, fn2, fn1)

    def wait_store(slot):
        pltpu.make_async_copy(tile.at[slot], out2.at[pl.ds(0, HB), :], s_sem.at[slot]).wait()

    def wide_copy(i):
        src = e_all.at[rows, :] if i == 0 else g_all.at[rows, pl.ds((i - 1) * DIM, DIM)]
        return pltpu.make_async_copy(src, wide.at[i], wide_sem.at[i])

    start_tile(0)
    wide_copy(0).start()
    start_tile(1)

    @pl.loop(0, n2 + 2 * n1)
    def _(t):
        slot = lax.rem(t, 4)
        n_slot = lax.rem(t, 3)

        @pl.when(t >= 2)
        def _():
            wait_store(lax.rem(t + 2, 4))

        @pl.when(t + 2 < n2 + 2 * n1)
        def _():
            start_tile(t + 2)

        for i in range(1, 3):

            @pl.when(t == n2 + (i - 1) * n1 - 4)
            def _():
                wide_copy(i).start()

        for i in range(3):

            @pl.when(t == (0 if i == 0 else n2 + (i - 1) * n1))
            def _():
                wide_copy(i).wait()

        pltpu.make_async_copy(a_all.at[rows, pl.ds(0, HB)], narrow.at[n_slot], n_sem.at[n_slot]).wait()
        pltpu.make_async_copy(acc2.at[pl.ds(0, HB), :], tile.at[slot], l_sem.at[slot]).wait()
        which = jnp.where(t < n2, 0, 1 + (t - n2) // n1)
        tile[slot] += dot_tn(narrow[n_slot], wide[which])
        start_store(t)

    wait_store(2)
    wait_store(3)


def add_tail(x_all, e_all, a_all, g_all, acc1, acc2):
    hbm = pl.BlockSpec(memory_space=pl.ANY)
    dma = pltpu.SemaphoreType.DMA
    return pl.pallas_call(
        tail_kernel,
        in_specs=[hbm] * 6,
        out_specs=[hbm] * 2,
        out_shape=[jax.ShapeDtypeStruct(acc1.shape, F32), jax.ShapeDtypeStruct(acc2.shape, F32)],
        scratch_shapes=[
            pltpu.VMEM((3, GTOK, DIM), BF),
            pltpu.VMEM((3, GTOK, HB), BF),
            pltpu.VMEM((4, HB, DIM), F32),
            dma((3,)), dma((3,)), dma((4,)), dma((4,)),
        ],
        compiler_params=pltpu.CompilerParams(vmem_limit_bytes=60_000_000),
        name="tail",
    )(x_all, e_all, a_all, g_all, acc1, acc2)


def solution(mesh):
    def stage_step(inputs, targets, w_in, w_out):
        tokens = N_MB * TOK
        x_in = inputs.reshape(tokens, DIM)
        tgt = targets.reshape(tokens, DIM)
        x_all, e_all, _, a_all, g_all, _, _, _, acc1, acc2, loss = run_pipeline(x_in, tgt, w_in[0, 0], w_out[0, 0])
        grad_in, grad_out = add_tail(x_all, e_all, a_all, g_all, acc1, acc2)
        total = jnp.sum(loss) * (0.5 / N_ELEM)
        return grad_in[None, None], grad_out[None, None], jnp.reshape(total, (1,))

    return jax.shard_map(
        stage_step,
        mesh=mesh,
        in_specs=(P("data", None, None), P("data", None, None), P("stage", None, None, "model"), P("stage", None, "model", None)),
        out_specs=(P(("data", "stage"), None, None, "model"), P(("data", "stage"), None, "model", None), P("data")),
        check_vma=False,
    )
```

```python
import jax
import jax.numpy as jnp
from jax import lax
from jax.experimental import pallas as pl
from jax.experimental.pallas import tpu as pltpu
from jax.sharding import PartitionSpec as P

GELU_COEF = 0.7978845608028654
CUBIC_COEF = 0.044715

N_MB = 24
TOK = 256
HALF = TOK // 2
DIM = 2560
HID = 5120
HB = 512
N_BLK = HID // HB
W_SLOTS = 4
WT = HB // 2
N_WT = 6
GROUP = 4
N_GRP = N_MB // GROUP - 1
GTOK = GROUP * TOK
N_ELEM = N_MB * TOK * DIM
RELAY0 = 3
RELAY3 = 6
LEAD3 = 3
MESH = pl.DeviceIdType.MESH
BF = jnp.bfloat16
F32 = jnp.float32


def dot_nn(a, b):
    return lax.dot_general(a, b, (((1,), (0,)), ((), ())), preferred_element_type=F32)


def dot_nt(a, b):
    return lax.dot_general(a, b, (((1,), (1,)), ((), ())), preferred_element_type=F32)


def dot_tn(a, b):
    return lax.dot_general(a, b, (((0,), (0,)), ((), ())), preferred_element_type=F32)


def gelu(v):
    return 0.5 * v * (1.0 + jnp.tanh(GELU_COEF * (v + CUBIC_COEF * v * v * v)))


def gelu_slope(v):
    t = jnp.tanh(GELU_COEF * (v + CUBIC_COEF * v * v * v))
    return 0.5 * (1.0 + t) + 0.5 * v * (1.0 - t * t) * GELU_COEF * (1.0 + 3.0 * CUBIC_COEF * v * v)


def pipeline_kernel(
    x_in, tgt, w1, w2,
    x_all, e_all, u_all, a_all, g_all, rsf, rsb, fwd, acc1, acc2, loss,
    xbuf, tall, flat, ubuf0, ubuf1, uin0, uin1, qbuf0, qbuf1, mid, accf, accb, rsv, res, tbuf, yf, yb, wide, narrow, wtile, lsum, lrx,
    t_sem, f_sem, x_sem, uo_sem, m_sem, ui_sem, p_sem, wd_sem, wn_sem, wl_sem, ws_sem,
    xr_sem, er_sem, rf_sem, rb_sem, sf_sem, sb_sem, yf_sem, yb_sem, fr_sem, fs_sem, ls_sem, lr_sem,
):
    my = lax.axis_index("model")
    st = lax.axis_index("stage")
    other = 1 - my
    last = st == 3
    first = st == 0
    warm = jnp.where(st == 0, 16, jnp.where(st == 1, 9, jnp.where(st == 2, 5, 2)))
    partner = {"model": other}
    nxt = jnp.minimum(st + 1, 3)
    prv = jnp.maximum(st - 1, 0)

    def rows_of(m, half):
        return pl.ds(pl.multiple_of(m * TOK + half * HALF, HALF), HALF)

    def mb_rows(m):
        return pl.ds(pl.multiple_of(m * TOK, TOK), TOK)

    def half_rows(half):
        return pl.ds(pl.multiple_of(half * HALF, HALF), HALF)

    def cols(j, width=HB):
        return pl.ds(pl.multiple_of(j * width, width), width)

    ubuf, uin, qbuf = (ubuf0, ubuf1), (uin0, uin1), (qbuf0, qbuf1)
    n_back = jnp.where(first, N_BLK, 2 * N_BLK)

    def tall_start(at):
        slot = lax.rem(at, W_SLOTS)
        j = lax.rem(at, 2 * N_BLK)
        i = jnp.maximum(j - N_BLK, 0)

        @pl.when(j < N_BLK)
        def _():
            pltpu.make_async_copy(w1.at[:, cols(j)], tall.at[slot], t_sem.at[slot]).start()

        @pl.when(j >= N_BLK)
        def _():
            pltpu.make_async_copy(w2.at[cols(lax.rem(i, 2), DIM), cols(i // 2)], tall.at[slot], t_sem.at[slot]).start()

    def tall_wait(slot):
        pltpu.make_async_copy(w1.at[:, cols(0)], tall.at[slot], t_sem.at[slot]).wait()

    def flat_start(at):
        slot = lax.rem(at, W_SLOTS)
        j = lax.rem(at, n_back)
        i = jnp.maximum(j - N_BLK, 0)

        @pl.when(j < N_BLK)
        def _():
            pltpu.make_async_copy(w2.at[cols(j), :], flat.at[slot], f_sem.at[slot]).start()

        @pl.when(j >= N_BLK)
        def _():
            pltpu.make_async_copy(w1.at[cols(i // 2), cols(lax.rem(i, 2), DIM)], flat.at[slot], f_sem.at[slot]).start()

    def flat_wait(slot):
        pltpu.make_async_copy(w2.at[cols(0), :], flat.at[slot], f_sem.at[slot]).wait()

    def use(start, wait, at):
        slot = lax.rem(at, W_SLOTS)
        wait(slot)
        start(at + W_SLOTS - 1)
        return slot

    def rs_copy(acc, slot, buf, m, send, recv):
        return pltpu.make_async_remote_copy(
            src_ref=acc.at[slot, half_rows(other), :],
            dst_ref=buf.at[pl.ds(pl.multiple_of(m * HALF, HALF), HALF), :],
            send_sem=send.at[slot],
            recv_sem=recv.at[m],
            device_id=partner,
            device_id_type=MESH,
        )

    def rs_part(acc, slot, buf, m, c, send, recv):
        return pltpu.make_async_remote_copy(
            src_ref=acc.at[slot, half_rows(other), cols(c)],
            dst_ref=buf.at[pl.ds(pl.multiple_of(m * HALF, HALF), HALF), cols(c)],
            send_sem=send.at[slot],
            recv_sem=recv.at[m],
            device_id=partner,
            device_id_type=MESH,
        )

    def half_copy(src, slot, dst, m, half, send, k, recv, dev):
        return pltpu.make_async_remote_copy(
            src_ref=src.at[slot],
            dst_ref=dst.at[rows_of(m, half), :],
            send_sem=send.at[slot, k],
            recv_sem=recv.at[m, half],
            device_id=dev,
            device_id_type=MESH,
        )

    def yf_pair(m, slot):
        return (
            half_copy(yf, slot, x_all, m, my, yf_sem, 0, xr_sem, {"model": my, "stage": nxt}),
            half_copy(yf, slot, x_all, m, my, yf_sem, 1, xr_sem, {"model": other, "stage": nxt}),
        )

    def fwd_rows(m):
        return pl.ds(pl.multiple_of(m * HALF, HALF), HALF)

    def fwd_send(m, slot):
        return pltpu.make_async_remote_copy(
            src_ref=yf.at[slot],
            dst_ref=fwd.at[fwd_rows(m), :],
            send_sem=yf_sem.at[slot, 1],
            recv_sem=fr_sem.at[m],
            device_id=partner,
            device_id_type=MESH,
        )

    def relay_copy(m, dst, recv, to):
        return pltpu.make_async_remote_copy(
            src_ref=fwd.at[fwd_rows(m), :],
            dst_ref=dst.at[rows_of(m, other), :],
            send_sem=fs_sem.at[lax.rem(m, 2)],
            recv_sem=recv.at[m, other],
            device_id={"model": my, "stage": to},
            device_id_type=MESH,
        )

    def relay_x(m):
        return relay_copy(m, x_all, xr_sem, 2)

    def relay_e(m):
        return relay_copy(m, e_all, er_sem, 2)

    def far_send(m, slot):
        return pltpu.make_async_remote_copy(
            src_ref=yb.at[slot],
            dst_ref=fwd.at[fwd_rows(m), :],
            send_sem=yb_sem.at[slot, 1],
            recv_sem=fr_sem.at[m],
            device_id={"model": other, "stage": 0},
            device_id_type=MESH,
        )

    def yl_own(m, slot):
        return pltpu.make_async_copy(yf.at[slot], e_all.at[rows_of(m, my), :], er_sem.at[m, my])

    def yl_send(m, slot):
        return half_copy(yf, slot, e_all, m, my, yf_sem, 1, er_sem, partner)

    def yb_pair(m, slot):
        return (
            half_copy(yb, slot, e_all, m, my, yb_sem, 0, er_sem, {"model": my, "stage": prv}),
            half_copy(yb, slot, e_all, m, my, yb_sem, 1, er_sem, {"model": other, "stage": prv}),
        )

    def wait_in(dst, m, recv):
        for half in range(2):
            ref = dst.at[rows_of(m, half), :]
            pltpu.make_async_copy(ref, ref, recv.at[m, half]).wait()

    def out_copy(buf, slot, dst, m, j, sem):
        return pltpu.make_async_copy(buf[slot], dst.at[mb_rows(m), cols(j)], sem.at[slot])

    def mid_copy(dst, m):
        return pltpu.make_async_copy(mid, dst.at[mb_rows(m), :], m_sem)

    def u_load(m, j, slot):
        return pltpu.make_async_copy(u_all.at[mb_rows(m), cols(j)], uin[slot], ui_sem.at[slot])

    def load_x(src, m, also=None):
        cp = pltpu.make_async_copy(src.at[mb_rows(m), :], xbuf, x_sem)
        cp.start()
        if also is not None:
            also()
        cp.wait()

    def forward(m, also):
        slot_m = lax.rem(m, 2)
        base = m * 2 * N_BLK

        @pl.when(first)
        def _():
            load_x(x_in, m)

            @pl.when(m >= N_GRP * GROUP)
            def _():
                cp = pltpu.make_async_copy(xbuf, x_all.at[mb_rows(m), :], x_sem)
                cp.start()
                cp.wait()

        @pl.when(jnp.logical_not(first))
        def _():
            with jax.named_scope('fwait'):
                wait_in(x_all, m, xr_sem)
            with jax.named_scope('fload'):
                load_x(x_all, m, also)

        @pl.when(m >= 2)
        def _():
            rs_copy(accf, slot_m, rsf, m - 2, sf_sem, rf_sem).wait_send()

        def activate(j, slot):
            mid[:, cols(j)] = gelu(ubuf[slot][...].astype(F32)).astype(BF)

        def block(j, slot):
            ws = use(tall_start, tall_wait, base + j)

            @pl.when(j >= 2)
            def _():
                out_copy(ubuf, slot, u_all, m, j, uo_sem).wait()

            ubuf[slot][...] = dot_nn(xbuf[...], tall[ws]).astype(BF)
            if not (isinstance(j, int) and j == 0):
                activate(j - 1, 1 - slot)
            out_copy(ubuf, slot, u_all, m, j, uo_sem).start()

        block(0, 0)

        @pl.loop(0, (N_BLK - 2) // 2)
        def _(i):
            block(2 * i + 1, 1)
            block(2 * i + 2, 0)

        block(N_BLK - 1, 1)
        activate(N_BLK - 1, 1)
        mid_copy(a_all, m).start()

        @pl.loop(0, DIM // HB)
        def _(c):
            ws = use(tall_start, tall_wait, base + N_BLK + 2 * c)
            accf[slot_m, :, cols(c)] = dot_nn(mid[:, 0:DIM], tall[ws])
            ws = use(tall_start, tall_wait, base + N_BLK + 2 * c + 1)
            accf[slot_m, :, cols(c)] += dot_nn(mid[:, DIM:HID], tall[ws])
            rs_part(accf, slot_m, rsf, m, c, sf_sem, rf_sem).start()

        for slot in range(2):
            out_copy(ubuf, slot, u_all, m, slot, uo_sem).wait()
        mid_copy(a_all, m).wait()

    def load_post(acc_buf, m, recv, src):
        ref = acc_buf.at[pl.ds(pl.multiple_of(m * HALF, HALF), HALF), :]
        with jax.named_scope('pwait'):
            pltpu.make_async_copy(ref, ref, recv.at[m]).wait()
        a = pltpu.make_async_copy(ref, rsv, p_sem.at[0])
        a.start()
        b = pltpu.make_async_copy(src.at[rows_of(m, my), :], res, p_sem.at[1])
        b.start()
        return a, b

    def forward_post(m):
        slot = lax.rem(m, 2)

        def run(src):
            t = pltpu.make_async_copy(tgt.at[rows_of(m, my), :], tbuf, p_sem.at[2])
            t.start()
            for cp in load_post(rsf, m, rf_sem, src):
                cp.wait()
            t.wait()

        @pl.when(first)
        def _():
            run(x_in)

        @pl.when(jnp.logical_not(first))
        def _():
            run(x_all)

        @pl.when(m >= 2)
        def _():
            @pl.when(last)
            def _():
                yl_send(m, slot).wait_send()

            @pl.when(jnp.logical_not(last))
            def _():
                for cp in yf_pair(m, slot):
                    cp.wait_send()

        y = (res[...].astype(F32) + (accf[slot, half_rows(my), :] + rsv[...])).astype(BF)

        @pl.when(jnp.logical_not(last))
        def _():
            yf[slot] = y
            own, cross = yf_pair(m, slot)
            own.start()
            by_pair = jnp.logical_and(st == 1, m >= RELAY0)

            @pl.when(by_pair)
            def _():
                fwd_send(m, slot).start()

            @pl.when(jnp.logical_not(by_pair))
            def _():
                cross.start()

        @pl.when(last)
        def _():
            err = y.astype(F32) - tbuf[...].astype(F32)
            yf[slot] = (err * (1.0 / N_ELEM)).astype(BF)
            sq = err * err
            part = sq[:, 0:128]
            for c in range(1, DIM // 128):
                part = part + sq[:, c * 128 : (c + 1) * 128]
            lsum[...] += jnp.sum(part.reshape(HALF // 8, 8, 128), axis=0)
            yl_own(m, slot).start()
            yl_send(m, slot).start()

            @pl.when(m == N_MB - 1)
            def _():
                pltpu.make_async_copy(lsum, lrx.at[my], lr_sem.at[my]).start()
                for cond, cp in loss_sends():
                    pl.when(cond)(cp.start)

    def pass_on(m, base, copy):
        ref = fwd.at[fwd_rows(m), :]
        pltpu.make_async_copy(ref, ref, fr_sem.at[m]).wait()

        @pl.when(m >= base + 2)
        def _():
            copy(m - 2).wait_send()

        copy(m).start()

    def relay(m):
        @pl.when(jnp.logical_and(st == 1, jnp.logical_and(m >= RELAY0, m < N_MB)))
        def _():
            pass_on(m, RELAY0, relay_x)

    def relay_back(m):
        @pl.when(jnp.logical_and(first, jnp.logical_and(m >= RELAY3, m < N_MB)))
        def _():
            pass_on(m, RELAY3, relay_e)

    def loss_sends():
        for y in range(2):
            for s in range(4):
                cp = pltpu.make_async_remote_copy(
                    src_ref=lsum,
                    dst_ref=lrx.at[my],
                    send_sem=ls_sem.at[y * 4 + s],
                    recv_sem=lr_sem.at[my],
                    device_id={"model": y, "stage": s},
                    device_id_type=MESH,
                )
                yield (True if s < 3 else my != y), cp

    def backward(m):
        base = m * n_back
        with jax.named_scope('bwait'):
            wait_in(e_all, m, er_sem)
        with jax.named_scope('bload'):
            load_x(e_all, m)

        @pl.when(jnp.logical_and(m >= 1, jnp.logical_not(first)))
        def _():
            rs_copy(accb, 0, rsb, m - 1, sb_sem, rb_sem).wait_send()

        def slope(j, slot):
            mid[:, cols(j)] = (gelu_slope(uin[slot][...].astype(F32)) * qbuf[slot][...].astype(F32)).astype(BF)

        def block(j, slot):
            start = isinstance(j, int) and j == 0
            ws = use(flat_start, flat_wait, base + j)
            u_load(m, j, slot).start()
            if not start:
                u_load(m, j - 1, 1 - slot).wait()
            qbuf[slot][...] = dot_nt(xbuf[...], flat[ws]).astype(BF)
            if not start:
                slope(j - 1, 1 - slot)

        block(0, 0)

        @pl.loop(0, (N_BLK - 2) // 2)
        def _(i):
            block(2 * i + 1, 1)
            block(2 * i + 2, 0)

        block(N_BLK - 1, 1)
        u_load(m, N_BLK - 1, 1).wait()
        slope(N_BLK - 1, 1)
        mid_copy(g_all, m).start()

        @pl.when(jnp.logical_not(first))
        def _():
            @pl.loop(0, DIM // HB)
            def _(c):
                ws = use(flat_start, flat_wait, base + N_BLK + 2 * c)
                accb[0, :, cols(c)] = dot_nt(mid[:, 0:DIM], flat[ws])
                ws = use(flat_start, flat_wait, base + N_BLK + 2 * c + 1)
                accb[0, :, cols(c)] += dot_nt(mid[:, DIM:HID], flat[ws])
                rs_part(accb, 0, rsb, m, c, sb_sem, rb_sem).start()

        mid_copy(g_all, m).wait()

    def backward_post(m):
        slot = lax.rem(m, 2)
        for cp in load_post(rsb, m, rb_sem, e_all):
            cp.wait()

        @pl.when(m >= 2)
        def _():
            for cp in yb_pair(m, slot):
                cp.wait_send()

        yb[slot] = (res[...].astype(F32) + (accb[0, half_rows(my), :] + rsv[...])).astype(BF)
        own, cross = yb_pair(m, slot)
        own.start()
        far = jnp.logical_and(last, m >= RELAY3)

        @pl.when(far)
        def _():
            far_send(m, slot).start()

        @pl.when(jnp.logical_not(far))
        def _():
            cross.start()

    def weight_ops(v):
        grp = v // GROUP
        quart = lax.rem(v, GROUP)
        rows = pl.ds(pl.multiple_of(grp * GTOK, GTOK), GTOK)
        out2 = quart < 2

        def on_tile(t, fn2, fn1):
            @pl.when(out2)
            def _():
                fn2(cols(quart * (HID // WT // 2) + t, WT))

            @pl.when(jnp.logical_not(out2))
            def _():
                fn1(cols(t, WT), cols(quart - 2, DIM))

        def start_tile(t):
            n_slot = lax.rem(t, 4)
            slot = lax.rem(t, N_WT)

            def fn2(blk):
                pltpu.make_async_copy(a_all.at[rows, blk], narrow.at[n_slot], wn_sem.at[n_slot]).start()

                @pl.when(grp > 0)
                def _():
                    pltpu.make_async_copy(acc2.at[blk, :], wtile.at[slot], wl_sem.at[slot]).start()

            def fn1(dblk, half):
                @pl.when(first)
                def _():
                    pltpu.make_async_copy(x_in.at[rows, dblk], narrow.at[n_slot], wn_sem.at[n_slot]).start()

                @pl.when(jnp.logical_not(first))
                def _():
                    pltpu.make_async_copy(x_all.at[rows, dblk], narrow.at[n_slot], wn_sem.at[n_slot]).start()

                @pl.when(grp > 0)
                def _():
                    pltpu.make_async_copy(acc1.at[dblk, half], wtile.at[slot], wl_sem.at[slot]).start()

            on_tile(t, fn2, fn1)

        def start_store(t):
            slot = lax.rem(t, N_WT)

            def fn2(blk):
                pltpu.make_async_copy(wtile.at[slot], acc2.at[blk, :], ws_sem.at[slot]).start()

            def fn1(dblk, half):
                pltpu.make_async_copy(wtile.at[slot], acc1.at[dblk, half], ws_sem.at[slot]).start()

            on_tile(t, fn2, fn1)

        def wait_store(slot):
            pltpu.make_async_copy(wtile.at[slot], acc2.at[pl.ds(0, WT), :], ws_sem.at[slot]).wait()

        def start():
            @pl.when(out2)
            def _():
                pltpu.make_async_copy(e_all.at[rows, :], wide, wd_sem).start()

            @pl.when(jnp.logical_not(out2))
            def _():
                pltpu.make_async_copy(g_all.at[rows, cols(quart - 2, DIM)], wide, wd_sem).start()

            for t in range(N_WT // 2):
                start_tile(t)

        n_tiles = DIM // WT

        def run(low, high):
            if low == 0:
                pltpu.make_async_copy(e_all.at[rows, :], wide, wd_sem).wait()

            @pl.loop(low, high)
            def _(t):
                slot = lax.rem(t, N_WT)
                n_slot = lax.rem(t, 4)

                @pl.when(t >= N_WT // 2)
                def _():
                    wait_store(lax.rem(t + N_WT // 2, N_WT))

                @pl.when(t + N_WT // 2 < n_tiles)
                def _():
                    start_tile(t + N_WT // 2)

                pltpu.make_async_copy(a_all.at[rows, pl.ds(0, WT)], narrow.at[n_slot], wn_sem.at[n_slot]).wait()

                @pl.when(grp > 0)
                def _():
                    pltpu.make_async_copy(acc2.at[pl.ds(0, WT), :], wtile.at[slot], wl_sem.at[slot]).wait()

                @pl.when(grp == 0)
                def _():
                    wtile[slot] = jnp.zeros((WT, DIM), F32)

                wtile[slot] += dot_tn(narrow[n_slot], wide[...])
                start_store(t)

            if high == n_tiles:
                for t in range(n_tiles - N_WT // 2, n_tiles):
                    wait_store(t % N_WT)

        return start, run

    lsum[...] = jnp.zeros((8, 128), F32)
    for j in range(W_SLOTS - 1):
        tall_start(j)
        flat_start(j)

    @pl.loop(0, N_MB + warm)
    def _(k):
        b = k - warm
        p = k - 1
        v = b - GROUP
        b_on = b >= 0
        f_on = k < N_MB
        p_on = jnp.logical_and(p >= 0, p < N_MB)
        pb_on = jnp.logical_and(b_on, jnp.logical_not(first))
        w_on = jnp.logical_and(v >= 0, jnp.logical_not(first))

        @pl.when(jnp.logical_and(first, v >= 0))
        def _():
            start, run = weight_ops(v)
            with jax.named_scope('W'):
                start()
                run(0, DIM // WT)

        @pl.when(b_on)
        def _():
            with jax.named_scope('B'):
                backward(b)
            with jax.named_scope('RB'):
                relay_back(b + LEAD3)

        @pl.when(jnp.logical_and(b_on, p_on))
        def _():
            with jax.named_scope('PF'):
                forward_post(p)

        @pl.when(b_on)
        def _():
            with jax.named_scope('RX'):
                relay(k - 2)

        @pl.when(jnp.logical_and(w_on, jnp.logical_not(f_on)))
        def _():
            weight_ops(v)[0]()

        @pl.when(f_on)
        def _():
            with jax.named_scope('F'):
                forward(k, lambda: pl.when(w_on)(weight_ops(v)[0]))

        @pl.when(jnp.logical_and(jnp.logical_not(b_on), p_on))
        def _():
            with jax.named_scope('PF'):
                forward_post(p)

        @pl.when(jnp.logical_not(b_on))
        def _():
            with jax.named_scope('RX'):
                relay(k - 2)

        @pl.when(pb_on)
        def _():
            with jax.named_scope('PB'):
                backward_post(b)

        @pl.when(w_on)
        def _():
            with jax.named_scope('W'):
                weight_ops(v)[1](0, DIM // WT)

    for half in range(2):
        pltpu.make_async_copy(lsum, lrx.at[half], lr_sem.at[half]).wait()
    loss[...] = lrx[0] + lrx[1]

    for j in range(W_SLOTS - 1):
        tall_wait(j)
        flat_wait(j)
    for m in (N_MB - 2, N_MB - 1):
        slot = m % 2
        rs_copy(accf, slot, rsf, m, sf_sem, rf_sem).wait_send()

        @pl.when(jnp.logical_not(first))
        def _():
            if m == N_MB - 1:
                rs_copy(accb, 0, rsb, m, sb_sem, rb_sem).wait_send()
            for cp in yb_pair(m, slot):
                cp.wait_send()

        @pl.when(last)
        def _():
            yl_send(m, slot).wait_send()

        @pl.when(jnp.logical_not(last))
        def _():
            for cp in yf_pair(m, slot):
                cp.wait_send()

        @pl.when(st == 1)
        def _():
            relay_x(m).wait_send()

        @pl.when(first)
        def _():
            relay_e(m).wait_send()

    @pl.when(last)
    def _():
        for cond, cp in loss_sends():
            pl.when(cond)(cp.wait_send)


def run_pipeline(x_in, tgt, w1, w2):
    tokens = N_MB * TOK
    hbm = pl.BlockSpec(memory_space=pl.ANY)
    dma = pltpu.SemaphoreType.DMA
    shapes = [
        ((tokens, DIM), BF), ((tokens, DIM), BF),
        ((tokens, HID), BF), ((tokens, HID), BF), ((tokens, HID), BF),
        ((tokens // 2, DIM), F32), ((tokens // 2, DIM), F32), ((tokens // 2, DIM), BF),
        ((DIM, HID), F32), ((HID, DIM), F32),
    ]
    out_shape = [jax.ShapeDtypeStruct(s, d) for s, d in shapes] + [jax.ShapeDtypeStruct((8, 128), F32)]
    return pl.pallas_call(
        pipeline_kernel,
        out_shape=out_shape,
        in_specs=[hbm] * 4,
        out_specs=[hbm] * 10 + [pl.BlockSpec(memory_space=pltpu.VMEM)],
        scratch_shapes=[
            pltpu.VMEM((TOK, DIM), BF),
            pltpu.VMEM((W_SLOTS, DIM, HB), BF),
            pltpu.VMEM((W_SLOTS, HB, DIM), BF),
            pltpu.VMEM((TOK, HB), BF), pltpu.VMEM((TOK, HB), BF),
            pltpu.VMEM((TOK, HB), BF), pltpu.VMEM((TOK, HB), BF),
            pltpu.VMEM((TOK, HB), BF), pltpu.VMEM((TOK, HB), BF),
            pltpu.VMEM((TOK, HID), BF),
            pltpu.VMEM((2, TOK, DIM), F32),
            pltpu.VMEM((1, TOK, DIM), F32),
            pltpu.VMEM((HALF, DIM), F32),
            pltpu.VMEM((HALF, DIM), BF),
            pltpu.VMEM((HALF, DIM), BF),
            pltpu.VMEM((2, HALF, DIM), BF),
            pltpu.VMEM((2, HALF, DIM), BF),
            pltpu.VMEM((GTOK, DIM), BF),
            pltpu.VMEM((4, GTOK, WT), BF),
            pltpu.VMEM((N_WT, WT, DIM), F32),
            pltpu.VMEM((8, 128), F32),
            pltpu.VMEM((2, 8, 128), F32),
            dma((W_SLOTS,)), dma((W_SLOTS,)), dma, dma((2,)), dma, dma((2,)), dma((3,)), dma, dma((4,)), dma((N_WT,)), dma((N_WT,)),
            dma((N_MB, 2)), dma((N_MB, 2)), dma((N_MB,)), dma((N_MB,)), dma((2,)), dma((1,)), dma((2, 2)), dma((2, 2)),
            dma((N_MB,)), dma((2,)), dma((8,)), dma((2,)),
        ],
        compiler_params=pltpu.CompilerParams(vmem_limit_bytes=67_000_000, has_side_effects=True),
        name="pipeline",
    )(x_in, tgt, w1, w2)


def tail_kernel(x_all, e_all, a_all, g_all, acc1, acc2, out1, out2, wide, narrow, tile, wide_sem, n_sem, l_sem, s_sem):
    rows = pl.ds(N_GRP * GTOK, GTOK)
    n2 = HID // HB
    n1 = DIM // HB

    def cols(j, width=HB):
        return pl.ds(pl.multiple_of(j * width, width), width)

    def on_tile(t, fn2, fn1):
        @pl.when(t < n2)
        def _():
            fn2(cols(t))

        @pl.when(t >= n2)
        def _():
            fn1(cols(lax.rem(t - n2, n1)), cols((t - n2) // n1, DIM))

    def start_tile(t):
        slot = lax.rem(t, 4)
        n_slot = lax.rem(t, 3)

        def fn2(blk):
            pltpu.make_async_copy(acc2.at[blk, :], tile.at[slot], l_sem.at[slot]).start()
            pltpu.make_async_copy(a_all.at[rows, blk], narrow.at[n_slot], n_sem.at[n_slot]).start()

        def fn1(dblk, half):
            pltpu.make_async_copy(acc1.at[dblk, half], tile.at[slot], l_sem.at[slot]).start()
            pltpu.make_async_copy(x_all.at[rows, dblk], narrow.at[n_slot], n_sem.at[n_slot]).start()

        on_tile(t, fn2, fn1)

    def start_store(t):
        slot = lax.rem(t, 4)

        def fn2(blk):
            pltpu.make_async_copy(tile.at[slot], out2.at[blk, :], s_sem.at[slot]).start()

        def fn1(dblk, half):
            pltpu.make_async_copy(tile.at[slot], out1.at[dblk, half], s_sem.at[slot]).start()

        on_tile(t, fn2, fn1)

    def wait_store(slot):
        pltpu.make_async_copy(tile.at[slot], out2.at[pl.ds(0, HB), :], s_sem.at[slot]).wait()

    def wide_copy(i):
        src = e_all.at[rows, :] if i == 0 else g_all.at[rows, pl.ds((i - 1) * DIM, DIM)]
        return pltpu.make_async_copy(src, wide.at[i], wide_sem.at[i])

    start_tile(0)
    wide_copy(0).start()
    start_tile(1)

    @pl.loop(0, n2 + 2 * n1)
    def _(t):
        slot = lax.rem(t, 4)
        n_slot = lax.rem(t, 3)

        @pl.when(t >= 2)
        def _():
            wait_store(lax.rem(t + 2, 4))

        @pl.when(t + 2 < n2 + 2 * n1)
        def _():
            start_tile(t + 2)

        for i in range(1, 3):

            @pl.when(t == n2 + (i - 1) * n1 - 4)
            def _():
                wide_copy(i).start()

        for i in range(3):

            @pl.when(t == (0 if i == 0 else n2 + (i - 1) * n1))
            def _():
                wide_copy(i).wait()

        pltpu.make_async_copy(a_all.at[rows, pl.ds(0, HB)], narrow.at[n_slot], n_sem.at[n_slot]).wait()
        pltpu.make_async_copy(acc2.at[pl.ds(0, HB), :], tile.at[slot], l_sem.at[slot]).wait()
        which = jnp.where(t < n2, 0, 1 + (t - n2) // n1)
        tile[slot] += dot_tn(narrow[n_slot], wide[which])
        start_store(t)

    wait_store(2)
    wait_store(3)


def add_tail(x_all, e_all, a_all, g_all, acc1, acc2):
    hbm = pl.BlockSpec(memory_space=pl.ANY)
    dma = pltpu.SemaphoreType.DMA
    return pl.pallas_call(
        tail_kernel,
        in_specs=[hbm] * 6,
        out_specs=[hbm] * 2,
        out_shape=[jax.ShapeDtypeStruct(acc1.shape, F32), jax.ShapeDtypeStruct(acc2.shape, F32)],
        scratch_shapes=[
            pltpu.VMEM((3, GTOK, DIM), BF),
            pltpu.VMEM((3, GTOK, HB), BF),
            pltpu.VMEM((4, HB, DIM), F32),
            dma((3,)), dma((3,)), dma((4,)), dma((4,)),
        ],
        compiler_params=pltpu.CompilerParams(vmem_limit_bytes=60_000_000),
        name="tail",
    )(x_all, e_all, a_all, g_all, acc1, acc2)


def solution(mesh):
    def stage_step(inputs, targets, w_in, w_out):
        tokens = N_MB * TOK
        x_in = inputs.reshape(tokens, DIM)
        tgt = targets.reshape(tokens, DIM)
        x_all, e_all, _, a_all, g_all, _, _, _, acc1, acc2, loss = run_pipeline(x_in, tgt, w_in[0, 0], w_out[0, 0])
        grad_in, grad_out = add_tail(x_all, e_all, a_all, g_all, acc1, acc2)
        total = jnp.sum(loss) * (0.5 / N_ELEM)
        return grad_in[None, None], grad_out[None, None], jnp.reshape(total, (1,))

    return jax.shard_map(
        stage_step,
        mesh=mesh,
        in_specs=(P("data", None, None), P("data", None, None), P("stage", None, None, "model"), P("stage", None, "model", None)),
        out_specs=(P(("data", "stage"), None, None, "model"), P(("data", "stage"), None, "model", None), P("data")),
        check_vma=False,
    )
```

```python
import jax
import jax.numpy as jnp
from jax import lax
from jax.experimental import pallas as pl
from jax.experimental.pallas import tpu as pltpu
from jax.sharding import PartitionSpec as P

GELU_COEF = 0.7978845608028654
CUBIC_COEF = 0.044715

N_MB = 24
TOK = 256
HALF = TOK // 2
DIM = 2560
HID = 5120
HB = 512
N_BLK = HID // HB
W_SLOTS = 4
WT = HB // 2
N_WT = 6
GROUP = 4
N_GRP = N_MB // GROUP - 1
GTOK = GROUP * TOK
N_ELEM = N_MB * TOK * DIM
RELAY0 = 5
RELAY3 = 8
EAGER = 3
LEAD3 = 3
MESH = pl.DeviceIdType.MESH
BF = jnp.bfloat16
F32 = jnp.float32


def dot_nn(a, b):
    return lax.dot_general(a, b, (((1,), (0,)), ((), ())), preferred_element_type=F32)


def dot_nt(a, b):
    return lax.dot_general(a, b, (((1,), (1,)), ((), ())), preferred_element_type=F32)


def dot_tn(a, b):
    return lax.dot_general(a, b, (((0,), (0,)), ((), ())), preferred_element_type=F32)


def gelu(v):
    return 0.5 * v * (1.0 + jnp.tanh(GELU_COEF * (v + CUBIC_COEF * v * v * v)))


def gelu_slope(v):
    t = jnp.tanh(GELU_COEF * (v + CUBIC_COEF * v * v * v))
    return 0.5 * (1.0 + t) + 0.5 * v * (1.0 - t * t) * GELU_COEF * (1.0 + 3.0 * CUBIC_COEF * v * v)


def pipeline_kernel(
    x_in, tgt, w1, w2,
    x_all, e_all, u_all, a_all, g_all, rsf, rsb, fwd, acc1, acc2, loss,
    xbuf, tall, flat, ubuf0, ubuf1, uin0, uin1, qbuf0, qbuf1, mid, accf, accb, rsv, res, tbuf, yf, yb, wide, narrow, wtile, lsum, lrx,
    t_sem, f_sem, x_sem, uo_sem, m_sem, ui_sem, p_sem, wd_sem, wn_sem, wl_sem, ws_sem,
    xr_sem, er_sem, rf_sem, rb_sem, sf_sem, sb_sem, yf_sem, yb_sem, fr_sem, fs_sem, ls_sem, lr_sem,
):
    my = lax.axis_index("model")
    st = lax.axis_index("stage")
    other = 1 - my
    last = st == 3
    first = st == 0
    warm = jnp.where(st == 0, 16, jnp.where(st == 1, 9, jnp.where(st == 2, 5, 2)))
    partner = {"model": other}
    nxt = jnp.minimum(st + 1, 3)
    prv = jnp.maximum(st - 1, 0)

    def rows_of(m, half):
        return pl.ds(pl.multiple_of(m * TOK + half * HALF, HALF), HALF)

    def mb_rows(m):
        return pl.ds(pl.multiple_of(m * TOK, TOK), TOK)

    def half_rows(half):
        return pl.ds(pl.multiple_of(half * HALF, HALF), HALF)

    def cols(j, width=HB):
        return pl.ds(pl.multiple_of(j * width, width), width)

    ubuf, uin, qbuf = (ubuf0, ubuf1), (uin0, uin1), (qbuf0, qbuf1)
    n_back = jnp.where(first, N_BLK, 2 * N_BLK)

    def tall_start(at):
        slot = lax.rem(at, W_SLOTS)
        j = lax.rem(at, 2 * N_BLK)
        i = jnp.maximum(j - N_BLK, 0)

        @pl.when(j < N_BLK)
        def _():
            pltpu.make_async_copy(w1.at[:, cols(j)], tall.at[slot], t_sem.at[slot]).start()

        @pl.when(j >= N_BLK)
        def _():
            pltpu.make_async_copy(w2.at[cols(lax.rem(i, 2), DIM), cols(i // 2)], tall.at[slot], t_sem.at[slot]).start()

    def tall_wait(slot):
        pltpu.make_async_copy(w1.at[:, cols(0)], tall.at[slot], t_sem.at[slot]).wait()

    def flat_start(at):
        slot = lax.rem(at, W_SLOTS)
        j = lax.rem(at, n_back)
        i = jnp.maximum(j - N_BLK, 0)

        @pl.when(j < N_BLK)
        def _():
            pltpu.make_async_copy(w2.at[cols(j), :], flat.at[slot], f_sem.at[slot]).start()

        @pl.when(j >= N_BLK)
        def _():
            pltpu.make_async_copy(w1.at[cols(i // 2), cols(lax.rem(i, 2), DIM)], flat.at[slot], f_sem.at[slot]).start()

    def flat_wait(slot):
        pltpu.make_async_copy(w2.at[cols(0), :], flat.at[slot], f_sem.at[slot]).wait()

    def use(start, wait, at):
        slot = lax.rem(at, W_SLOTS)
        wait(slot)
        start(at + W_SLOTS - 1)
        return slot

    def rs_copy(acc, slot, buf, m, send, recv):
        return pltpu.make_async_remote_copy(
            src_ref=acc.at[slot, half_rows(other), :],
            dst_ref=buf.at[pl.ds(pl.multiple_of(m * HALF, HALF), HALF), :],
            send_sem=send.at[slot],
            recv_sem=recv.at[m],
            device_id=partner,
            device_id_type=MESH,
        )

    def rs_part(acc, slot, buf, m, c, send, recv):
        return pltpu.make_async_remote_copy(
            src_ref=acc.at[slot, half_rows(other), cols(c)],
            dst_ref=buf.at[pl.ds(pl.multiple_of(m * HALF, HALF), HALF), cols(c)],
            send_sem=send.at[slot],
            recv_sem=recv.at[m],
            device_id=partner,
            device_id_type=MESH,
        )

    def half_copy(src, slot, dst, m, half, send, k, recv, dev):
        return pltpu.make_async_remote_copy(
            src_ref=src.at[slot],
            dst_ref=dst.at[rows_of(m, half), :],
            send_sem=send.at[slot, k],
            recv_sem=recv.at[m, half],
            device_id=dev,
            device_id_type=MESH,
        )

    def yf_pair(m, slot):
        return (
            half_copy(yf, slot, x_all, m, my, yf_sem, 0, xr_sem, {"model": my, "stage": nxt}),
            half_copy(yf, slot, x_all, m, my, yf_sem, 1, xr_sem, {"model": other, "stage": nxt}),
        )

    def fwd_rows(m):
        return pl.ds(pl.multiple_of(m * HALF, HALF), HALF)

    def fwd_send(m, slot):
        return pltpu.make_async_remote_copy(
            src_ref=yf.at[slot],
            dst_ref=fwd.at[fwd_rows(m), :],
            send_sem=yf_sem.at[slot, 1],
            recv_sem=fr_sem.at[m],
            device_id=partner,
            device_id_type=MESH,
        )

    def relay_copy(m, dst, recv, to):
        return pltpu.make_async_remote_copy(
            src_ref=fwd.at[fwd_rows(m), :],
            dst_ref=dst.at[rows_of(m, other), :],
            send_sem=fs_sem.at[lax.rem(m, 2)],
            recv_sem=recv.at[m, other],
            device_id={"model": my, "stage": to},
            device_id_type=MESH,
        )

    def relay_x(m):
        return relay_copy(m, x_all, xr_sem, 2)

    def relay_e(m):
        return relay_copy(m, e_all, er_sem, 2)

    def far_send(m, slot):
        return pltpu.make_async_remote_copy(
            src_ref=yb.at[slot],
            dst_ref=fwd.at[fwd_rows(m), :],
            send_sem=yb_sem.at[slot, 1],
            recv_sem=fr_sem.at[m],
            device_id={"model": other, "stage": 0},
            device_id_type=MESH,
        )

    def yl_own(m, slot):
        return pltpu.make_async_copy(yf.at[slot], e_all.at[rows_of(m, my), :], er_sem.at[m, my])

    def yl_send(m, slot):
        return half_copy(yf, slot, e_all, m, my, yf_sem, 1, er_sem, partner)

    def yb_pair(m, slot):
        return (
            half_copy(yb, slot, e_all, m, my, yb_sem, 0, er_sem, {"model": my, "stage": prv}),
            half_copy(yb, slot, e_all, m, my, yb_sem, 1, er_sem, {"model": other, "stage": prv}),
        )

    def wait_in(dst, m, recv):
        for half in range(2):
            ref = dst.at[rows_of(m, half), :]
            pltpu.make_async_copy(ref, ref, recv.at[m, half]).wait()

    def out_copy(buf, slot, dst, m, j, sem):
        return pltpu.make_async_copy(buf[slot], dst.at[mb_rows(m), cols(j)], sem.at[slot])

    def mid_copy(dst, m):
        return pltpu.make_async_copy(mid, dst.at[mb_rows(m), :], m_sem)

    def u_load(m, j, slot):
        return pltpu.make_async_copy(u_all.at[mb_rows(m), cols(j)], uin[slot], ui_sem.at[slot])

    def load_x(src, m, also=None):
        cp = pltpu.make_async_copy(src.at[mb_rows(m), :], xbuf, x_sem)
        cp.start()
        if also is not None:
            also()
        cp.wait()

    def forward(m, also):
        slot_m = lax.rem(m, 2)
        base = m * 2 * N_BLK

        @pl.when(first)
        def _():
            load_x(x_in, m)

            @pl.when(m >= N_GRP * GROUP)
            def _():
                cp = pltpu.make_async_copy(xbuf, x_all.at[mb_rows(m), :], x_sem)
                cp.start()
                cp.wait()

        @pl.when(jnp.logical_not(first))
        def _():
            with jax.named_scope('fwait'):
                wait_in(x_all, m, xr_sem)
            with jax.named_scope('fload'):
                load_x(x_all, m, also)

        @pl.when(m >= 2)
        def _():
            rs_copy(accf, slot_m, rsf, m - 2, sf_sem, rf_sem).wait_send()

        def activate(j, slot):
            mid[:, cols(j)] = gelu(ubuf[slot][...].astype(F32)).astype(BF)

        def block(j, slot):
            ws = use(tall_start, tall_wait, base + j)

            @pl.when(j >= 2)
            def _():
                out_copy(ubuf, slot, u_all, m, j, uo_sem).wait()

            ubuf[slot][...] = dot_nn(xbuf[...], tall[ws]).astype(BF)
            if not (isinstance(j, int) and j == 0):
                activate(j - 1, 1 - slot)
            out_copy(ubuf, slot, u_all, m, j, uo_sem).start()

        block(0, 0)

        @pl.loop(0, (N_BLK - 2) // 2)
        def _(i):
            block(2 * i + 1, 1)
            block(2 * i + 2, 0)

        block(N_BLK - 1, 1)
        activate(N_BLK - 1, 1)
        mid_copy(a_all, m).start()

        @pl.loop(0, DIM // HB)
        def _(c):
            ws = use(tall_start, tall_wait, base + N_BLK + 2 * c)
            accf[slot_m, :, cols(c)] = dot_nn(mid[:, 0:DIM], tall[ws])
            ws = use(tall_start, tall_wait, base + N_BLK + 2 * c + 1)
            accf[slot_m, :, cols(c)] += dot_nn(mid[:, DIM:HID], tall[ws])
            rs_part(accf, slot_m, rsf, m, c, sf_sem, rf_sem).start()

        for slot in range(2):
            out_copy(ubuf, slot, u_all, m, slot, uo_sem).wait()
        mid_copy(a_all, m).wait()

    def load_post(acc_buf, m, recv, src):
        ref = acc_buf.at[pl.ds(pl.multiple_of(m * HALF, HALF), HALF), :]
        with jax.named_scope('pwait'):
            pltpu.make_async_copy(ref, ref, recv.at[m]).wait()
        a = pltpu.make_async_copy(ref, rsv, p_sem.at[0])
        a.start()
        b = pltpu.make_async_copy(src.at[rows_of(m, my), :], res, p_sem.at[1])
        b.start()
        return a, b

    def forward_post(m):
        slot = lax.rem(m, 2)

        def run(src):
            t = pltpu.make_async_copy(tgt.at[rows_of(m, my), :], tbuf, p_sem.at[2])
            t.start()
            for cp in load_post(rsf, m, rf_sem, src):
                cp.wait()
            t.wait()

        @pl.when(first)
        def _():
            run(x_in)

        @pl.when(jnp.logical_not(first))
        def _():
            run(x_all)

        @pl.when(m >= 2)
        def _():
            @pl.when(last)
            def _():
                yl_send(m, slot).wait_send()

            @pl.when(jnp.logical_not(last))
            def _():
                for cp in yf_pair(m, slot):
                    cp.wait_send()

        y = (res[...].astype(F32) + (accf[slot, half_rows(my), :] + rsv[...])).astype(BF)

        @pl.when(jnp.logical_not(last))
        def _():
            yf[slot] = y
            own, cross = yf_pair(m, slot)
            own.start()
            by_pair = jnp.logical_and(st == 1, m >= RELAY0)

            @pl.when(by_pair)
            def _():
                fwd_send(m, slot).start()

            @pl.when(jnp.logical_not(by_pair))
            def _():
                cross.start()

        @pl.when(last)
        def _():
            err = y.astype(F32) - tbuf[...].astype(F32)
            yf[slot] = (err * (1.0 / N_ELEM)).astype(BF)
            sq = err * err
            part = sq[:, 0:128]
            for c in range(1, DIM // 128):
                part = part + sq[:, c * 128 : (c + 1) * 128]
            lsum[...] += jnp.sum(part.reshape(HALF // 8, 8, 128), axis=0)
            yl_own(m, slot).start()
            yl_send(m, slot).start()

            @pl.when(m == N_MB - 1)
            def _():
                pltpu.make_async_copy(lsum, lrx.at[my], lr_sem.at[my]).start()
                for cond, cp in loss_sends():
                    pl.when(cond)(cp.start)

    def pass_on(m, base, copy):
        ref = fwd.at[fwd_rows(m), :]
        pltpu.make_async_copy(ref, ref, fr_sem.at[m]).wait()

        @pl.when(m >= base + 2)
        def _():
            copy(m - 2).wait_send()

        copy(m).start()

    def relay(m):
        @pl.when(jnp.logical_and(st == 1, jnp.logical_and(m >= RELAY0, m < N_MB)))
        def _():
            pass_on(m, RELAY0, relay_x)

    def relay_back(m):
        @pl.when(jnp.logical_and(first, jnp.logical_and(m >= RELAY3, m < N_MB)))
        def _():
            pass_on(m, RELAY3, relay_e)

    def loss_sends():
        for y in range(2):
            for s in range(4):
                cp = pltpu.make_async_remote_copy(
                    src_ref=lsum,
                    dst_ref=lrx.at[my],
                    send_sem=ls_sem.at[y * 4 + s],
                    recv_sem=lr_sem.at[my],
                    device_id={"model": y, "stage": s},
                    device_id_type=MESH,
                )
                yield (True if s < 3 else my != y), cp

    def backward(m):
        base = m * n_back
        with jax.named_scope('bwait'):
            wait_in(e_all, m, er_sem)
        with jax.named_scope('bload'):
            load_x(e_all, m)

        @pl.when(jnp.logical_and(m >= 1, jnp.logical_not(first)))
        def _():
            rs_copy(accb, 0, rsb, m - 1, sb_sem, rb_sem).wait_send()

        def slope(j, slot):
            mid[:, cols(j)] = (gelu_slope(uin[slot][...].astype(F32)) * qbuf[slot][...].astype(F32)).astype(BF)

        def block(j, slot):
            start = isinstance(j, int) and j == 0
            ws = use(flat_start, flat_wait, base + j)
            u_load(m, j, slot).start()
            if not start:
                u_load(m, j - 1, 1 - slot).wait()
            qbuf[slot][...] = dot_nt(xbuf[...], flat[ws]).astype(BF)
            if not start:
                slope(j - 1, 1 - slot)

        block(0, 0)

        @pl.loop(0, (N_BLK - 2) // 2)
        def _(i):
            block(2 * i + 1, 1)
            block(2 * i + 2, 0)

        block(N_BLK - 1, 1)
        u_load(m, N_BLK - 1, 1).wait()
        slope(N_BLK - 1, 1)
        mid_copy(g_all, m).start()

        @pl.when(jnp.logical_not(first))
        def _():
            @pl.loop(0, DIM // HB)
            def _(c):
                ws = use(flat_start, flat_wait, base + N_BLK + 2 * c)
                accb[0, :, cols(c)] = dot_nt(mid[:, 0:DIM], flat[ws])
                ws = use(flat_start, flat_wait, base + N_BLK + 2 * c + 1)
                accb[0, :, cols(c)] += dot_nt(mid[:, DIM:HID], flat[ws])
                rs_part(accb, 0, rsb, m, c, sb_sem, rb_sem).start()

        mid_copy(g_all, m).wait()

    def backward_post(m):
        slot = lax.rem(m, 2)
        for cp in load_post(rsb, m, rb_sem, e_all):
            cp.wait()

        @pl.when(m >= 2)
        def _():
            for cp in yb_pair(m, slot):
                cp.wait_send()

        yb[slot] = (res[...].astype(F32) + (accb[0, half_rows(my), :] + rsv[...])).astype(BF)
        own, cross = yb_pair(m, slot)
        own.start()
        far = jnp.logical_and(last, m >= RELAY3)

        @pl.when(far)
        def _():
            far_send(m, slot).start()

        @pl.when(jnp.logical_not(far))
        def _():
            cross.start()

    def weight_ops(v):
        grp = v // GROUP
        quart = lax.rem(v, GROUP)
        rows = pl.ds(pl.multiple_of(grp * GTOK, GTOK), GTOK)
        out2 = quart < 2

        def on_tile(t, fn2, fn1):
            @pl.when(out2)
            def _():
                fn2(cols(quart * (HID // WT // 2) + t, WT))

            @pl.when(jnp.logical_not(out2))
            def _():
                fn1(cols(t, WT), cols(quart - 2, DIM))

        def start_tile(t):
            n_slot = lax.rem(t, 4)
            slot = lax.rem(t, N_WT)

            def fn2(blk):
                pltpu.make_async_copy(a_all.at[rows, blk], narrow.at[n_slot], wn_sem.at[n_slot]).start()

                @pl.when(grp > 0)
                def _():
                    pltpu.make_async_copy(acc2.at[blk, :], wtile.at[slot], wl_sem.at[slot]).start()

            def fn1(dblk, half):
                @pl.when(first)
                def _():
                    pltpu.make_async_copy(x_in.at[rows, dblk], narrow.at[n_slot], wn_sem.at[n_slot]).start()

                @pl.when(jnp.logical_not(first))
                def _():
                    pltpu.make_async_copy(x_all.at[rows, dblk], narrow.at[n_slot], wn_sem.at[n_slot]).start()

                @pl.when(grp > 0)
                def _():
                    pltpu.make_async_copy(acc1.at[dblk, half], wtile.at[slot], wl_sem.at[slot]).start()

            on_tile(t, fn2, fn1)

        def start_store(t):
            slot = lax.rem(t, N_WT)

            def fn2(blk):
                pltpu.make_async_copy(wtile.at[slot], acc2.at[blk, :], ws_sem.at[slot]).start()

            def fn1(dblk, half):
                pltpu.make_async_copy(wtile.at[slot], acc1.at[dblk, half], ws_sem.at[slot]).start()

            on_tile(t, fn2, fn1)

        def wait_store(slot):
            pltpu.make_async_copy(wtile.at[slot], acc2.at[pl.ds(0, WT), :], ws_sem.at[slot]).wait()

        def start():
            @pl.when(out2)
            def _():
                pltpu.make_async_copy(e_all.at[rows, :], wide, wd_sem).start()

            @pl.when(jnp.logical_not(out2))
            def _():
                pltpu.make_async_copy(g_all.at[rows, cols(quart - 2, DIM)], wide, wd_sem).start()

            for t in range(N_WT // 2):
                start_tile(t)

        n_tiles = DIM // WT

        def run(low, high):
            if low == 0:
                pltpu.make_async_copy(e_all.at[rows, :], wide, wd_sem).wait()

            @pl.loop(low, high)
            def _(t):
                slot = lax.rem(t, N_WT)
                n_slot = lax.rem(t, 4)

                @pl.when(t >= N_WT // 2)
                def _():
                    wait_store(lax.rem(t + N_WT // 2, N_WT))

                @pl.when(t + N_WT // 2 < n_tiles)
                def _():
                    start_tile(t + N_WT // 2)

                pltpu.make_async_copy(a_all.at[rows, pl.ds(0, WT)], narrow.at[n_slot], wn_sem.at[n_slot]).wait()

                @pl.when(grp > 0)
                def _():
                    pltpu.make_async_copy(acc2.at[pl.ds(0, WT), :], wtile.at[slot], wl_sem.at[slot]).wait()

                @pl.when(grp == 0)
                def _():
                    wtile[slot] = jnp.zeros((WT, DIM), F32)

                wtile[slot] += dot_tn(narrow[n_slot], wide[...])
                start_store(t)

            if high == n_tiles:
                for t in range(n_tiles - N_WT // 2, n_tiles):
                    wait_store(t % N_WT)

        return start, run

    lsum[...] = jnp.zeros((8, 128), F32)
    for j in range(W_SLOTS - 1):
        tall_start(j)
        flat_start(j)

    @pl.loop(0, N_MB + warm)
    def _(k):
        b = k - warm
        p = k - 1
        v = b - GROUP
        b_on = b >= 0
        f_on = k < N_MB
        p_on = jnp.logical_and(p >= EAGER, p < N_MB)
        pb_on = jnp.logical_and(b_on, jnp.logical_not(first))
        w_on = jnp.logical_and(v >= 0, jnp.logical_not(first))

        @pl.when(jnp.logical_and(first, v >= 0))
        def _():
            start, run = weight_ops(v)
            with jax.named_scope('W'):
                start()
                run(0, DIM // WT)

        @pl.when(b_on)
        def _():
            with jax.named_scope('B'):
                backward(b)
            with jax.named_scope('RB'):
                relay_back(b + LEAD3)

        @pl.when(jnp.logical_and(b_on, p_on))
        def _():
            with jax.named_scope('PF'):
                forward_post(p)

        @pl.when(b_on)
        def _():
            with jax.named_scope('RX'):
                relay(k - 2)

        @pl.when(jnp.logical_and(w_on, jnp.logical_not(f_on)))
        def _():
            weight_ops(v)[0]()

        @pl.when(f_on)
        def _():
            with jax.named_scope('F'):
                forward(k, lambda: pl.when(w_on)(weight_ops(v)[0]))

        @pl.when(k < EAGER)
        def _():
            with jax.named_scope('PF'):
                forward_post(k)

        @pl.when(jnp.logical_and(jnp.logical_not(b_on), p_on))
        def _():
            with jax.named_scope('PF'):
                forward_post(p)

        @pl.when(jnp.logical_not(b_on))
        def _():
            with jax.named_scope('RX'):
                relay(k - 2)

        post_first = jnp.logical_or(f_on, b == N_MB - 1)

        @pl.when(jnp.logical_and(pb_on, post_first))
        def _():
            with jax.named_scope('PB'):
                backward_post(b)

        @pl.when(w_on)
        def _():
            with jax.named_scope('W'):
                weight_ops(v)[1](0, DIM // WT)

        @pl.when(jnp.logical_and(pb_on, jnp.logical_not(post_first)))
        def _():
            with jax.named_scope('PB'):
                backward_post(b)

    for half in range(2):
        pltpu.make_async_copy(lsum, lrx.at[half], lr_sem.at[half]).wait()
    loss[...] = lrx[0] + lrx[1]

    for j in range(W_SLOTS - 1):
        tall_wait(j)
        flat_wait(j)
    for m in (N_MB - 2, N_MB - 1):
        slot = m % 2
        rs_copy(accf, slot, rsf, m, sf_sem, rf_sem).wait_send()

        @pl.when(jnp.logical_not(first))
        def _():
            if m == N_MB - 1:
                rs_copy(accb, 0, rsb, m, sb_sem, rb_sem).wait_send()
            for cp in yb_pair(m, slot):
                cp.wait_send()

        @pl.when(last)
        def _():
            yl_send(m, slot).wait_send()

        @pl.when(jnp.logical_not(last))
        def _():
            for cp in yf_pair(m, slot):
                cp.wait_send()

        @pl.when(st == 1)
        def _():
            relay_x(m).wait_send()

        @pl.when(first)
        def _():
            relay_e(m).wait_send()

    @pl.when(last)
    def _():
        for cond, cp in loss_sends():
            pl.when(cond)(cp.wait_send)


def run_pipeline(x_in, tgt, w1, w2):
    tokens = N_MB * TOK
    hbm = pl.BlockSpec(memory_space=pl.ANY)
    dma = pltpu.SemaphoreType.DMA
    shapes = [
        ((tokens, DIM), BF), ((tokens, DIM), BF),
        ((tokens, HID), BF), ((tokens, HID), BF), ((tokens, HID), BF),
        ((tokens // 2, DIM), F32), ((tokens // 2, DIM), F32), ((tokens // 2, DIM), BF),
        ((DIM, HID), F32), ((HID, DIM), F32),
    ]
    out_shape = [jax.ShapeDtypeStruct(s, d) for s, d in shapes] + [jax.ShapeDtypeStruct((8, 128), F32)]
    return pl.pallas_call(
        pipeline_kernel,
        out_shape=out_shape,
        in_specs=[hbm] * 4,
        out_specs=[hbm] * 10 + [pl.BlockSpec(memory_space=pltpu.VMEM)],
        scratch_shapes=[
            pltpu.VMEM((TOK, DIM), BF),
            pltpu.VMEM((W_SLOTS, DIM, HB), BF),
            pltpu.VMEM((W_SLOTS, HB, DIM), BF),
            pltpu.VMEM((TOK, HB), BF), pltpu.VMEM((TOK, HB), BF),
            pltpu.VMEM((TOK, HB), BF), pltpu.VMEM((TOK, HB), BF),
            pltpu.VMEM((TOK, HB), BF), pltpu.VMEM((TOK, HB), BF),
            pltpu.VMEM((TOK, HID), BF),
            pltpu.VMEM((2, TOK, DIM), F32),
            pltpu.VMEM((1, TOK, DIM), F32),
            pltpu.VMEM((HALF, DIM), F32),
            pltpu.VMEM((HALF, DIM), BF),
            pltpu.VMEM((HALF, DIM), BF),
            pltpu.VMEM((2, HALF, DIM), BF),
            pltpu.VMEM((2, HALF, DIM), BF),
            pltpu.VMEM((GTOK, DIM), BF),
            pltpu.VMEM((4, GTOK, WT), BF),
            pltpu.VMEM((N_WT, WT, DIM), F32),
            pltpu.VMEM((8, 128), F32),
            pltpu.VMEM((2, 8, 128), F32),
            dma((W_SLOTS,)), dma((W_SLOTS,)), dma, dma((2,)), dma, dma((2,)), dma((3,)), dma, dma((4,)), dma((N_WT,)), dma((N_WT,)),
            dma((N_MB, 2)), dma((N_MB, 2)), dma((N_MB,)), dma((N_MB,)), dma((2,)), dma((1,)), dma((2, 2)), dma((2, 2)),
            dma((N_MB,)), dma((2,)), dma((8,)), dma((2,)),
        ],
        compiler_params=pltpu.CompilerParams(vmem_limit_bytes=67_000_000, has_side_effects=True),
        name="pipeline",
    )(x_in, tgt, w1, w2)


def tail_kernel(x_all, e_all, a_all, g_all, acc1, acc2, out1, out2, wide, narrow, tile, wide_sem, n_sem, l_sem, s_sem):
    rows = pl.ds(N_GRP * GTOK, GTOK)
    n2 = HID // HB
    n1 = DIM // HB

    def cols(j, width=HB):
        return pl.ds(pl.multiple_of(j * width, width), width)

    def on_tile(t, fn2, fn1):
        @pl.when(t < n2)
        def _():
            fn2(cols(t))

        @pl.when(t >= n2)
        def _():
            fn1(cols(lax.rem(t - n2, n1)), cols((t - n2) // n1, DIM))

    def start_tile(t):
        slot = lax.rem(t, 4)
        n_slot = lax.rem(t, 3)

        def fn2(blk):
            pltpu.make_async_copy(acc2.at[blk, :], tile.at[slot], l_sem.at[slot]).start()
            pltpu.make_async_copy(a_all.at[rows, blk], narrow.at[n_slot], n_sem.at[n_slot]).start()

        def fn1(dblk, half):
            pltpu.make_async_copy(acc1.at[dblk, half], tile.at[slot], l_sem.at[slot]).start()
            pltpu.make_async_copy(x_all.at[rows, dblk], narrow.at[n_slot], n_sem.at[n_slot]).start()

        on_tile(t, fn2, fn1)

    def start_store(t):
        slot = lax.rem(t, 4)

        def fn2(blk):
            pltpu.make_async_copy(tile.at[slot], out2.at[blk, :], s_sem.at[slot]).start()

        def fn1(dblk, half):
            pltpu.make_async_copy(tile.at[slot], out1.at[dblk, half], s_sem.at[slot]).start()

        on_tile(t, fn2, fn1)

    def wait_store(slot):
        pltpu.make_async_copy(tile.at[slot], out2.at[pl.ds(0, HB), :], s_sem.at[slot]).wait()

    def wide_copy(i):
        src = e_all.at[rows, :] if i == 0 else g_all.at[rows, pl.ds((i - 1) * DIM, DIM)]
        return pltpu.make_async_copy(src, wide.at[i], wide_sem.at[i])

    start_tile(0)
    wide_copy(0).start()
    start_tile(1)

    @pl.loop(0, n2 + 2 * n1)
    def _(t):
        slot = lax.rem(t, 4)
        n_slot = lax.rem(t, 3)

        @pl.when(t >= 2)
        def _():
            wait_store(lax.rem(t + 2, 4))

        @pl.when(t + 2 < n2 + 2 * n1)
        def _():
            start_tile(t + 2)

        for i in range(1, 3):

            @pl.when(t == n2 + (i - 1) * n1 - 4)
            def _():
                wide_copy(i).start()

        for i in range(3):

            @pl.when(t == (0 if i == 0 else n2 + (i - 1) * n1))
            def _():
                wide_copy(i).wait()

        pltpu.make_async_copy(a_all.at[rows, pl.ds(0, HB)], narrow.at[n_slot], n_sem.at[n_slot]).wait()
        pltpu.make_async_copy(acc2.at[pl.ds(0, HB), :], tile.at[slot], l_sem.at[slot]).wait()
        which = jnp.where(t < n2, 0, 1 + (t - n2) // n1)
        tile[slot] += dot_tn(narrow[n_slot], wide[which])
        start_store(t)

    wait_store(2)
    wait_store(3)


def add_tail(x_all, e_all, a_all, g_all, acc1, acc2):
    hbm = pl.BlockSpec(memory_space=pl.ANY)
    dma = pltpu.SemaphoreType.DMA
    return pl.pallas_call(
        tail_kernel,
        in_specs=[hbm] * 6,
        out_specs=[hbm] * 2,
        out_shape=[jax.ShapeDtypeStruct(acc1.shape, F32), jax.ShapeDtypeStruct(acc2.shape, F32)],
        scratch_shapes=[
            pltpu.VMEM((3, GTOK, DIM), BF),
            pltpu.VMEM((3, GTOK, HB), BF),
            pltpu.VMEM((4, HB, DIM), F32),
            dma((3,)), dma((3,)), dma((4,)), dma((4,)),
        ],
        compiler_params=pltpu.CompilerParams(vmem_limit_bytes=60_000_000),
        name="tail",
    )(x_all, e_all, a_all, g_all, acc1, acc2)


def solution(mesh):
    def stage_step(inputs, targets, w_in, w_out):
        tokens = N_MB * TOK
        x_in = inputs.reshape(tokens, DIM)
        tgt = targets.reshape(tokens, DIM)
        x_all, e_all, _, a_all, g_all, _, _, _, acc1, acc2, loss = run_pipeline(x_in, tgt, w_in[0, 0], w_out[0, 0])
        grad_in, grad_out = add_tail(x_all, e_all, a_all, g_all, acc1, acc2)
        total = jnp.sum(loss) * (0.5 / N_ELEM)
        return grad_in[None, None], grad_out[None, None], jnp.reshape(total, (1,))

    return jax.shard_map(
        stage_step,
        mesh=mesh,
        in_specs=(P("data", None, None), P("data", None, None), P("stage", None, None, "model"), P("stage", None, "model", None)),
        out_specs=(P(("data", "stage"), None, None, "model"), P(("data", "stage"), None, "model", None), P("data")),
        check_vma=False,
    )
```

```python
import jax
import jax.numpy as jnp
from jax import lax
from jax.experimental import pallas as pl
from jax.experimental.pallas import tpu as pltpu
from jax.sharding import PartitionSpec as P

GELU_COEF = 0.7978845608028654
CUBIC_COEF = 0.044715

N_MB = 24
TOK = 256
HALF = TOK // 2
DIM = 2560
HID = 5120
HB = 512
N_BLK = HID // HB
W_SLOTS = 4
WT = HB // 2
N_WT = 6
GROUP = 4
N_GRP = N_MB // GROUP - 1
GTOK = GROUP * TOK
N_ELEM = N_MB * TOK * DIM
RELAY0 = 5
RELAY3 = 8
EAGER = 3
LEAD3 = 3
MESH = pl.DeviceIdType.MESH
BF = jnp.bfloat16
F32 = jnp.float32


def dot_nn(a, b):
    return lax.dot_general(a, b, (((1,), (0,)), ((), ())), preferred_element_type=F32)


def dot_nt(a, b):
    return lax.dot_general(a, b, (((1,), (1,)), ((), ())), preferred_element_type=F32)


def dot_tn(a, b):
    return lax.dot_general(a, b, (((0,), (0,)), ((), ())), preferred_element_type=F32)


def gelu(v):
    return 0.5 * v * (1.0 + jnp.tanh(GELU_COEF * (v + CUBIC_COEF * v * v * v)))


def gelu_slope(v):
    t = jnp.tanh(GELU_COEF * (v + CUBIC_COEF * v * v * v))
    return 0.5 * (1.0 + t) + 0.5 * v * (1.0 - t * t) * GELU_COEF * (1.0 + 3.0 * CUBIC_COEF * v * v)


def pipeline_kernel(
    x_in, tgt, w1, w2,
    x_all, e_all, u_all, a_all, g_all, rsf, rsb, fwd, acc1, acc2, loss,
    xbuf, tall, flat, ubuf0, ubuf1, uin0, uin1, qbuf0, qbuf1, mid, accf, accb, rsv, res, tbuf, yf, yb, wide, narrow, wtile, lsum, lrx,
    t_sem, f_sem, x_sem, uo_sem, m_sem, ui_sem, p_sem, wd_sem, wn_sem, wl_sem, ws_sem,
    xr_sem, er_sem, rf_sem, rb_sem, sf_sem, sb_sem, yf_sem, yb_sem, fr_sem, fs_sem, ls_sem, lr_sem,
):
    my = lax.axis_index("model")
    st = lax.axis_index("stage")
    other = 1 - my
    last = st == 3
    first = st == 0
    warm = jnp.where(st == 0, 16, jnp.where(st == 1, 9, jnp.where(st == 2, 5, 2)))
    partner = {"model": other}
    nxt = jnp.minimum(st + 1, 3)
    prv = jnp.maximum(st - 1, 0)

    def rows_of(m, half):
        return pl.ds(pl.multiple_of(m * TOK + half * HALF, HALF), HALF)

    def mb_rows(m):
        return pl.ds(pl.multiple_of(m * TOK, TOK), TOK)

    def half_rows(half):
        return pl.ds(pl.multiple_of(half * HALF, HALF), HALF)

    def cols(j, width=HB):
        return pl.ds(pl.multiple_of(j * width, width), width)

    ubuf, uin, qbuf = (ubuf0, ubuf1), (uin0, uin1), (qbuf0, qbuf1)
    n_back = jnp.where(first, N_BLK, 2 * N_BLK)

    def tall_start(at):
        slot = lax.rem(at, W_SLOTS)
        j = lax.rem(at, 2 * N_BLK)
        i = jnp.maximum(j - N_BLK, 0)

        @pl.when(j < N_BLK)
        def _():
            pltpu.make_async_copy(w1.at[:, cols(j)], tall.at[slot], t_sem.at[slot]).start()

        @pl.when(j >= N_BLK)
        def _():
            pltpu.make_async_copy(w2.at[cols(lax.rem(i, 2), DIM), cols(i // 2)], tall.at[slot], t_sem.at[slot]).start()

    def tall_wait(slot):
        pltpu.make_async_copy(w1.at[:, cols(0)], tall.at[slot], t_sem.at[slot]).wait()

    def flat_start(at):
        slot = lax.rem(at, W_SLOTS)
        j = lax.rem(at, n_back)
        i = jnp.maximum(j - N_BLK, 0)

        @pl.when(j < N_BLK)
        def _():
            pltpu.make_async_copy(w2.at[cols(j), :], flat.at[slot], f_sem.at[slot]).start()

        @pl.when(j >= N_BLK)
        def _():
            pltpu.make_async_copy(w1.at[cols(i // 2), cols(lax.rem(i, 2), DIM)], flat.at[slot], f_sem.at[slot]).start()

    def flat_wait(slot):
        pltpu.make_async_copy(w2.at[cols(0), :], flat.at[slot], f_sem.at[slot]).wait()

    def use(start, wait, at):
        slot = lax.rem(at, W_SLOTS)
        wait(slot)
        start(at + W_SLOTS - 1)
        return slot

    def rs_copy(acc, slot, buf, m, send, recv):
        return pltpu.make_async_remote_copy(
            src_ref=acc.at[slot, half_rows(other), :],
            dst_ref=buf.at[pl.ds(pl.multiple_of(m * HALF, HALF), HALF), :],
            send_sem=send.at[slot],
            recv_sem=recv.at[m],
            device_id=partner,
            device_id_type=MESH,
        )

    def rs_part(acc, slot, buf, m, c, send, recv):
        return pltpu.make_async_remote_copy(
            src_ref=acc.at[slot, half_rows(other), cols(c)],
            dst_ref=buf.at[pl.ds(pl.multiple_of(m * HALF, HALF), HALF), cols(c)],
            send_sem=send.at[slot],
            recv_sem=recv.at[m],
            device_id=partner,
            device_id_type=MESH,
        )

    def half_copy(src, slot, dst, m, half, send, k, recv, dev):
        return pltpu.make_async_remote_copy(
            src_ref=src.at[slot],
            dst_ref=dst.at[rows_of(m, half), :],
            send_sem=send.at[slot, k],
            recv_sem=recv.at[m, half],
            device_id=dev,
            device_id_type=MESH,
        )

    def yf_pair(m, slot):
        return (
            half_copy(yf, slot, x_all, m, my, yf_sem, 0, xr_sem, {"model": my, "stage": nxt}),
            half_copy(yf, slot, x_all, m, my, yf_sem, 1, xr_sem, {"model": other, "stage": nxt}),
        )

    def fwd_rows(m):
        return pl.ds(pl.multiple_of(m * HALF, HALF), HALF)

    def fwd_send(m, slot):
        return pltpu.make_async_remote_copy(
            src_ref=yf.at[slot],
            dst_ref=fwd.at[fwd_rows(m), :],
            send_sem=yf_sem.at[slot, 1],
            recv_sem=fr_sem.at[m],
            device_id=partner,
            device_id_type=MESH,
        )

    def relay_copy(m, dst, recv, to):
        return pltpu.make_async_remote_copy(
            src_ref=fwd.at[fwd_rows(m), :],
            dst_ref=dst.at[rows_of(m, other), :],
            send_sem=fs_sem.at[lax.rem(m, 2)],
            recv_sem=recv.at[m, other],
            device_id={"model": my, "stage": to},
            device_id_type=MESH,
        )

    def relay_x(m):
        return relay_copy(m, x_all, xr_sem, 2)

    def relay_e(m):
        return relay_copy(m, e_all, er_sem, 2)

    def far_send(m, slot):
        return pltpu.make_async_remote_copy(
            src_ref=yb.at[slot],
            dst_ref=fwd.at[fwd_rows(m), :],
            send_sem=yb_sem.at[slot, 1],
            recv_sem=fr_sem.at[m],
            device_id={"model": other, "stage": 0},
            device_id_type=MESH,
        )

    def yl_own(m, slot):
        return pltpu.make_async_copy(yf.at[slot], e_all.at[rows_of(m, my), :], er_sem.at[m, my])

    def yl_send(m, slot):
        return half_copy(yf, slot, e_all, m, my, yf_sem, 1, er_sem, partner)

    def yb_pair(m, slot):
        return (
            half_copy(yb, slot, e_all, m, my, yb_sem, 0, er_sem, {"model": my, "stage": prv}),
            half_copy(yb, slot, e_all, m, my, yb_sem, 1, er_sem, {"model": other, "stage": prv}),
        )

    def wait_in(dst, m, recv):
        for half in range(2):
            ref = dst.at[rows_of(m, half), :]
            pltpu.make_async_copy(ref, ref, recv.at[m, half]).wait()

    def out_copy(buf, slot, dst, m, j, sem):
        return pltpu.make_async_copy(buf[slot], dst.at[mb_rows(m), cols(j)], sem.at[slot])

    def mid_copy(dst, m):
        return pltpu.make_async_copy(mid, dst.at[mb_rows(m), :], m_sem)

    def u_load(m, j, slot):
        return pltpu.make_async_copy(u_all.at[mb_rows(m), cols(j)], uin[slot], ui_sem.at[slot])

    def load_x(src, m, also=None):
        cp = pltpu.make_async_copy(src.at[mb_rows(m), :], xbuf, x_sem)
        cp.start()
        if also is not None:
            also()
        cp.wait()

    def forward(m, also):
        slot_m = lax.rem(m, 2)
        base = m * 2 * N_BLK

        @pl.when(first)
        def _():
            load_x(x_in, m)

            @pl.when(m >= N_GRP * GROUP)
            def _():
                cp = pltpu.make_async_copy(xbuf, x_all.at[mb_rows(m), :], x_sem)
                cp.start()
                cp.wait()

        @pl.when(jnp.logical_not(first))
        def _():
            wait_in(x_all, m, xr_sem)
            load_x(x_all, m, also)

        @pl.when(m >= 2)
        def _():
            rs_copy(accf, slot_m, rsf, m - 2, sf_sem, rf_sem).wait_send()

        def activate(j, slot):
            mid[:, cols(j)] = gelu(ubuf[slot][...].astype(F32)).astype(BF)

        def block(j, slot):
            ws = use(tall_start, tall_wait, base + j)

            @pl.when(j >= 2)
            def _():
                out_copy(ubuf, slot, u_all, m, j, uo_sem).wait()

            ubuf[slot][...] = dot_nn(xbuf[...], tall[ws]).astype(BF)
            if not (isinstance(j, int) and j == 0):
                activate(j - 1, 1 - slot)
            out_copy(ubuf, slot, u_all, m, j, uo_sem).start()

        block(0, 0)

        @pl.loop(0, (N_BLK - 2) // 2)
        def _(i):
            block(2 * i + 1, 1)
            block(2 * i + 2, 0)

        block(N_BLK - 1, 1)
        activate(N_BLK - 1, 1)
        mid_copy(a_all, m).start()

        @pl.loop(0, DIM // HB)
        def _(c):
            ws = use(tall_start, tall_wait, base + N_BLK + 2 * c)
            accf[slot_m, :, cols(c)] = dot_nn(mid[:, 0:DIM], tall[ws])
            ws = use(tall_start, tall_wait, base + N_BLK + 2 * c + 1)
            accf[slot_m, :, cols(c)] += dot_nn(mid[:, DIM:HID], tall[ws])
            rs_part(accf, slot_m, rsf, m, c, sf_sem, rf_sem).start()

        for slot in range(2):
            out_copy(ubuf, slot, u_all, m, slot, uo_sem).wait()
        mid_copy(a_all, m).wait()

    def load_post(acc_buf, m, recv, src):
        ref = acc_buf.at[pl.ds(pl.multiple_of(m * HALF, HALF), HALF), :]
        pltpu.make_async_copy(ref, ref, recv.at[m]).wait()
        a = pltpu.make_async_copy(ref, rsv, p_sem.at[0])
        a.start()
        b = pltpu.make_async_copy(src.at[rows_of(m, my), :], res, p_sem.at[1])
        b.start()
        return a, b

    def forward_post(m):
        slot = lax.rem(m, 2)

        def run(src):
            t = pltpu.make_async_copy(tgt.at[rows_of(m, my), :], tbuf, p_sem.at[2])
            t.start()
            for cp in load_post(rsf, m, rf_sem, src):
                cp.wait()
            t.wait()

        @pl.when(first)
        def _():
            run(x_in)

        @pl.when(jnp.logical_not(first))
        def _():
            run(x_all)

        @pl.when(m >= 2)
        def _():
            @pl.when(last)
            def _():
                yl_send(m, slot).wait_send()

            @pl.when(jnp.logical_not(last))
            def _():
                for cp in yf_pair(m, slot):
                    cp.wait_send()

        y = (res[...].astype(F32) + (accf[slot, half_rows(my), :] + rsv[...])).astype(BF)

        @pl.when(jnp.logical_not(last))
        def _():
            yf[slot] = y
            own, cross = yf_pair(m, slot)
            own.start()
            by_pair = jnp.logical_and(st == 1, m >= RELAY0)

            @pl.when(by_pair)
            def _():
                fwd_send(m, slot).start()

            @pl.when(jnp.logical_not(by_pair))
            def _():
                cross.start()

        @pl.when(last)
        def _():
            err = y.astype(F32) - tbuf[...].astype(F32)
            yf[slot] = (err * (1.0 / N_ELEM)).astype(BF)
            sq = err * err
            part = sq[:, 0:128]
            for c in range(1, DIM // 128):
                part = part + sq[:, c * 128 : (c + 1) * 128]
            lsum[...] += jnp.sum(part.reshape(HALF // 8, 8, 128), axis=0)
            yl_own(m, slot).start()
            yl_send(m, slot).start()

            @pl.when(m == N_MB - 1)
            def _():
                pltpu.make_async_copy(lsum, lrx.at[my], lr_sem.at[my]).start()
                for cond, cp in loss_sends():
                    pl.when(cond)(cp.start)

    def pass_on(m, base, copy):
        ref = fwd.at[fwd_rows(m), :]
        pltpu.make_async_copy(ref, ref, fr_sem.at[m]).wait()

        @pl.when(m >= base + 2)
        def _():
            copy(m - 2).wait_send()

        copy(m).start()

    def relay(m):
        @pl.when(jnp.logical_and(st == 1, jnp.logical_and(m >= RELAY0, m < N_MB)))
        def _():
            pass_on(m, RELAY0, relay_x)

    def relay_back(m):
        @pl.when(jnp.logical_and(first, jnp.logical_and(m >= RELAY3, m < N_MB)))
        def _():
            pass_on(m, RELAY3, relay_e)

    def loss_sends():
        for y in range(2):
            for s in range(4):
                cp = pltpu.make_async_remote_copy(
                    src_ref=lsum,
                    dst_ref=lrx.at[my],
                    send_sem=ls_sem.at[y * 4 + s],
                    recv_sem=lr_sem.at[my],
                    device_id={"model": y, "stage": s},
                    device_id_type=MESH,
                )
                yield (True if s < 3 else my != y), cp

    def backward(m):
        base = m * n_back
        wait_in(e_all, m, er_sem)
        load_x(e_all, m)

        @pl.when(jnp.logical_and(m >= 1, jnp.logical_not(first)))
        def _():
            rs_copy(accb, 0, rsb, m - 1, sb_sem, rb_sem).wait_send()

        def slope(j, slot):
            mid[:, cols(j)] = (gelu_slope(uin[slot][...].astype(F32)) * qbuf[slot][...].astype(F32)).astype(BF)

        def block(j, slot):
            start = isinstance(j, int) and j == 0
            ws = use(flat_start, flat_wait, base + j)
            u_load(m, j, slot).start()
            if not start:
                u_load(m, j - 1, 1 - slot).wait()
            qbuf[slot][...] = dot_nt(xbuf[...], flat[ws]).astype(BF)
            if not start:
                slope(j - 1, 1 - slot)

        block(0, 0)

        @pl.loop(0, (N_BLK - 2) // 2)
        def _(i):
            block(2 * i + 1, 1)
            block(2 * i + 2, 0)

        block(N_BLK - 1, 1)
        u_load(m, N_BLK - 1, 1).wait()
        slope(N_BLK - 1, 1)
        mid_copy(g_all, m).start()

        @pl.when(jnp.logical_not(first))
        def _():
            @pl.loop(0, DIM // HB)
            def _(c):
                ws = use(flat_start, flat_wait, base + N_BLK + 2 * c)
                accb[0, :, cols(c)] = dot_nt(mid[:, 0:DIM], flat[ws])
                ws = use(flat_start, flat_wait, base + N_BLK + 2 * c + 1)
                accb[0, :, cols(c)] += dot_nt(mid[:, DIM:HID], flat[ws])
                rs_part(accb, 0, rsb, m, c, sb_sem, rb_sem).start()

        mid_copy(g_all, m).wait()

    def backward_post(m):
        slot = lax.rem(m, 2)
        for cp in load_post(rsb, m, rb_sem, e_all):
            cp.wait()

        @pl.when(m >= 2)
        def _():
            for cp in yb_pair(m, slot):
                cp.wait_send()

        yb[slot] = (res[...].astype(F32) + (accb[0, half_rows(my), :] + rsv[...])).astype(BF)
        own, cross = yb_pair(m, slot)
        own.start()
        far = jnp.logical_and(last, m >= RELAY3)

        @pl.when(far)
        def _():
            far_send(m, slot).start()

        @pl.when(jnp.logical_not(far))
        def _():
            cross.start()

    def weight_ops(v):
        grp = v // GROUP
        quart = lax.rem(v, GROUP)
        rows = pl.ds(pl.multiple_of(grp * GTOK, GTOK), GTOK)
        out2 = quart < 2

        def on_tile(t, fn2, fn1):
            @pl.when(out2)
            def _():
                fn2(cols(quart * (HID // WT // 2) + t, WT))

            @pl.when(jnp.logical_not(out2))
            def _():
                fn1(cols(t, WT), cols(quart - 2, DIM))

        def start_tile(t):
            n_slot = lax.rem(t, 4)
            slot = lax.rem(t, N_WT)

            def fn2(blk):
                pltpu.make_async_copy(a_all.at[rows, blk], narrow.at[n_slot], wn_sem.at[n_slot]).start()

                @pl.when(grp > 0)
                def _():
                    pltpu.make_async_copy(acc2.at[blk, :], wtile.at[slot], wl_sem.at[slot]).start()

            def fn1(dblk, half):
                @pl.when(first)
                def _():
                    pltpu.make_async_copy(x_in.at[rows, dblk], narrow.at[n_slot], wn_sem.at[n_slot]).start()

                @pl.when(jnp.logical_not(first))
                def _():
                    pltpu.make_async_copy(x_all.at[rows, dblk], narrow.at[n_slot], wn_sem.at[n_slot]).start()

                @pl.when(grp > 0)
                def _():
                    pltpu.make_async_copy(acc1.at[dblk, half], wtile.at[slot], wl_sem.at[slot]).start()

            on_tile(t, fn2, fn1)

        def start_store(t):
            slot = lax.rem(t, N_WT)

            def fn2(blk):
                pltpu.make_async_copy(wtile.at[slot], acc2.at[blk, :], ws_sem.at[slot]).start()

            def fn1(dblk, half):
                pltpu.make_async_copy(wtile.at[slot], acc1.at[dblk, half], ws_sem.at[slot]).start()

            on_tile(t, fn2, fn1)

        def wait_store(slot):
            pltpu.make_async_copy(wtile.at[slot], acc2.at[pl.ds(0, WT), :], ws_sem.at[slot]).wait()

        def start():
            @pl.when(out2)
            def _():
                pltpu.make_async_copy(e_all.at[rows, :], wide, wd_sem).start()

            @pl.when(jnp.logical_not(out2))
            def _():
                pltpu.make_async_copy(g_all.at[rows, cols(quart - 2, DIM)], wide, wd_sem).start()

            for t in range(N_WT // 2):
                start_tile(t)

        n_tiles = DIM // WT

        def run(low, high):
            if low == 0:
                pltpu.make_async_copy(e_all.at[rows, :], wide, wd_sem).wait()

            @pl.loop(low, high)
            def _(t):
                slot = lax.rem(t, N_WT)
                n_slot = lax.rem(t, 4)

                @pl.when(t >= N_WT // 2)
                def _():
                    wait_store(lax.rem(t + N_WT // 2, N_WT))

                @pl.when(t + N_WT // 2 < n_tiles)
                def _():
                    start_tile(t + N_WT // 2)

                pltpu.make_async_copy(a_all.at[rows, pl.ds(0, WT)], narrow.at[n_slot], wn_sem.at[n_slot]).wait()

                @pl.when(grp > 0)
                def _():
                    pltpu.make_async_copy(acc2.at[pl.ds(0, WT), :], wtile.at[slot], wl_sem.at[slot]).wait()

                @pl.when(grp == 0)
                def _():
                    wtile[slot] = jnp.zeros((WT, DIM), F32)

                wtile[slot] += dot_tn(narrow[n_slot], wide[...])
                start_store(t)

            if high == n_tiles:
                for t in range(n_tiles - N_WT // 2, n_tiles):
                    wait_store(t % N_WT)

        return start, run

    lsum[...] = jnp.zeros((8, 128), F32)
    for j in range(W_SLOTS - 1):
        tall_start(j)
        flat_start(j)

    @pl.loop(0, N_MB + warm)
    def _(k):
        b = k - warm
        p = k - 1
        v = b - GROUP
        b_on = b >= 0
        f_on = k < N_MB
        p_on = jnp.logical_and(p >= EAGER, p < N_MB)
        pb_on = jnp.logical_and(b_on, jnp.logical_not(first))
        w_on = jnp.logical_and(v >= 0, jnp.logical_not(first))

        @pl.when(jnp.logical_and(first, v >= 0))
        def _():
            start, run = weight_ops(v)
            start()
            run(0, DIM // WT)

        @pl.when(b_on)
        def _():
            backward(b)
            relay_back(b + LEAD3)

        @pl.when(jnp.logical_and(b_on, p_on))
        def _():
            forward_post(p)

        @pl.when(b_on)
        def _():
            relay(k - 2)

        @pl.when(jnp.logical_and(w_on, jnp.logical_not(f_on)))
        def _():
            weight_ops(v)[0]()

        @pl.when(f_on)
        def _():
            forward(k, lambda: pl.when(w_on)(weight_ops(v)[0]))

        @pl.when(k < EAGER)
        def _():
            forward_post(k)

        @pl.when(jnp.logical_and(jnp.logical_not(b_on), p_on))
        def _():
            forward_post(p)

        @pl.when(jnp.logical_not(b_on))
        def _():
            relay(k - 2)

        post_first = jnp.logical_or(f_on, b >= jnp.where(st == 1, N_MB - 1, N_MB - 2))

        @pl.when(jnp.logical_and(pb_on, post_first))
        def _():
            backward_post(b)

        @pl.when(w_on)
        def _():
            weight_ops(v)[1](0, DIM // WT)

        @pl.when(jnp.logical_and(pb_on, jnp.logical_not(post_first)))
        def _():
            backward_post(b)

    for half in range(2):
        pltpu.make_async_copy(lsum, lrx.at[half], lr_sem.at[half]).wait()
    loss[...] = lrx[0] + lrx[1]

    for j in range(W_SLOTS - 1):
        tall_wait(j)
        flat_wait(j)
    for m in (N_MB - 2, N_MB - 1):
        slot = m % 2
        rs_copy(accf, slot, rsf, m, sf_sem, rf_sem).wait_send()

        @pl.when(jnp.logical_not(first))
        def _():
            if m == N_MB - 1:
                rs_copy(accb, 0, rsb, m, sb_sem, rb_sem).wait_send()
            for cp in yb_pair(m, slot):
                cp.wait_send()

        @pl.when(last)
        def _():
            yl_send(m, slot).wait_send()

        @pl.when(jnp.logical_not(last))
        def _():
            for cp in yf_pair(m, slot):
                cp.wait_send()

        @pl.when(st == 1)
        def _():
            relay_x(m).wait_send()

        @pl.when(first)
        def _():
            relay_e(m).wait_send()

    @pl.when(last)
    def _():
        for cond, cp in loss_sends():
            pl.when(cond)(cp.wait_send)


def run_pipeline(x_in, tgt, w1, w2):
    tokens = N_MB * TOK
    hbm = pl.BlockSpec(memory_space=pl.ANY)
    dma = pltpu.SemaphoreType.DMA
    shapes = [
        ((tokens, DIM), BF), ((tokens, DIM), BF),
        ((tokens, HID), BF), ((tokens, HID), BF), ((tokens, HID), BF),
        ((tokens // 2, DIM), F32), ((tokens // 2, DIM), F32), ((tokens // 2, DIM), BF),
        ((DIM, HID), F32), ((HID, DIM), F32),
    ]
    out_shape = [jax.ShapeDtypeStruct(s, d) for s, d in shapes] + [jax.ShapeDtypeStruct((8, 128), F32)]
    return pl.pallas_call(
        pipeline_kernel,
        out_shape=out_shape,
        in_specs=[hbm] * 4,
        out_specs=[hbm] * 10 + [pl.BlockSpec(memory_space=pltpu.VMEM)],
        scratch_shapes=[
            pltpu.VMEM((TOK, DIM), BF),
            pltpu.VMEM((W_SLOTS, DIM, HB), BF),
            pltpu.VMEM((W_SLOTS, HB, DIM), BF),
            pltpu.VMEM((TOK, HB), BF), pltpu.VMEM((TOK, HB), BF),
            pltpu.VMEM((TOK, HB), BF), pltpu.VMEM((TOK, HB), BF),
            pltpu.VMEM((TOK, HB), BF), pltpu.VMEM((TOK, HB), BF),
            pltpu.VMEM((TOK, HID), BF),
            pltpu.VMEM((2, TOK, DIM), F32),
            pltpu.VMEM((1, TOK, DIM), F32),
            pltpu.VMEM((HALF, DIM), F32),
            pltpu.VMEM((HALF, DIM), BF),
            pltpu.VMEM((HALF, DIM), BF),
            pltpu.VMEM((2, HALF, DIM), BF),
            pltpu.VMEM((2, HALF, DIM), BF),
            pltpu.VMEM((GTOK, DIM), BF),
            pltpu.VMEM((4, GTOK, WT), BF),
            pltpu.VMEM((N_WT, WT, DIM), F32),
            pltpu.VMEM((8, 128), F32),
            pltpu.VMEM((2, 8, 128), F32),
            dma((W_SLOTS,)), dma((W_SLOTS,)), dma, dma((2,)), dma, dma((2,)), dma((3,)), dma, dma((4,)), dma((N_WT,)), dma((N_WT,)),
            dma((N_MB, 2)), dma((N_MB, 2)), dma((N_MB,)), dma((N_MB,)), dma((2,)), dma((1,)), dma((2, 2)), dma((2, 2)),
            dma((N_MB,)), dma((2,)), dma((8,)), dma((2,)),
        ],
        compiler_params=pltpu.CompilerParams(vmem_limit_bytes=67_000_000, has_side_effects=True),
        name="pipeline",
    )(x_in, tgt, w1, w2)


def tail_kernel(x_all, e_all, a_all, g_all, acc1, acc2, out1, out2, wide, narrow, tile, wide_sem, n_sem, l_sem, s_sem):
    rows = pl.ds(N_GRP * GTOK, GTOK)
    n2 = HID // HB
    n1 = DIM // HB

    def cols(j, width=HB):
        return pl.ds(pl.multiple_of(j * width, width), width)

    def on_tile(t, fn2, fn1):
        @pl.when(t < n2)
        def _():
            fn2(cols(t))

        @pl.when(t >= n2)
        def _():
            fn1(cols(lax.rem(t - n2, n1)), cols((t - n2) // n1, DIM))

    def start_tile(t):
        slot = lax.rem(t, 4)
        n_slot = lax.rem(t, 3)

        def fn2(blk):
            pltpu.make_async_copy(acc2.at[blk, :], tile.at[slot], l_sem.at[slot]).start()
            pltpu.make_async_copy(a_all.at[rows, blk], narrow.at[n_slot], n_sem.at[n_slot]).start()

        def fn1(dblk, half):
            pltpu.make_async_copy(acc1.at[dblk, half], tile.at[slot], l_sem.at[slot]).start()
            pltpu.make_async_copy(x_all.at[rows, dblk], narrow.at[n_slot], n_sem.at[n_slot]).start()

        on_tile(t, fn2, fn1)

    def start_store(t):
        slot = lax.rem(t, 4)

        def fn2(blk):
            pltpu.make_async_copy(tile.at[slot], out2.at[blk, :], s_sem.at[slot]).start()

        def fn1(dblk, half):
            pltpu.make_async_copy(tile.at[slot], out1.at[dblk, half], s_sem.at[slot]).start()

        on_tile(t, fn2, fn1)

    def wait_store(slot):
        pltpu.make_async_copy(tile.at[slot], out2.at[pl.ds(0, HB), :], s_sem.at[slot]).wait()

    def wide_copy(i):
        src = e_all.at[rows, :] if i == 0 else g_all.at[rows, pl.ds((i - 1) * DIM, DIM)]
        return pltpu.make_async_copy(src, wide.at[i], wide_sem.at[i])

    start_tile(0)
    wide_copy(0).start()
    start_tile(1)

    @pl.loop(0, n2 + 2 * n1)
    def _(t):
        slot = lax.rem(t, 4)
        n_slot = lax.rem(t, 3)

        @pl.when(t >= 2)
        def _():
            wait_store(lax.rem(t + 2, 4))

        @pl.when(t + 2 < n2 + 2 * n1)
        def _():
            start_tile(t + 2)

        for i in range(1, 3):

            @pl.when(t == n2 + (i - 1) * n1 - 4)
            def _():
                wide_copy(i).start()

        for i in range(3):

            @pl.when(t == (0 if i == 0 else n2 + (i - 1) * n1))
            def _():
                wide_copy(i).wait()

        pltpu.make_async_copy(a_all.at[rows, pl.ds(0, HB)], narrow.at[n_slot], n_sem.at[n_slot]).wait()
        pltpu.make_async_copy(acc2.at[pl.ds(0, HB), :], tile.at[slot], l_sem.at[slot]).wait()
        which = jnp.where(t < n2, 0, 1 + (t - n2) // n1)
        tile[slot] += dot_tn(narrow[n_slot], wide[which])
        start_store(t)

    wait_store(2)
    wait_store(3)


def add_tail(x_all, e_all, a_all, g_all, acc1, acc2):
    hbm = pl.BlockSpec(memory_space=pl.ANY)
    dma = pltpu.SemaphoreType.DMA
    return pl.pallas_call(
        tail_kernel,
        in_specs=[hbm] * 6,
        out_specs=[hbm] * 2,
        out_shape=[jax.ShapeDtypeStruct(acc1.shape, F32), jax.ShapeDtypeStruct(acc2.shape, F32)],
        scratch_shapes=[
            pltpu.VMEM((3, GTOK, DIM), BF),
            pltpu.VMEM((3, GTOK, HB), BF),
            pltpu.VMEM((4, HB, DIM), F32),
            dma((3,)), dma((3,)), dma((4,)), dma((4,)),
        ],
        compiler_params=pltpu.CompilerParams(vmem_limit_bytes=60_000_000),
        name="tail",
    )(x_all, e_all, a_all, g_all, acc1, acc2)


def solution(mesh):
    def stage_step(inputs, targets, w_in, w_out):
        tokens = N_MB * TOK
        x_in = inputs.reshape(tokens, DIM)
        tgt = targets.reshape(tokens, DIM)
        x_all, e_all, _, a_all, g_all, _, _, _, acc1, acc2, loss = run_pipeline(x_in, tgt, w_in[0, 0], w_out[0, 0])
        grad_in, grad_out = add_tail(x_all, e_all, a_all, g_all, acc1, acc2)
        total = jnp.sum(loss) * (0.5 / N_ELEM)
        return grad_in[None, None], grad_out[None, None], jnp.reshape(total, (1,))

    return jax.shard_map(
        stage_step,
        mesh=mesh,
        in_specs=(P("data", None, None), P("data", None, None), P("stage", None, None, "model"), P("stage", None, "model", None)),
        out_specs=(P(("data", "stage"), None, None, "model"), P(("data", "stage"), None, "model", None), P("data")),
        check_vma=False,
    )
```
